256 devices in a mesh: tp: 8 (over x, core), cp: 32 (over z, y).
Axes of the slice: x: 4, y: 4, z: 8, core: 2. Of those that a mesh axis runs over, the one named last changes fastest.
Arguments:
- tokens: bfloat16 [1024, 8192], P(('cp', 'tp')), may hold values from -6 to 6
- attention_gain: float32 [8192], replicated, may hold values from 0.1 to 1.9
- query_weight: bfloat16 [8192, 8192], P('cp', 'tp'), may hold values from -0.0625 to 0.0625
- key_weight: bfloat16 [8192, 1024], P('cp', 'tp'), may hold values from -0.0625 to 0.0625
- value_weight: bfloat16 [8192, 1024], P('cp', 'tp'), may hold values from -0.0625 to 0.0625
- out_weight: bfloat16 [8192, 8192], P('tp', 'cp'), may hold values from -0.0625 to 0.0625
- feed_gain: float32 [8192], replicated, may hold values from 0.1 to 1.9
- gate_weight: bfloat16 [8192, 28672], P('tp', 'cp'), may hold values from -0.0625 to 0.0625
- up_weight: bfloat16 [8192, 28672], P('tp', 'cp'), may hold values from -0.0625 to 0.0625
- down_weight: bfloat16 [28672, 8192], P('cp', 'tp'), may hold values from -0.03125 to 0.03125
Outputs:
- attended: bfloat16 [1024, 8192], P(('cp', 'tp'))
- mixed: bfloat16 [1024, 8192], P(('cp', 'tp'))
The draws below stay inside these ranges and needn't reach their ends.
All inputs are finite; a program needn't handle non-finite values.
Results may differ from the reference program's by a relative error of at most 0.035.
Values may be sent and summed in bfloat16 or wider, within the bound.
A program may use at most 64 MiB of HBM per device.

```python
import jax
import jax.numpy as jnp
from jax import lax

D = 8192
HQ = 64
KV = 8
HD = 128
FF = 28672
SEQ = 1024


def levels(own_key, shape, split, smallest, high):
    factor_of, own = 1.0, jax.random.fold_in(own_key, 6)
    for position, shards_of in split:
        steps = jnp.exp(jax.random.uniform(jax.random.fold_in(own, position), (shards_of,), jnp.float32, smallest / len(split), high / len(split)))
        factor_of = factor_of * jnp.repeat(steps, shape[position] // shards_of).reshape([-1 if axis == position else 1 for axis in range(len(shape))])
    return factor_of


def centred(key, extent, spread, bound, cuts=(), kind=jnp.bfloat16):
    result = spread * jax.random.normal(key, extent, jnp.float32)
    if cuts:
        result = result * levels(key, extent, cuts, -0.22, 0.18)
    return jnp.clip(result, -bound, bound).astype(kind)


def setup_inputs(seed: int = 0) -> dict:
    key_list = jax.random.split(jax.random.key(seed), 11)
    return {
        "tokens": centred(key_list[0], (SEQ, D), 0.5, 6.0, ((0, 256),)),
        "attention_gain": jnp.clip(1.0 + 0.18 * jax.random.normal(key_list[1], (D,), jnp.float32), 0.1, 1.9),
        "query_weight": centred(key_list[2], (D, HQ * HD), D ** -0.5, 0.0625, ((0, 32), (1, 8))),
        "key_weight": centred(key_list[3], (D, KV * HD), D ** -0.5, 0.0625, ((0, 32), (1, 8))),
        "value_weight": centred(key_list[4], (D, KV * HD), D ** -0.5, 0.0625, ((0, 32), (1, 8))),
        "out_weight": centred(key_list[5], (HQ * HD, D), (HQ * HD) ** -0.5, 0.0625, ((0, 8), (1, 32))),
        "feed_gain": jnp.clip(1.0 + 0.18 * jax.random.normal(key_list[6], (D,), jnp.float32), 0.1, 1.9),
        "gate_weight": centred(key_list[7], (D, FF), D ** -0.5, 0.0625, ((0, 8), (1, 32))),
        "up_weight": centred(key_list[8], (D, FF), D ** -0.5, 0.0625, ((0, 8), (1, 32))),
        "down_weight": centred(key_list[9], (FF, D), FF ** -0.5, 0.03125, ((0, 32), (1, 8))),
    }


epsilon = 1e-05
rope_base = 500000.0

def normalize(values, gain):
    widened = values.astype(jnp.float32)
    mean_square = lax.optimization_barrier(jnp.mean(widened * widened, axis=-1, keepdims=True))
    return (widened * lax.rsqrt(mean_square + epsilon) * gain).astype(jnp.bfloat16)

def rotate(values, positions):
    row_count = values.shape[0]
    heads = values.reshape(row_count, -1, HD)
    half = HD // 2
    inverse = rope_base ** (-(jnp.arange(half, dtype=jnp.float32) * 2.0 / HD))
    angles = positions.astype(jnp.float32)[:, None] * inverse[None, :]
    cosine = jnp.cos(angles)[:, None, :]
    sine = jnp.sin(angles)[:, None, :]
    first = heads[..., :half]
    second = heads[..., half:]
    turned = jnp.concatenate([first * cosine - second * sine, second * cosine + first * sine], axis=-1)
    return turned.reshape(row_count, -1)

def reference(tokens, attention_gain, query_weight, key_weight, value_weight, out_weight, feed_gain, gate_weight, up_weight, down_weight):
    normed = normalize(tokens, attention_gain)
    positions = jnp.arange(SEQ, dtype=jnp.int32)
    query = rotate(jnp.dot(normed, query_weight, preferred_element_type=jnp.float32), positions).astype(jnp.bfloat16)
    keys = rotate(jnp.dot(normed, key_weight, preferred_element_type=jnp.float32), positions).astype(jnp.bfloat16)
    values = jnp.dot(normed, value_weight, preferred_element_type=jnp.float32).astype(jnp.bfloat16)
    group_size = HQ // KV
    query_heads = query.astype(jnp.float32).reshape(SEQ, KV, group_size, HD).transpose(1, 0, 2, 3)
    key_heads = keys.astype(jnp.float32).reshape(SEQ, KV, HD).transpose(1, 0, 2)
    value_heads = values.astype(jnp.float32).reshape(SEQ, KV, HD).transpose(1, 0, 2)
    allowed = positions[None, :] <= positions[:, None]
    scale = HD ** (-0.5)

    def one_head(operands):
        head_query, head_keys, head_values = operands
        scores = jnp.einsum('qgd,sd->gqs', head_query, head_keys, precision=lax.Precision.HIGHEST) * scale
        scores = jnp.where(allowed[None], scores, -1e+30)
        weights = jax.nn.softmax(scores, axis=-1)
        return jnp.einsum('gqs,sd->qgd', weights, head_values, precision=lax.Precision.HIGHEST)
    head_outputs = lax.map(one_head, (query_heads, key_heads, value_heads))
    attention = head_outputs.transpose(1, 0, 2, 3).reshape(SEQ, HQ * HD).astype(jnp.bfloat16)
    projected = jnp.dot(attention, out_weight, preferred_element_type=jnp.float32)
    attended = (tokens.astype(jnp.float32) + projected).astype(jnp.bfloat16)
    normed_feed = normalize(attended, feed_gain)
    gate = jnp.dot(normed_feed, gate_weight, preferred_element_type=jnp.float32)
    upward = jnp.dot(normed_feed, up_weight, preferred_element_type=jnp.float32)
    hidden = (jax.nn.silu(gate) * upward).astype(jnp.bfloat16)
    lowered = jnp.dot(hidden, down_weight, preferred_element_type=jnp.float32)
    mixed = (attended.astype(jnp.float32) + lowered).astype(jnp.bfloat16)
    return (attended, mixed)
```

```python
import collections
import functools

import jax
import jax.numpy as jnp
from jax import lax
from jax.experimental import pallas as pl
from jax.experimental.pallas import tpu as pltpu
from jax.sharding import PartitionSpec as P

HD = 128
NZ, NY, NX = 8, 4, 4
CP, TP = NZ * NY, NX * 2
MESH = pl.DeviceIdType.MESH
F32, BF16 = jnp.float32, jnp.bfloat16

epsilon = 1e-05
rope_base = 500000.0
masked = -1e30


class Wires:
    def __init__(self, send, recv):
        self.send, self.recv, self.used, self.sent = send, recv, 0, []

    def copy(self, src, dst, device):
        i = self.used
        self.used += 1
        c = pltpu.make_async_remote_copy(
            src_ref=src,
            dst_ref=dst,
            send_sem=self.send.at[i],
            recv_sem=self.recv.at[i],
            device_id=device,
            device_id_type=MESH,
        )
        c.start()
        self.sent.append(c)
        return c

    def drain(self):
        for c in self.sent:
            c.wait_send()


class Steps:
    def __init__(self):
        self.queue = collections.deque()

    def add(self, gen):
        if next(gen, self) is not self:
            self.queue.append(gen)

    def run(self):
        while self.queue:
            self.add(self.queue.popleft())


class Place:
    def __init__(self):
        self.cp, self.tp = lax.axis_index("cp"), lax.axis_index("tp")
        self.z, self.y = self.cp // NY, self.cp % NY
        self.x, self.core = self.tp // 2, self.tp % 2

    def along_z(self, z):
        return {"cp": z * NY + self.y}

    def along_y(self, y):
        return {"cp": self.z * NY + y}

    def along_x(self, x):
        return {"tp": x * 2 + self.core}

    def partner(self):
        return {"tp": self.x * 2 + 1 - self.core}


def ring(n, me, device_of):
    return device_of((me + 1) % n), device_of((me + n - 1) % n)


def greet(devices):
    barrier = pltpu.get_barrier_semaphore()
    for device in devices:
        pl.semaphore_signal(barrier, inc=1, device_id=device, device_id_type=MESH)
    return len(devices)


def greet_group(axis, n, me):
    barrier = pltpu.get_barrier_semaphore()

    def signal(off, carry):
        pl.semaphore_signal(
            barrier, inc=1, device_id={axis: (me + off) % n}, device_id_type=MESH
        )
        return carry

    lax.fori_loop(1, n, signal, 0)
    return n - 1


def await_greetings(count):
    pl.semaphore_wait(pltpu.get_barrier_semaphore(), count)


def half_of(ref, h):
    d = ref.shape[0] // 2
    return ref.at[pl.ds(h * d, d)]


def ring_gather(wires, block, n, me, device_of, arrived=None):
    right, left = ring(n, me, device_of)
    last = n // 2 - 1

    def send(k):
        r, l = block((me + n - k) % n), block((me + k) % n)
        if k == last:
            r, l = half_of(r, 0), half_of(l, 1)
        return wires.copy(r, r, right), wires.copy(l, l, left)

    flying = send(0)
    if arrived:
        arrived(me)
    for k in range(1, n // 2 + 1):
        yield
        for c in flying:
            c.wait_recv()
        if k <= last:
            flying = send(k)
            if arrived:
                arrived((me + n - k) % n)
                arrived((me + k) % n)
        elif arrived:
            arrived((me + n // 2) % n)


def add_rows(dst, terms, finish=None):
    if len(dst.shape) == 3:
        for i in range(dst.shape[0]):
            add_rows(dst.at[i], [t.at[i] for t in terms])
        return
    rows = dst.shape[0]
    step = min(rows, 16)

    def body(i, carry):
        at = pl.ds(pl.multiple_of(i * step, step), step)
        total = terms[0][at, :].astype(F32)
        for t in terms[1:]:
            total = total + t[at, :].astype(F32)
        dst[at, :] = total.astype(dst.dtype)
        return carry

    lax.fori_loop(0, rows // step, body, 0)


def ring_scatter(wires, own, out, from_left, from_right, n, me, device_of):
    right, left = ring(n, me, device_of)
    m = n // 2
    far = own((me + m) % n)
    r = wires.copy(half_of(far, 0), half_of(from_left.at[0], 0), right)
    l = wires.copy(half_of(far, 1), half_of(from_right.at[0], 1), left)
    for k in range(1, m):
        yield
        to_right, to_left = own((me + m - k) % n), own((me + n - m + k) % n)
        got_left, got_right = from_left.at[k - 1], from_right.at[k - 1]
        r.wait_recv()
        if k == 1:
            add_rows(half_of(got_left, 0), [half_of(got_left, 0), half_of(to_right, 0)])
            add_rows(half_of(got_left, 1), [half_of(to_right, 1)])
        else:
            add_rows(got_left, [got_left, to_right])
        r = wires.copy(got_left, from_left.at[k], right)
        l.wait_recv()
        if k == 1:
            add_rows(half_of(got_right, 1), [half_of(got_right, 1), half_of(to_left, 1)])
            add_rows(half_of(got_right, 0), [half_of(to_left, 0)])
        else:
            add_rows(got_right, [got_right, to_left])
        l = wires.copy(got_right, from_right.at[k], left)
    yield
    r.wait_recv()
    l.wait_recv()
    add_rows(out, [own(me), from_left.at[m - 1], from_right.at[m - 1]])


def exchange(send_sem, recv_sem, source, target, axis, n, me, meanwhile=None):
    def copy(off):
        peer = (me + off) % n
        return pltpu.make_async_remote_copy(
            src_ref=source(peer),
            dst_ref=target(me),
            send_sem=send_sem.at[off],
            recv_sem=recv_sem.at[off],
            device_id={axis: peer},
            device_id_type=MESH,
        )

    def start(off, carry):
        copy(off).start()
        return carry

    def wait(off, carry):
        copy(off).wait()
        return carry

    lax.fori_loop(1, n, start, 0)
    if meanwhile:
        meanwhile()
    lax.fori_loop(1, n, wait, 0)


VMEM = pl.BlockSpec(memory_space=pltpu.VMEM)


def call(kernel, out_shape, inputs, scratch, collective_id, name):
    return pl.pallas_call(
        kernel,
        out_shape=out_shape,
        in_specs=[VMEM] * len(inputs),
        out_specs=jax.tree.map(lambda _: VMEM, out_shape),
        scratch_shapes=scratch,
        compiler_params=pltpu.CompilerParams(
            collective_id=collective_id,
            has_side_effects=True,
            vmem_limit_bytes=56 * 1024 * 1024,
        ),
        name=name,
    )(*inputs)


def dma(count):
    return pltpu.SemaphoreType.DMA((count,))


def spread_kernel(x_ref, out_ref, got, s0, r0, s1, r1):
    at = Place()
    await_greetings(greet_group("cp", CP, at.cp) + greet_group("tp", TP, at.tp))

    def keep():
        got[at.cp] = x_ref[at.cp]

    exchange(s0, r0, lambda p: x_ref.at[p], lambda p: got.at[p], "cp", CP, at.cp, keep)

    def keep_too():
        out_ref[at.tp] = got[...]

    exchange(s1, r1, lambda p: got, lambda p: out_ref.at[p], "tp", TP, at.tp, keep_too)


def spread(x, collective_id):
    return call(
        spread_kernel,
        jax.ShapeDtypeStruct((TP, *x.shape), x.dtype),
        (x,),
        [pltpu.VMEM(x.shape, x.dtype), dma(CP), dma(CP), dma(TP), dma(TP)],
        collective_id,
        "spread",
    )


def collect_kernel(x_ref, out_ref, got, total, s0, r0, s1, r1):
    at = Place()
    await_greetings(greet_group("cp", CP, at.cp) + greet_group("tp", TP, at.tp))

    def keep():
        got[at.tp] = x_ref[at.tp]

    exchange(s0, r0, lambda p: x_ref.at[p], lambda p: got.at[p], "tp", TP, at.tp, keep)

    def body(i, carry):
        parts = got[0, i].astype(F32)
        for t in range(1, TP):
            parts = parts + got[t, i].astype(F32)
        total[i] = parts.astype(BF16)
        return carry

    lax.fori_loop(0, CP, body, 0)

    def keep_too():
        out_ref[at.cp] = total[at.cp]

    exchange(s1, r1, lambda p: total.at[p], lambda p: out_ref.at[p], "cp", CP, at.cp, keep_too)


def collect(x, collective_id):
    return call(
        collect_kernel,
        jax.ShapeDtypeStruct(x.shape[1:], x.dtype),
        (x,),
        [
            pltpu.VMEM(x.shape, x.dtype),
            pltpu.VMEM(x.shape[1:], x.dtype),
            dma(TP),
            dma(TP),
            dma(CP),
            dma(CP),
        ],
        collective_id,
        "collect",
    )


def swap_kernel(x_ref, out_ref, s0, r0):
    at = Place()
    await_greetings(greet_group("tp", TP, at.tp))

    def keep():
        out_ref[at.tp] = x_ref[at.tp]

    exchange(s0, r0, lambda p: x_ref.at[p], lambda p: out_ref.at[p], "tp", TP, at.tp, keep)


def swap(x, collective_id):
    return call(
        swap_kernel,
        jax.ShapeDtypeStruct(x.shape, x.dtype),
        (x,),
        [dma(TP), dma(TP)],
        collective_id,
        "swap",
    )


def greet_context(at):
    return greet([*ring(NZ, at.z, at.along_z), *ring(NY, at.y, at.along_y)])


def gather_rows(wires, steps, at, out_ref, split):
    first, rest = pl.ds(0, split), pl.ds(split, out_ref.shape[-1] - split)

    def y_first():
        yield from ring_gather(
            wires, lambda j: out_ref.at[at.z, j, :, rest], NY, at.y, at.along_y
        )
        yield from ring_gather(
            wires, lambda i: out_ref.at[i, :, :, rest], NZ, at.z, at.along_z
        )

    def to_y(i):
        steps.add(
            ring_gather(wires, lambda j: out_ref.at[i, j, :, first], NY, at.y, at.along_y)
        )

    steps.add(y_first())
    steps.add(
        ring_gather(
            wires, lambda i: out_ref.at[i, at.y, :, first], NZ, at.z, at.along_z, to_y
        )
    )


GATHER_COPIES = 2 * (NY // 2 + NZ // 2) + NZ + NZ * NY


def gather_kernel(split, x_ref, out_ref, send, recv):
    at = Place()
    greeted = greet_context(at)
    out_ref[at.z, at.y] = x_ref[...]
    await_greetings(greeted)
    wires, steps = Wires(send, recv), Steps()
    gather_rows(wires, steps, at, out_ref, split)
    steps.run()
    wires.drain()


def gather(x, split, collective_id):
    return call(
        functools.partial(gather_kernel, split),
        jax.ShapeDtypeStruct((NZ, NY, *x.shape), x.dtype),
        (x,),
        [dma(GATHER_COPIES), dma(GATHER_COPIES)],
        collective_id,
        "gather",
    )


def product_into(part, x_ref, w_ref, start):
    width = w_ref.shape[1]
    tile = min(width, 256)

    def body(i, carry):
        at = pl.multiple_of(i * tile, tile)
        p = jnp.dot(x_ref[...], w_ref[:, pl.ds(at, tile)], preferred_element_type=F32)
        part[:, :, :, pl.ds(pl.multiple_of(start + at, 128), tile)] = p.astype(BF16).reshape(
            *part.shape[:3], tile
        )
        return carry

    lax.fori_loop(0, width // tile, body, 0)


def scatter_rows(wires, steps, at, part, out, split, bufs):
    zl, zr, yl, yr, y_sum, yl2, yr2, zl2, zr2, z_sum = bufs
    first, rest = pl.ds(0, split), pl.ds(split, part.shape[-1] - split)

    def z_first():
        yield from ring_scatter(
            wires, lambda i: part.at[i, :, :, first], y_sum, zl, zr, NZ, at.z, at.along_z
        )
        yield from ring_scatter(
            wires, lambda j: y_sum.at[j], out.at[:, first], yl, yr, NY, at.y, at.along_y
        )

    def y_first():
        yield from ring_scatter(
            wires, lambda j: part.at[:, j, :, rest], z_sum, yl2, yr2, NY, at.y, at.along_y
        )
        yield from ring_scatter(
            wires, lambda i: z_sum.at[i], out.at[:, rest], zl2, zr2, NZ, at.z, at.along_z
        )

    steps.add(y_first())
    steps.add(z_first())


SCATTER_COPIES = 2 * (NZ + NY)


def scatter_scratch(rows, width, split):
    a, b = split, width - split

    def both(*shape):
        return [pltpu.VMEM(shape, BF16), pltpu.VMEM(shape, BF16)]

    return [
        *both(NZ // 2, NY, rows, a),
        *both(NY // 2, rows, a),
        pltpu.VMEM((NY, rows, a), BF16),
        *both(NY // 2, NZ, rows, b),
        *both(NZ // 2, rows, b),
        pltpu.VMEM((NZ, rows, b), BF16),
    ]


def project_kernel(split, count, *refs):
    x_ref, weights, out_ref = refs[0], refs[1 : 1 + count], refs[1 + count]
    part, *bufs = refs[2 + count : -2]
    send, recv = refs[-2:]
    at = Place()
    greeted = greet_context(at)
    start = 0
    for w_ref in weights:
        product_into(part, x_ref, w_ref, start)
        start += w_ref.shape[1]
    await_greetings(greeted)
    wires, steps = Wires(send, recv), Steps()
    scatter_rows(wires, steps, at, part, out_ref, split, bufs)
    steps.run()
    wires.drain()


def project(x, weights, split, collective_id):
    rows = x.shape[0] // CP
    width = sum(w.shape[1] for w in weights)
    return call(
        functools.partial(project_kernel, split, len(weights)),
        jax.ShapeDtypeStruct((rows, width), F32),
        (x, *weights),
        [
            pltpu.VMEM((NZ, NY, rows, width), BF16),
            *scatter_scratch(rows, width, split),
            dma(SCATTER_COPIES),
            dma(SCATTER_COPIES),
        ],
        collective_id,
        "project",
    )


UNITS = 2


def feed_kernel(x_ref, gate_ref, up_ref, out_ref, part, held, fl, fr, total, send, recv):
    at = Place()
    partner = at.partner()
    await_greetings(greet([*ring(NX, at.x, at.along_x), partner]))
    wires, steps = Wires(send, recv), Steps()
    units = gate_ref.shape[1]
    block = part.shape[2]
    rows = block // UNITS
    other = 1 - at.core

    def product(i):
        x = x_ref.at[pl.ds(pl.multiple_of(i * 2 * block, 2 * block), 2 * block)]

        def tile(w_ref, col, width, start):
            p = jnp.dot(x[...], w_ref[:, pl.ds(col, width)], preferred_element_type=F32)
            part[i, :, :, pl.ds(start + col, width)] = p.astype(BF16).reshape(2, block, width)

        def body(t, carry):
            col = pl.multiple_of(t * 256, 256)
            tile(gate_ref, col, 256, 0)
            tile(up_ref, col, 256, units)
            return carry

        lax.fori_loop(0, units // 256, body, 0)
        if units % 256:
            tile(gate_ref, units // 256 * 256, units % 256, 0)
            tile(up_ref, units // 256 * 256, units % 256, units)
        return wires.copy(part.at[i, other], held.at[i], partner)

    def combine(i, c):
        c.wait_recv()
        add_rows(held.at[i], [held.at[i], part.at[i, at.core]])

    def line(u):
        at_rows = pl.ds(u * rows, rows)
        yield from ring_scatter(
            wires,
            lambda i: held.at[i, at_rows],
            total.at[u],
            fl.at[u],
            fr.at[u],
            NX,
            at.x,
            at.along_x,
        )

        def body(i, carry):
            r = pl.ds(pl.multiple_of(i * 16, 16), 16)
            gate, up = total[u, r, pl.ds(0, units)], total[u, r, pl.ds(units, units)]
            out_ref[at.x, at.core, pl.ds(pl.multiple_of(u * rows + i * 16, 16), 16), :] = (
                jax.nn.silu(gate) * up
            ).astype(BF16)
            return carry

        lax.fori_loop(0, rows // 16, body, 0)

        def hand_over(i):
            ref = out_ref.at[i, at.core, at_rows]
            handed.append(wires.copy(ref, ref, partner))

        yield from ring_gather(
            wires, lambda i: out_ref.at[i, at.core, at_rows], NX, at.x, at.along_x, hand_over
        )

    handed = []
    order = [(at.x + 2) % NX, (at.x + 1) % NX, (at.x + 3) % NX, at.x]
    copies = [product(order[0])]
    copies.append(product(order[1]))
    combine(order[0], copies[0])
    for u in range(UNITS):
        steps.add(line(u))
    copies.append(product(order[2]))
    combine(order[1], copies[1])
    copies.append(product(order[3]))
    combine(order[2], copies[2])
    combine(order[3], copies[3])
    steps.run()
    for c in handed:
        c.wait_recv()
    wires.drain()


def feed(x, gate, up, collective_id):
    block = x.shape[0] // TP
    units = gate.shape[1]
    copies = NX + UNITS * (2 * NX + NX)
    steps = NX // 2
    return call(
        feed_kernel,
        jax.ShapeDtypeStruct((NX, 2, block, units), BF16),
        (x, gate, up),
        [
            pltpu.VMEM((NX, 2, block, 2 * units), BF16),
            pltpu.VMEM((NX, block, 2 * units), BF16),
            pltpu.VMEM((UNITS, steps, block // UNITS, 2 * units), BF16),
            pltpu.VMEM((UNITS, steps, block // UNITS, 2 * units), BF16),
            pltpu.VMEM((UNITS, block // UNITS, 2 * units), F32),
            dma(copies),
            dma(copies),
        ],
        collective_id,
        "feed",
    )


def normalize(values, gain):
    widened = values.astype(F32)
    mean_square = jnp.mean(widened * widened, axis=-1, keepdims=True)
    return (widened * lax.rsqrt(mean_square + epsilon) * gain).astype(BF16)


def rotate(values, positions):
    row_count = values.shape[0]
    heads = values.reshape(row_count, -1, HD)
    half = HD // 2
    inverse = rope_base ** (-(jnp.arange(half, dtype=F32) * 2.0 / HD))
    angles = positions.astype(F32)[:, None] * inverse[None, :]
    cosine = jnp.cos(angles)[:, None, :]
    sine = jnp.sin(angles)[:, None, :]
    first = heads[..., :half]
    second = heads[..., half:]
    turned = jnp.concatenate(
        [first * cosine - second * sine, second * cosine + first * sine], axis=-1
    )
    return turned.reshape(row_count, -1)


def attend(query, keys, values, positions):
    block_rows, query_width = query.shape
    everywhere = keys.shape[0]
    shared_heads = keys.shape[1] // HD
    query_heads = query.reshape(block_rows, shared_heads, -1, HD)
    key_heads = keys.reshape(everywhere, shared_heads, HD)
    value_heads = values.reshape(everywhere, shared_heads, HD)
    scores = jnp.einsum("qkgd,skd->kgqs", query_heads, key_heads, preferred_element_type=F32)
    scores = scores * HD ** (-0.5)
    allowed = jnp.arange(everywhere, dtype=jnp.int32)[None, :] <= positions[:, None]
    scores = jnp.where(allowed, scores, masked)
    top = jnp.max(scores, axis=-1)
    weights = jnp.where(allowed, jnp.exp(scores - top[..., None]), 0.0)
    total = jnp.sum(weights, axis=-1)
    weighted = jnp.einsum(
        "kgqs,skd->kgqd",
        weights,
        value_heads.astype(F32),
        precision=lax.Precision.HIGHEST,
    )
    mean = weighted / total[..., None]
    return mean.transpose(2, 0, 1, 3).reshape(block_rows, query_width).astype(BF16)


def on_device(
    tokens,
    attention_gain,
    query_weight,
    key_weight,
    value_weight,
    out_weight,
    feed_gain,
    gate_weight,
    up_weight,
    down_weight,
):
    local_rows, model = tokens.shape
    block_rows = local_rows * TP
    rows = block_rows * CP
    query_width, key_width = query_weight.shape[1], key_weight.shape[1]

    normed = normalize(tokens, attention_gain)
    slices = normed.reshape(local_rows, CP, -1).transpose(1, 0, 2)
    columns = spread(slices, 0).transpose(1, 0, 2, 3).reshape(rows, -1)
    summed = project(columns, (query_weight, key_weight, value_weight), 640, 1)
    positions = lax.axis_index("cp") * block_rows + jnp.arange(block_rows, dtype=jnp.int32)
    query = rotate(summed[:, :query_width], positions).astype(BF16)
    keys = rotate(summed[:, query_width : query_width + key_width], positions).astype(BF16)
    values = summed[:, query_width + key_width :].astype(BF16)
    shared = gather(jnp.concatenate([keys, values], axis=1), key_width, 2)
    shared = shared.reshape(rows, 2 * key_width)
    attention = attend(query, shared[:, :key_width], shared[:, key_width:], positions)

    everywhere = gather(attention, 640, 3).reshape(rows, -1)
    partial_out = jnp.dot(everywhere, out_weight, preferred_element_type=F32).astype(BF16)
    by_owner = partial_out.reshape(CP, TP, local_rows, -1).transpose(1, 0, 2, 3)
    projected = collect(by_owner, 4).transpose(1, 0, 2).reshape(local_rows, model)
    attended = (tokens.astype(F32) + projected.astype(F32)).astype(BF16)

    normed_feed = normalize(attended, feed_gain)
    by_width = normed_feed.reshape(local_rows, TP, -1).transpose(1, 0, 2)
    block = swap(by_width, 5).reshape(block_rows, -1)
    stream = gather(block, 640, 6).reshape(rows, -1)
    hidden = feed(stream, gate_weight, up_weight, 7).reshape(rows, -1)
    reduced = project(hidden, (down_weight,), 512, 8)
    by_token = reduced.astype(BF16).reshape(TP, local_rows, -1)
    lowered = swap(by_token, 9).transpose(1, 0, 2).reshape(local_rows, model)
    mixed = (attended.astype(F32) + lowered.astype(F32)).astype(BF16)
    return attended, mixed


def solution(mesh):
    in_specs = (
        P(("cp", "tp"), None),
        P(),
        P("cp", "tp"),
        P("cp", "tp"),
        P("cp", "tp"),
        P("tp", "cp"),
        P(),
        P("tp", "cp"),
        P("tp", "cp"),
        P("cp", "tp"),
    )
    out_specs = (P(("cp", "tp"), None), P(("cp", "tp"), None))
    return jax.shard_map(
        on_device, mesh=mesh, in_specs=in_specs, out_specs=out_specs, check_vma=False
    )
```

```python
import collections
import functools

import jax
import jax.numpy as jnp
from jax import lax
from jax.experimental import pallas as pl
from jax.experimental.pallas import tpu as pltpu
from jax.sharding import PartitionSpec as P

HD = 128
NZ, NY, NX = 8, 4, 4
CP, TP = NZ * NY, NX * 2
MESH = pl.DeviceIdType.MESH
F32, BF16 = jnp.float32, jnp.bfloat16

epsilon = 1e-05
rope_base = 500000.0
masked = -1e30


class Wires:
    def __init__(self, send, recv):
        self.send, self.recv, self.used, self.sent = send, recv, 0, []

    def copy(self, src, dst, device):
        i = self.used
        self.used += 1
        c = pltpu.make_async_remote_copy(
            src_ref=src,
            dst_ref=dst,
            send_sem=self.send.at[i],
            recv_sem=self.recv.at[i],
            device_id=device,
            device_id_type=MESH,
        )
        c.start()
        self.sent.append(c)
        return c

    def drain(self):
        for c in self.sent:
            c.wait_send()


class Steps:
    def __init__(self):
        self.queue = collections.deque()

    def add(self, gen):
        if next(gen, self) is not self:
            self.queue.append(gen)

    def run(self):
        while self.queue:
            self.add(self.queue.popleft())


class Place:
    def __init__(self):
        self.cp, self.tp = lax.axis_index("cp"), lax.axis_index("tp")
        self.z, self.y = self.cp // NY, self.cp % NY
        self.x, self.core = self.tp // 2, self.tp % 2

    def along_z(self, z):
        return {"cp": z * NY + self.y}

    def along_y(self, y):
        return {"cp": self.z * NY + y}

    def along_x(self, x):
        return {"tp": x * 2 + self.core}

    def partner(self):
        return {"tp": self.x * 2 + 1 - self.core}


def ring(n, me, device_of):
    return device_of((me + 1) % n), device_of((me + n - 1) % n)


def greet(devices):
    barrier = pltpu.get_barrier_semaphore()
    for device in devices:
        pl.semaphore_signal(barrier, inc=1, device_id=device, device_id_type=MESH)
    return len(devices)


def greet_group(axis, n, me):
    barrier = pltpu.get_barrier_semaphore()

    def signal(off, carry):
        pl.semaphore_signal(
            barrier, inc=1, device_id={axis: (me + off) % n}, device_id_type=MESH
        )
        return carry

    lax.fori_loop(1, n, signal, 0)
    return n - 1


def await_greetings(count):
    pl.semaphore_wait(pltpu.get_barrier_semaphore(), count)


def half_of(ref, h):
    d = ref.shape[0] // 2
    return ref.at[pl.ds(h * d, d)]


def ring_gather(wires, block, n, me, device_of, arrived=None):
    right, left = ring(n, me, device_of)
    last = n // 2 - 1

    def send(k):
        r, l = block((me + n - k) % n), block((me + k) % n)
        if k == last:
            r, l = half_of(r, 0), half_of(l, 1)
        return wires.copy(r, r, right), wires.copy(l, l, left)

    flying = send(0)
    if arrived:
        arrived(me)
    for k in range(1, n // 2 + 1):
        yield
        for c in flying:
            c.wait_recv()
        if k <= last:
            flying = send(k)
            if arrived:
                arrived((me + n - k) % n)
                arrived((me + k) % n)
        elif arrived:
            arrived((me + n // 2) % n)


def add_rows(dst, terms, finish=None):
    if len(dst.shape) == 3:
        for i in range(dst.shape[0]):
            add_rows(dst.at[i], [t.at[i] for t in terms])
        return
    rows = dst.shape[0]
    step = min(rows, 16)

    def body(i, carry):
        at = pl.ds(pl.multiple_of(i * step, step), step)
        total = terms[0][at, :].astype(F32)
        for t in terms[1:]:
            total = total + t[at, :].astype(F32)
        dst[at, :] = total.astype(dst.dtype)
        return carry

    lax.fori_loop(0, rows // step, body, 0)


def ring_scatter(wires, own, out, from_left, from_right, n, me, device_of):
    right, left = ring(n, me, device_of)
    m = n // 2
    far = own((me + m) % n)
    r = wires.copy(half_of(far, 0), half_of(from_left.at[0], 0), right)
    l = wires.copy(half_of(far, 1), half_of(from_right.at[0], 1), left)
    for k in range(1, m):
        yield
        to_right, to_left = own((me + m - k) % n), own((me + n - m + k) % n)
        got_left, got_right = from_left.at[k - 1], from_right.at[k - 1]
        r.wait_recv()
        if k == 1:
            add_rows(half_of(got_left, 0), [half_of(got_left, 0), half_of(to_right, 0)])
            add_rows(half_of(got_left, 1), [half_of(to_right, 1)])
        else:
            add_rows(got_left, [got_left, to_right])
        r = wires.copy(got_left, from_left.at[k], right)
        l.wait_recv()
        if k == 1:
            add_rows(half_of(got_right, 1), [half_of(got_right, 1), half_of(to_left, 1)])
            add_rows(half_of(got_right, 0), [half_of(to_left, 0)])
        else:
            add_rows(got_right, [got_right, to_left])
        l = wires.copy(got_right, from_right.at[k], left)
    yield
    r.wait_recv()
    l.wait_recv()
    add_rows(out, [own(me), from_left.at[m - 1], from_right.at[m - 1]])


def far_gather(wires, block, n, me, device_of, arrived):
    def to(off):
        return device_of((me + n + off) % n)

    def whole(off):
        return block((me + n + off) % n)

    def send(ref, off):
        return wires.copy(ref, ref, to(off))

    own = block(me)
    p2, m2, p1, m1 = send(own, 2), send(own, -2), send(own, 1), send(own, -1)
    arrived(me)
    yield
    p2.wait_recv()
    p3, p4 = send(whole(-2), 1), send(half_of(whole(-2), 0), 2)
    m2.wait_recv()
    m3, m4 = send(whole(2), -1), send(half_of(whole(2), 1), -2)
    p1.wait_recv()
    arrived((me + n - 1) % n)
    m1.wait_recv()
    arrived((me + 1) % n)
    arrived((me + n - 2) % n)
    arrived((me + 2) % n)
    yield
    p3.wait_recv()
    arrived((me + n - 3) % n)
    m3.wait_recv()
    arrived((me + 3) % n)
    p4.wait_recv()
    m4.wait_recv()
    arrived((me + 4) % n)


def far_scatter(wires, own, out, bufs, n, me, device_of):
    near_l, near_r, turn_l, turn_r, far_l, far_r, sum_l, sum_r = [bufs.at[i] for i in range(8)]

    def to(off):
        return device_of((me + n + off) % n)

    def term(off):
        return own((me + n + off) % n)

    opposite = term(4)
    f_l = wires.copy(half_of(opposite, 0), half_of(far_l, 0), to(2))
    f_r = wires.copy(half_of(opposite, 1), half_of(far_r, 1), to(-2))
    t_l = wires.copy(term(3), turn_l, to(1))
    t_r = wires.copy(term(-3), turn_r, to(-1))
    n_l = wires.copy(term(1), near_l, to(1))
    n_r = wires.copy(term(-1), near_r, to(-1))
    yield
    t_l.wait_recv()
    f_l.wait_recv()
    mine = term(2)
    add_rows(half_of(turn_l, 0), [half_of(r, 0) for r in (turn_l, far_l, mine)])
    add_rows(half_of(turn_l, 1), [half_of(r, 1) for r in (turn_l, mine)])
    s_l = wires.copy(turn_l, sum_l, to(2))
    t_r.wait_recv()
    f_r.wait_recv()
    mine = term(-2)
    add_rows(half_of(turn_r, 1), [half_of(r, 1) for r in (turn_r, far_r, mine)])
    add_rows(half_of(turn_r, 0), [half_of(r, 0) for r in (turn_r, mine)])
    s_r = wires.copy(turn_r, sum_r, to(-2))
    yield
    for c in (n_l, n_r, s_l, s_r):
        c.wait_recv()
    add_rows(out, [own(me), near_l, near_r, sum_l, sum_r])


def exchange(send_sem, recv_sem, source, target, axis, n, me, meanwhile=None):
    def copy(off):
        peer = (me + off) % n
        return pltpu.make_async_remote_copy(
            src_ref=source(peer),
            dst_ref=target(me),
            send_sem=send_sem.at[off],
            recv_sem=recv_sem.at[off],
            device_id={axis: peer},
            device_id_type=MESH,
        )

    def start(off, carry):
        copy(off).start()
        return carry

    def wait(off, carry):
        copy(off).wait()
        return carry

    lax.fori_loop(1, n, start, 0)
    if meanwhile:
        meanwhile()
    lax.fori_loop(1, n, wait, 0)


UNITS = 2
Z_FIRST, Y_FIRST = "z", "y"
QKV_PARTS = ((0, 256, Y_FIRST), (256, 256, Y_FIRST), (512, 384, Y_FIRST), (896, 384, Z_FIRST))
DOWN_PARTS = ((0, 384, Y_FIRST), (384, 384, Y_FIRST), (768, 256, Z_FIRST))
GATHER_SPLIT = 768


def gather_rows(wires, steps, at, out_ref, split):
    first, rest = pl.ds(0, split), pl.ds(split, out_ref.shape[-1] - split)

    def y_first():
        yield from ring_gather(
            wires, lambda j: out_ref.at[at.z, j, :, rest], NY, at.y, at.along_y
        )
        yield from far_gather(
            wires, lambda i: out_ref.at[i, :, :, rest], NZ, at.z, at.along_z, lambda i: None
        )

    def to_y(i):
        steps.add(
            ring_gather(wires, lambda j: out_ref.at[i, j, :, first], NY, at.y, at.along_y)
        )

    steps.add(y_first())
    steps.add(
        far_gather(
            wires, lambda i: out_ref.at[i, at.y, :, first], NZ, at.z, at.along_z, to_y
        )
    )


def gather_small(wires, at, ref):
    handed = []

    def to_y(i):
        block = ref.at[i, at.y]
        for off in (1, 3, 2):
            handed.append(wires.copy(block, block, at.along_y((at.y + off) % NY)))

    own = ref.at[at.z, at.y]
    order = (4, 3, 5, 2, 6, 1, 7)
    copies = {off: wires.copy(own, own, at.along_z((at.z + off) % NZ)) for off in order}
    to_y(at.z)
    yield
    for off in (1, 7, 2, 6, 3, 5, 4):
        copies[off].wait_recv()
        to_y((at.z + NZ - off) % NZ)
    yield
    for c in handed:
        c.wait_recv()


def scatter_part(wires, at, part, out, columns, way, bufs):
    if way == Z_FIRST:
        z_bufs, y_left, y_right, y_sum = bufs
        yield from far_scatter(
            wires, lambda i: part.at[i, :, :, columns], y_sum, z_bufs, NZ, at.z, at.along_z
        )
        yield from ring_scatter(
            wires,
            lambda j: y_sum.at[j],
            out.at[:, columns],
            y_left,
            y_right,
            NY,
            at.y,
            at.along_y,
        )
    else:
        z_bufs, y_left, y_right, z_sum = bufs
        yield from ring_scatter(
            wires,
            lambda j: part.at[:, j, :, columns],
            z_sum,
            y_left,
            y_right,
            NY,
            at.y,
            at.along_y,
        )
        yield from far_scatter(
            wires, lambda i: z_sum.at[i], out.at[:, columns], z_bufs, NZ, at.z, at.along_z
        )


def scatter_scratch(prefix, parts, rows):
    scratch = {}
    for n, (_, width, way) in enumerate(parts):
        if way == Z_FIRST:
            shapes = (
                (NZ, NY, rows, width),
                (NY // 2, rows, width),
                (NY // 2, rows, width),
                (NY, rows, width),
            )
        else:
            shapes = (
                (NZ, rows, width),
                (NY // 2, NZ, rows, width),
                (NY // 2, NZ, rows, width),
                (NZ, rows, width),
            )
        for m, shape in enumerate(shapes):
            scratch[f"{prefix}{n}{m}"] = pltpu.VMEM(shape, BF16)
    return scratch


def product_into(part, x, w_ref, start):
    width = w_ref.shape[1]
    tile = min(width, 256)

    def body(i, carry):
        at = pl.multiple_of(i * tile, tile)
        p = jnp.dot(x(), w_ref[:, pl.ds(at, tile)], preferred_element_type=F32)
        part[:, :, :, pl.ds(pl.multiple_of(start + at, 128), tile)] = p.astype(BF16).reshape(
            *part.shape[:3], tile
        )
        return carry

    lax.fori_loop(0, width // tile, body, 0)


def feed(wires, steps, at, stream, gate_ref, up_ref, out_ref, part, held, fl, fr, total):
    partner = at.partner()
    units = gate_ref.shape[1]
    block = part.shape[2]
    rows = block // UNITS
    other = 1 - at.core
    zs = NZ // NX

    def product(i):
        def tile(w_ref, col, width, start):
            x = stream[pl.ds(i * zs, zs)].reshape(2 * block, -1)
            p = jnp.dot(x, w_ref[:, pl.ds(col, width)], preferred_element_type=F32)
            part[i, :, :, pl.ds(start + col, width)] = p.astype(BF16).reshape(2, block, width)

        def body(t, carry):
            col = pl.multiple_of(t * 256, 256)
            tile(gate_ref, col, 256, 0)
            tile(up_ref, col, 256, units)
            return carry

        lax.fori_loop(0, units // 256, body, 0)
        if units % 256:
            tile(gate_ref, units // 256 * 256, units % 256, 0)
            tile(up_ref, units // 256 * 256, units % 256, units)
        return wires.copy(part.at[i, other], held.at[i], partner)

    def combine(i, c):
        c.wait_recv()
        add_rows(held.at[i], [held.at[i], part.at[i, at.core]])

    def line(u):
        at_rows = pl.ds(u * rows, rows)
        yield from ring_scatter(
            wires,
            lambda i: held.at[i, at_rows],
            total.at[u],
            fl.at[u],
            fr.at[u],
            NX,
            at.x,
            at.along_x,
        )

        def body(i, carry):
            r = pl.ds(pl.multiple_of(i * 16, 16), 16)
            gate, up = total[u, r, pl.ds(0, units)], total[u, r, pl.ds(units, units)]
            out_ref[at.x, at.core, pl.ds(pl.multiple_of(u * rows + i * 16, 16), 16), :] = (
                jax.nn.silu(gate) * up
            ).astype(BF16)
            return carry

        lax.fori_loop(0, rows // 16, body, 0)

        def hand_over(i):
            ref = out_ref.at[i, at.core, at_rows]
            handed.append(wires.copy(ref, ref, partner))

        yield from ring_gather(
            wires, lambda i: out_ref.at[i, at.core, at_rows], NX, at.x, at.along_x, hand_over
        )

    handed = []
    order = [(at.x + 2) % NX, (at.x + 1) % NX, (at.x + 3) % NX, at.x]
    copies = [product(order[0])]
    copies.append(product(order[1]))
    combine(order[0], copies[0])
    for u in range(UNITS):
        steps.add(line(u))
    copies.append(product(order[2]))
    combine(order[1], copies[1])
    copies.append(product(order[3]))
    combine(order[2], copies[2])
    combine(order[3], copies[3])
    steps.run()
    for c in handed:
        c.wait_recv()


def normalize(values, gain):
    mean_square = jnp.mean(values * values, axis=-1, keepdims=True)
    return (values * lax.rsqrt(mean_square + epsilon) * gain).astype(BF16)


WEIGHTS = ("key", "value", "query", "out", "gate", "up", "down")


def layer_kernel(names, *refs):
    r = dict(zip(names, refs))
    at = Place()
    wires, steps = Wires(r["send"], r["recv"]), Steps()
    tokens, attended, mixed = r["tokens"], r["attended"], r["mixed"]
    local_rows, model = tokens.shape
    cos, sin = r["cos"], r["sin"]

    greeted = greet_group("cp", CP, at.cp) + greet_group("tp", TP, at.tp)
    loads = {}
    for n, name in enumerate(WEIGHTS):
        loads[name] = pltpu.make_async_copy(
            r[name + "_weight"], r[name], r["load"].at[n]
        )
        loads[name].start()

    normed = normalize(tokens[...].astype(F32), r["attention_gain"][...])
    slices, got, columns = r["slices"], r["got"], r["columns"]
    width = slices.shape[-1]
    for c in range(CP):
        slices[c] = normed[:, c * width : (c + 1) * width]
    await_greetings(greeted)

    def keep_slice():
        got[at.cp] = slices[at.cp]

    exchange(
        r["s0"], r["r0"], lambda p: slices.at[p], lambda p: got.at[p], "cp", CP, at.cp, keep_slice
    )

    def keep_columns():
        columns[at.tp] = got[...]

    exchange(
        r["s1"], r["r1"], lambda p: got, lambda p: columns.at[p], "tp", TP, at.tp, keep_columns
    )
    rows_in = r["rows_in"]

    def in_order(b, carry):
        parts = [columns[t, b].astype(F32) for t in range(TP)]
        rows_in[b] = jnp.concatenate(parts, axis=0).astype(BF16)
        return carry

    lax.fori_loop(0, CP, in_order, 0)

    part, summed, shared = r["qkv_part"], r["summed"], r["shared"]

    def x():
        return rows_in[...].reshape(-1, width)

    def turned(v):
        return (v * cos[...] + pltpu.roll(v, HD // 2, 1) * sin[...]).astype(BF16)

    def unit(n, out, parts, partial, prefix):
        start, extent, way = parts[n]
        bufs = [r[f"{prefix}{n}{m}"] for m in range(4)]
        return scatter_part(wires, at, partial, out, pl.ds(start, extent), way, bufs)

    def keys_and_values():
        yield from unit(0, summed, QKV_PARTS, part, "q")
        shared[at.z, at.y, :, pl.ds(0, HD)] = turned(summed[:, pl.ds(0, HD)])
        shared[at.z, at.y, :, pl.ds(HD, HD)] = summed[:, pl.ds(HD, HD)].astype(BF16)
        yield from gather_small(wires, at, shared)

    loads["key"].wait()
    loads["value"].wait()
    product_into(part, x, r["key"], 0)
    product_into(part, x, r["value"], HD)
    steps.add(keys_and_values())
    loads["query"].wait()
    product_into(part, x, r["query"], 2 * HD)
    for n in range(1, len(QKV_PARTS)):
        steps.add(unit(n, summed, QKV_PARTS, part, "q"))
    steps.run()

    every = r["every"]
    heads = (summed.shape[1] - 2 * HD) // HD
    block = summed.shape[0]
    query = jnp.concatenate(
        [turned(summed[:, (2 + h) * HD : (3 + h) * HD]) for h in range(heads)], axis=0
    )
    keys = shared[:, :, :, 0:HD].reshape(-1, HD)
    values = shared[:, :, :, HD : 2 * HD].reshape(-1, HD)
    scores = lax.dot_general(
        query, keys, (((1,), (1,)), ((), ())), preferred_element_type=F32
    ) * HD ** (-0.5)
    key_at = lax.broadcasted_iota(jnp.int32, scores.shape, 1)
    query_at = lax.broadcasted_iota(jnp.int32, scores.shape, 0) % block + at.cp * block
    allowed = key_at <= query_at
    scores = jnp.where(allowed, scores, masked)
    top = jnp.max(scores, axis=-1, keepdims=True)
    weights = jnp.where(allowed, jnp.exp(scores - top), 0.0)
    total = jnp.sum(weights, axis=-1, keepdims=True)
    mean = jnp.dot(weights.astype(BF16), values, preferred_element_type=F32) / total
    mean = mean.astype(BF16)
    for h in range(heads):
        every[at.z, at.y, :, h * HD : (h + 1) * HD] = mean[h * block : (h + 1) * block]

    gather_rows(wires, steps, at, every, GATHER_SPLIT)
    steps.run()

    out_part, out_got, out_total, projected = (
        r["out_part"],
        r["out_got"],
        r["out_total"],
        r["projected"],
    )
    loads["out"].wait()

    def out_rows(i, carry):
        p = jnp.dot(
            every[pl.ds(i * 2, 2)].reshape(2 * NY * block, -1),
            r["out"][...],
            preferred_element_type=F32,
        )
        for b in range(2 * NY):
            for t in range(TP):
                first = b * block + t * local_rows
                out_part[t, i * 2 * NY + b] = p[first : first + local_rows].astype(BF16)
        return carry

    lax.fori_loop(0, NZ // 2, out_rows, 0)

    def keep_part():
        out_got[at.tp] = out_part[at.tp]

    exchange(
        r["s2"],
        r["r2"],
        lambda p: out_part.at[p],
        lambda p: out_got.at[p],
        "tp",
        TP,
        at.tp,
        keep_part,
    )

    def sum_part(i, carry):
        parts = out_got[0, i].astype(F32)
        for t in range(1, TP):
            parts = parts + out_got[t, i].astype(F32)
        out_total[i] = parts.astype(BF16)
        return carry

    lax.fori_loop(0, CP, sum_part, 0)

    def keep_total():
        projected[at.cp] = out_total[at.cp]

    exchange(
        r["s3"],
        r["r3"],
        lambda p: out_total.at[p],
        lambda p: projected.at[p],
        "cp",
        CP,
        at.cp,
        keep_total,
    )
    for c in range(CP):
        cols = slice(c * width, (c + 1) * width)
        attended[:, cols] = (tokens[:, cols].astype(F32) + projected[c].astype(F32)).astype(BF16)

    normed = normalize(attended[...].astype(F32), r["feed_gain"][...])
    by_width, got_width, stream = r["by_width"], r["got_width"], r["stream"]
    wide = by_width.shape[-1]
    for t in range(TP):
        by_width[t] = normed[:, t * wide : (t + 1) * wide]

    def keep_width():
        got_width[at.tp] = by_width[at.tp]

    exchange(
        r["s4"],
        r["r4"],
        lambda p: by_width.at[p],
        lambda p: got_width.at[p],
        "tp",
        TP,
        at.tp,
        keep_width,
    )
    stream[at.z, at.y] = jnp.concatenate(
        [got_width[t].astype(F32) for t in range(TP)], axis=0
    ).astype(BF16)
    gather_rows(wires, steps, at, stream, GATHER_SPLIT)
    steps.run()

    loads["gate"].wait()
    loads["up"].wait()
    hidden = r["hidden"]
    feed(
        wires,
        steps,
        at,
        stream,
        r["gate"],
        r["up"],
        hidden,
        r["unit_part"],
        r["held"],
        r["from_left"],
        r["from_right"],
        r["unit_total"],
    )

    down_part, reduced = r["down_part"], r["reduced"]
    loads["down"].wait()
    product_into(down_part, lambda: hidden[...].reshape(-1, hidden.shape[-1]), r["down"], 0)
    for n in range(len(DOWN_PARTS)):
        steps.add(unit(n, reduced, DOWN_PARTS, down_part, "d"))
    steps.run()
    by_token, lowered = r["by_token"], r["lowered"]
    for t in range(TP):
        by_token[t] = reduced[pl.ds(t * local_rows, local_rows), :].astype(BF16)

    def keep_token():
        lowered[at.tp] = by_token[at.tp]

    exchange(
        r["s5"],
        r["r5"],
        lambda p: by_token.at[p],
        lambda p: lowered.at[p],
        "tp",
        TP,
        at.tp,
        keep_token,
    )
    for t in range(TP):
        cols = slice(t * wide, (t + 1) * wide)
        mixed[:, cols] = (attended[:, cols].astype(F32) + lowered[t].astype(F32)).astype(BF16)
    wires.drain()


VMEM = pl.BlockSpec(memory_space=pltpu.VMEM)
ANY = pl.BlockSpec(memory_space=pl.ANY)
COPIES = 320


def dma(count):
    return pltpu.SemaphoreType.DMA((count,))


def on_device(
    tokens,
    attention_gain,
    query_weight,
    key_weight,
    value_weight,
    out_weight,
    feed_gain,
    gate_weight,
    up_weight,
    down_weight,
):
    local_rows, model = tokens.shape
    block = local_rows * TP
    rows = block * CP
    qkv = query_weight.shape[1] + key_weight.shape[1] + value_weight.shape[1]
    units = gate_weight.shape[1]
    wide, width = model // TP, model // CP

    inverse = rope_base ** (-(jnp.arange(HD // 2, dtype=F32) * 2.0 / HD))
    positions = lax.axis_index("cp") * block + jnp.arange(block, dtype=jnp.int32)
    angles = positions.astype(F32)[:, None] * inverse[None, :]
    cosine, sine = jnp.cos(angles), jnp.sin(angles)

    inputs = {
        "tokens": tokens,
        "attention_gain": attention_gain[None],
        "feed_gain": feed_gain[None],
        "cos": jnp.concatenate([cosine, cosine], axis=1),
        "sin": jnp.concatenate([-sine, sine], axis=1),
        "key_weight": key_weight,
        "value_weight": value_weight,
        "query_weight": query_weight,
        "out_weight": out_weight,
        "gate_weight": gate_weight,
        "up_weight": up_weight,
        "down_weight": down_weight,
    }

    def buf(*shape, kind=BF16):
        return pltpu.VMEM(shape, kind)

    scratch = {name: buf(*inputs[name + "_weight"].shape) for name in WEIGHTS}
    scratch |= {
        "slices": buf(CP, local_rows, width),
        "got": buf(CP, local_rows, width),
        "columns": buf(TP, CP, local_rows, width),
        "rows_in": buf(CP, block, width),
        "qkv_part": buf(NZ, NY, block, qkv),
        "summed": buf(block, qkv, kind=F32),
        "shared": buf(NZ, NY, block, 2 * HD),
        "every": buf(NZ, NY, block, wide),
        "out_part": buf(TP, CP, local_rows, width),
        "out_got": buf(TP, CP, local_rows, width),
        "out_total": buf(CP, local_rows, width),
        "projected": buf(CP, local_rows, width),
        "by_width": buf(TP, local_rows, wide),
        "got_width": buf(TP, local_rows, wide),
        "stream": buf(NZ, NY, block, wide),
        "unit_part": buf(NX, 2, rows // TP, 2 * units),
        "held": buf(NX, rows // TP, 2 * units),
        "from_left": buf(UNITS, NX // 2, rows // TP // UNITS, 2 * units),
        "from_right": buf(UNITS, NX // 2, rows // TP // UNITS, 2 * units),
        "unit_total": buf(UNITS, rows // TP // UNITS, 2 * units, kind=F32),
        "hidden": buf(NX, 2, rows // TP, units),
        "down_part": buf(NZ, NY, block, wide),
        "reduced": buf(block, wide, kind=F32),
        "by_token": buf(TP, local_rows, wide),
        "lowered": buf(TP, local_rows, wide),
    }
    scratch |= scatter_scratch("q", QKV_PARTS, block)
    scratch |= scatter_scratch("d", DOWN_PARTS, block)
    for n, count in enumerate((CP, TP, TP, CP, TP, TP)):
        scratch |= {f"s{n}": dma(count), f"r{n}": dma(count)}
    scratch |= {"load": dma(len(WEIGHTS)), "send": dma(COPIES), "recv": dma(COPIES)}

    names = (*inputs, "attended", "mixed", *scratch)
    shape = jax.ShapeDtypeStruct(tokens.shape, BF16)
    return pl.pallas_call(
        functools.partial(layer_kernel, names),
        out_shape=(shape, shape),
        in_specs=[ANY if name.endswith("_weight") else VMEM for name in inputs],
        out_specs=(VMEM, VMEM),
        scratch_shapes=list(scratch.values()),
        compiler_params=pltpu.CompilerParams(
            collective_id=0,
            has_side_effects=True,
            vmem_limit_bytes=60 * 1024 * 1024,
        ),
        name="layer",
    )(*inputs.values())


def solution(mesh):
    in_specs = (
        P(("cp", "tp"), None),
        P(),
        P("cp", "tp"),
        P("cp", "tp"),
        P("cp", "tp"),
        P("tp", "cp"),
        P(),
        P("tp", "cp"),
        P("tp", "cp"),
        P("cp", "tp"),
    )
    out_specs = (P(("cp", "tp"), None), P(("cp", "tp"), None))
    return jax.shard_map(
        on_device, mesh=mesh, in_specs=in_specs, out_specs=out_specs, check_vma=False
    )
```

```python
import collections
import functools

import jax
import jax.numpy as jnp
from jax import lax
from jax.experimental import pallas as pl
from jax.experimental.pallas import tpu as pltpu
from jax.sharding import PartitionSpec as P

HD = 128
NZ, NY, NX = 8, 4, 4
CP, TP = NZ * NY, NX * 2
MESH = pl.DeviceIdType.MESH
F32, BF16 = jnp.float32, jnp.bfloat16

epsilon = 1e-05
rope_base = 500000.0
masked = -1e30


class Wires:
    def __init__(self, send, recv):
        self.send, self.recv, self.used, self.sent = send, recv, 0, []

    def copy(self, src, dst, device):
        i = self.used
        self.used += 1
        assert i < self.send.shape[0]
        c = pltpu.make_async_remote_copy(
            src_ref=src,
            dst_ref=dst,
            send_sem=self.send.at[i],
            recv_sem=self.recv.at[i],
            device_id=device,
            device_id_type=MESH,
        )
        c.start()
        self.sent.append(c)
        return c

    def drain(self):
        for c in self.sent:
            c.wait_send()
        self.sent, self.used = [], 0


class Steps:
    def __init__(self):
        self.queue = collections.deque()

    def add(self, gen, name="line", step=0):
        with jax.named_scope(f"{name}_{step}"):
            going = next(gen, self) is not self
        if going:
            self.queue.append((gen, name, step + 1))

    def run(self):
        while self.queue:
            self.add(*self.queue.popleft())


class Phases:
    def __init__(self):
        self.scope = None

    def __call__(self, name):
        if self.scope:
            self.scope.__exit__(None, None, None)
        self.scope = jax.named_scope(name) if name else None
        if self.scope:
            self.scope.__enter__()


class Place:
    def __init__(self):
        self.cp, self.tp = lax.axis_index("cp"), lax.axis_index("tp")
        self.z, self.y = self.cp // NY, self.cp % NY
        self.x, self.core = self.tp // 2, self.tp % 2

    def along_z(self, z):
        return {"cp": z * NY + self.y}

    def along_y(self, y):
        return {"cp": self.z * NY + y}

    def along_x(self, x):
        return {"tp": x * 2 + self.core}

    def partner(self):
        return {"tp": self.x * 2 + 1 - self.core}


def ring(n, me, device_of):
    return device_of((me + 1) % n), device_of((me + n - 1) % n)


def greet(devices):
    barrier = pltpu.get_barrier_semaphore()
    for device in devices:
        pl.semaphore_signal(barrier, inc=1, device_id=device, device_id_type=MESH)
    return len(devices)


def greet_group(axis, n, me):
    barrier = pltpu.get_barrier_semaphore()

    def signal(off, carry):
        pl.semaphore_signal(
            barrier, inc=1, device_id={axis: (me + off) % n}, device_id_type=MESH
        )
        return carry

    lax.fori_loop(1, n, signal, 0)
    return n - 1


def await_greetings(count):
    pl.semaphore_wait(pltpu.get_barrier_semaphore(), count)


def half_of(ref, h):
    d = ref.shape[0] // 2
    return ref.at[pl.ds(h * d, d)]


def ring_gather(wires, block, n, me, device_of, arrived=None):
    right, left = ring(n, me, device_of)
    last = n // 2 - 1

    def send(k):
        r, l = block((me + n - k) % n), block((me + k) % n)
        if k == last:
            r, l = half_of(r, 0), half_of(l, 1)
        return wires.copy(r, r, right), wires.copy(l, l, left)

    flying = send(0)
    if arrived:
        arrived(me)
    for k in range(1, n // 2 + 1):
        yield
        for c in flying:
            c.wait_recv()
        if k <= last:
            flying = send(k)
            if arrived:
                arrived((me + n - k) % n)
                arrived((me + k) % n)
        elif arrived:
            arrived((me + n // 2) % n)


def add_rows(dst, terms, finish=None):
    if len(dst.shape) == 3:
        for i in range(dst.shape[0]):
            add_rows(dst.at[i], [t.at[i] for t in terms])
        return
    rows = dst.shape[0]
    step = min(rows, 16)

    def body(i, carry):
        at = pl.ds(pl.multiple_of(i * step, step), step)
        total = terms[0][at, :].astype(F32)
        for t in terms[1:]:
            total = total + t[at, :].astype(F32)
        dst[at, :] = total.astype(dst.dtype)
        return carry

    lax.fori_loop(0, rows // step, body, 0)


def ring_scatter(wires, own, out, from_left, from_right, n, me, device_of):
    right, left = ring(n, me, device_of)
    m = n // 2
    far = own((me + m) % n)
    r = wires.copy(half_of(far, 0), half_of(from_left.at[0], 0), right)
    l = wires.copy(half_of(far, 1), half_of(from_right.at[0], 1), left)
    for k in range(1, m):
        yield
        to_right, to_left = own((me + m - k) % n), own((me + n - m + k) % n)
        got_left, got_right = from_left.at[k - 1], from_right.at[k - 1]
        r.wait_recv()
        if k == 1:
            add_rows(half_of(got_left, 0), [half_of(got_left, 0), half_of(to_right, 0)])
            add_rows(half_of(got_left, 1), [half_of(to_right, 1)])
        else:
            add_rows(got_left, [got_left, to_right])
        r = wires.copy(got_left, from_left.at[k], right)
        l.wait_recv()
        if k == 1:
            add_rows(half_of(got_right, 1), [half_of(got_right, 1), half_of(to_left, 1)])
            add_rows(half_of(got_right, 0), [half_of(to_left, 0)])
        else:
            add_rows(got_right, [got_right, to_left])
        l = wires.copy(got_right, from_right.at[k], left)
    yield
    r.wait_recv()
    l.wait_recv()
    add_rows(out, [own(me), from_left.at[m - 1], from_right.at[m - 1]])


def far_gather(wires, block, n, me, device_of, arrived):
    def to(off):
        return device_of((me + n + off) % n)

    def whole(off):
        return block((me + n + off) % n)

    def send(ref, off):
        return wires.copy(ref, ref, to(off))

    own = block(me)
    p2, m2, p1, m1 = send(own, 2), send(own, -2), send(own, 1), send(own, -1)
    arrived(0)
    yield
    p2.wait_recv()
    p3, p4 = send(whole(-2), 1), send(half_of(whole(-2), 0), 2)
    m2.wait_recv()
    m3, m4 = send(whole(2), -1), send(half_of(whole(2), 1), -2)
    p1.wait_recv()
    arrived(7)
    m1.wait_recv()
    arrived(1)
    arrived(6)
    arrived(2)
    yield
    p3.wait_recv()
    arrived(5)
    m3.wait_recv()
    arrived(3)
    p4.wait_recv()
    m4.wait_recv()
    arrived(4)


def far_scatter(wires, own, out, bufs, n, me, device_of):
    near_l, near_r, turn_l, turn_r, far_l, far_r, sum_l, sum_r = [bufs.at[i] for i in range(8)]

    def to(off):
        return device_of((me + n + off) % n)

    def term(off):
        return own((me + n + off) % n)

    opposite = term(4)
    f_l = wires.copy(half_of(opposite, 0), half_of(far_l, 0), to(2))
    f_r = wires.copy(half_of(opposite, 1), half_of(far_r, 1), to(-2))
    t_l = wires.copy(term(3), turn_l, to(1))
    t_r = wires.copy(term(-3), turn_r, to(-1))
    n_l = wires.copy(term(1), near_l, to(1))
    n_r = wires.copy(term(-1), near_r, to(-1))
    yield
    t_l.wait_recv()
    f_l.wait_recv()
    mine = term(2)
    add_rows(half_of(turn_l, 0), [half_of(r, 0) for r in (turn_l, far_l, mine)])
    add_rows(half_of(turn_l, 1), [half_of(r, 1) for r in (turn_l, mine)])
    s_l = wires.copy(turn_l, sum_l, to(2))
    t_r.wait_recv()
    f_r.wait_recv()
    mine = term(-2)
    add_rows(half_of(turn_r, 1), [half_of(r, 1) for r in (turn_r, far_r, mine)])
    add_rows(half_of(turn_r, 0), [half_of(r, 0) for r in (turn_r, mine)])
    s_r = wires.copy(turn_r, sum_r, to(-2))
    yield
    for c in (n_l, n_r, s_l, s_r):
        c.wait_recv()
    add_rows(out, [own(me), near_l, near_r, sum_l, sum_r])


def exchange(send_sem, recv_sem, source, target, axis, n, me, meanwhile=None):
    def copy(off):
        peer = (me + off) % n
        return pltpu.make_async_remote_copy(
            src_ref=source(peer),
            dst_ref=target(me),
            send_sem=send_sem.at[off],
            recv_sem=recv_sem.at[off],
            device_id={axis: peer},
            device_id_type=MESH,
        )

    def start(off, carry):
        copy(off).start()
        return carry

    def wait(off, carry):
        copy(off).wait()
        return carry

    lax.fori_loop(1, n, start, 0)
    if meanwhile:
        meanwhile()
    lax.fori_loop(1, n, wait, 0)


Z_FIRST, Y_FIRST = "z", "y"
QKV_PARTS = ((0, 256, Y_FIRST), (256, 256, Y_FIRST), (512, 384, Y_FIRST), (896, 384, Z_FIRST))
GATHER_SPLIT = 768


CHUNKS = ((0, 7), (1, 6), (2, 5), (3, 4))


def gather_rows(wires, steps, at, out_ref, split, ready):
    first, rest = pl.ds(0, split), pl.ds(split, out_ref.shape[-1] - split)
    seen = collections.Counter()

    def z_at(off):
        return (at.z + off) % NZ

    def mark(off):
        seen[off] += 1
        for c, chunk in enumerate(CHUNKS):
            if off in chunk and all(seen[o] == 2 for o in chunk):
                steps.add(ready(c), f"chunk{c}")

    def y_first():
        yield from ring_gather(
            wires, lambda j: out_ref.at[at.z, j, :, rest], NY, at.y, at.along_y
        )
        yield from far_gather(
            wires, lambda i: out_ref.at[i, :, :, rest], NZ, at.z, at.along_z, mark
        )

    def to_y(off):
        def line():
            yield from ring_gather(
                wires, lambda j: out_ref.at[z_at(off), j, :, first], NY, at.y, at.along_y
            )
            mark(off)

        steps.add(line(), f"y{off}")

    steps.add(y_first(), "yz")
    steps.add(
        far_gather(
            wires, lambda i: out_ref.at[i, at.y, :, first], NZ, at.z, at.along_z, to_y
        ),
        "z",
    )


def gather_small(wires, at, ref):
    handed = []

    def to_y(i):
        block = ref.at[i, at.y]
        for off in (1, 3, 2):
            handed.append(wires.copy(block, block, at.along_y((at.y + off) % NY)))

    own = ref.at[at.z, at.y]
    order = (4, 3, 5, 2, 6, 1, 7)
    copies = {off: wires.copy(own, own, at.along_z((at.z + off) % NZ)) for off in order}
    to_y(at.z)
    yield
    for off in (1, 7, 2, 6, 3, 5, 4):
        copies[off].wait_recv()
        to_y((at.z + NZ - off) % NZ)
    yield
    for c in handed:
        c.wait_recv()


def scatter_part(wires, at, part, out, columns, way, bufs):
    if way == Z_FIRST:
        z_bufs, y_left, y_right, y_sum = bufs
        yield from far_scatter(
            wires, lambda i: part.at[i, :, :, columns], y_sum, z_bufs, NZ, at.z, at.along_z
        )
        yield from ring_scatter(
            wires,
            lambda j: y_sum.at[j],
            out.at[:, columns],
            y_left,
            y_right,
            NY,
            at.y,
            at.along_y,
        )
    else:
        z_bufs, y_left, y_right, z_sum = bufs
        yield from ring_scatter(
            wires,
            lambda j: part.at[:, j, :, columns],
            z_sum,
            y_left,
            y_right,
            NY,
            at.y,
            at.along_y,
        )
        yield from far_scatter(
            wires, lambda i: z_sum.at[i], out.at[:, columns], z_bufs, NZ, at.z, at.along_z
        )


def scatter_scratch(prefix, parts, rows):
    scratch = {}
    for n, (_, width, way) in enumerate(parts):
        if way == Z_FIRST:
            shapes = (
                (NZ, NY, rows, width),
                (NY // 2, rows, width),
                (NY // 2, rows, width),
                (NY, rows, width),
            )
        else:
            shapes = (
                (NZ, rows, width),
                (NY // 2, NZ, rows, width),
                (NY // 2, NZ, rows, width),
                (NZ, rows, width),
            )
        for m, shape in enumerate(shapes):
            scratch[f"{prefix}{n}{m}"] = pltpu.VMEM(shape, BF16)
    return scratch


def product_into(part, x, w_ref, start):
    width = w_ref.shape[1]
    tile = min(width, 256)

    def body(i, carry):
        at = pl.multiple_of(i * tile, tile)
        p = jnp.dot(x(), w_ref[:, pl.ds(at, tile)], preferred_element_type=F32)
        part[:, :, :, pl.ds(pl.multiple_of(start + at, 128), tile)] = p.astype(BF16).reshape(
            *part.shape[:3], tile
        )
        return carry

    lax.fori_loop(0, width // tile, body, 0)


def chunk_rows(ref, at, c):
    blocks = [ref[(at.z + off) % NZ] for off in CHUNKS[c]]
    return jnp.concatenate([b.reshape(-1, b.shape[-1]) for b in blocks], axis=0)


def feed_chunk(wires, at, r, c, finished):
    partner = at.partner()
    units = r["gate"].shape[1]
    part, held, total, hidden = (
        r["unit_part"].at[c],
        r["held"].at[c],
        r["unit_total"].at[c],
        r["hidden"].at[c],
    )
    rows = total.shape[0]

    def tile(w_ref, col, width, start):
        p = jnp.dot(
            chunk_rows(r["stream"], at, c), w_ref[:, pl.ds(col, width)], preferred_element_type=F32
        )
        part[:, :, :, pl.ds(start + col, width)] = p.astype(BF16).reshape(2, NY, rows, width)

    def body(t, carry):
        col = pl.multiple_of(t * 256, 256)
        tile(r["gate"], col, 256, 0)
        tile(r["up"], col, 256, units)
        return carry

    lax.fori_loop(0, units // 256, body, 0)
    if units % 256:
        tile(r["gate"], units // 256 * 256, units % 256, 0)
        tile(r["up"], units // 256 * 256, units % 256, units)
    copy = wires.copy(part.at[1 - at.core], held, partner)
    yield
    copy.wait_recv()
    add_rows(held, [held, part.at[at.core]])
    yield from ring_scatter(
        wires,
        lambda i: held.at[i],
        total,
        r["from_left"].at[c],
        r["from_right"].at[c],
        NX,
        at.x,
        at.along_x,
    )

    def activate(i, carry):
        here = pl.ds(pl.multiple_of(i * 16, 16), 16)
        gate, up = total[here, pl.ds(0, units)], total[here, pl.ds(units, units)]
        hidden[at.core, at.x, here, :] = (jax.nn.silu(gate) * up).astype(BF16)
        return carry

    lax.fori_loop(0, rows // 16, activate, 0)
    handed = []

    def hand_over(i):
        ref = hidden.at[at.core, i]
        handed.append(wires.copy(ref, ref, partner))

    yield from ring_gather(
        wires, lambda i: hidden.at[at.core, i], NX, at.x, at.along_x, hand_over
    )
    yield
    for copy in handed:
        copy.wait_recv()
    down_part = r["down_part"].at[c]

    def down(i, carry):
        cols = pl.ds(pl.multiple_of(i * 256, 256), 256)
        p = jnp.dot(
            hidden[...].reshape(2 * NX * rows, units), r["down"][:, cols], preferred_element_type=F32
        )
        down_part[:, :, :, cols] = p.astype(BF16).reshape(2, NY, rows, 256)
        return carry

    lax.fori_loop(0, down_part.shape[-1] // 256, down, 0)
    yield from ring_scatter(
        wires,
        lambda j: down_part.at[:, j],
        r["down_sum"].at[c],
        r["down_left"].at[c],
        r["down_right"].at[c],
        NY,
        at.y,
        at.along_y,
    )
    finished(c)


def far_scatter_parts(wires, steps, own, out, bufs, device_of):
    near_l, near_r, turn_l, turn_r, far_l, far_r, sum_l, sum_r = [bufs.at[i] for i in range(8)]
    sent = {}

    def last_round():
        yield
        for side, off, turn, far, into in (
            ("l", 2, turn_l, far_l, sum_l),
            ("r", 6, turn_r, far_r, sum_r),
        ):
            full, other = (0, 1) if side == "l" else (1, 0)
            sent["t" + side].wait_recv()
            sent["f" + side].wait_recv()
            mine = own(off)
            add_rows(half_of(turn, full), [half_of(x, full) for x in (turn, far, mine)])
            add_rows(half_of(turn, other), [half_of(x, other) for x in (turn, mine)])
            sent["s" + side] = wires.copy(turn, into, device_of(off))
        yield
        for name in ("nl", "nr", "sl", "sr"):
            sent[name].wait_recv()
        add_rows(out, [own(0), near_l, near_r, sum_l, sum_r])

    def finished(c):
        for off in CHUNKS[c]:
            term = own(off)
            if off == 1:
                sent["nl"] = wires.copy(term, near_l, device_of(1))
            elif off == 7:
                sent["nr"] = wires.copy(term, near_r, device_of(7))
            elif off == 3:
                sent["tl"] = wires.copy(term, turn_l, device_of(1))
            elif off == 5:
                sent["tr"] = wires.copy(term, turn_r, device_of(7))
            elif off == 4:
                sent["fl"] = wires.copy(half_of(term, 0), half_of(far_l, 0), device_of(2))
                sent["fr"] = wires.copy(half_of(term, 1), half_of(far_r, 1), device_of(6))
        if c == len(CHUNKS) - 1:
            steps.add(last_round(), "last")

    return finished


def normalize(values, gain):
    mean_square = jnp.mean(values * values, axis=-1, keepdims=True)
    return (values * lax.rsqrt(mean_square + epsilon) * gain).astype(BF16)


WEIGHTS = ("key", "value", "query", "out", "gate", "up", "down")


def layer_kernel(names, *refs):
    r = dict(zip(names, refs))
    at = Place()
    qkv_wires, wires, steps = Wires(r["send"], r["recv"]), Wires(r["send_2"], r["recv_2"]), Steps()
    out_wires = wires
    tokens, attended, mixed = r["tokens"], r["attended"], r["mixed"]
    local_rows, model = tokens.shape
    cos, sin = r["cos"], r["sin"]

    phase = Phases()
    phase("greet")
    greeted = greet_group("cp", CP, at.cp) + greet_group("tp", TP, at.tp)
    loads = {}
    for n, name in enumerate(WEIGHTS):
        loads[name] = pltpu.make_async_copy(
            r[name + "_weight"], r[name], r["load"].at[n]
        )
        loads[name].start()

    normed = normalize(tokens[...].astype(F32), r["attention_gain"][...])
    slices, got, columns = r["slices"], r["got"], r["columns"]
    width = slices.shape[-1]
    for c in range(CP):
        slices[c] = normed[:, c * width : (c + 1) * width]
    phase("barrier")
    await_greetings(greeted)

    phase("spread_cp")
    def keep_slice():
        got[at.cp] = slices[at.cp]

    exchange(
        r["s0"], r["r0"], lambda p: slices.at[p], lambda p: got.at[p], "cp", CP, at.cp, keep_slice
    )

    phase("spread_tp")
    def keep_columns():
        columns[at.tp] = got[...]

    exchange(
        r["s1"], r["r1"], lambda p: got, lambda p: columns.at[p], "tp", TP, at.tp, keep_columns
    )
    phase("relayout")
    rows_in = r["rows_in"]

    def in_order(b, carry):
        parts = [columns[t, b].astype(F32) for t in range(TP)]
        rows_in[b] = jnp.concatenate(parts, axis=0).astype(BF16)
        return carry

    lax.fori_loop(0, CP, in_order, 0)

    part, summed, shared = r["qkv_part"], r["summed"], r["shared"]

    def x():
        return rows_in[...].reshape(-1, width)

    def turned(v):
        return (v * cos[...] + pltpu.roll(v, HD // 2, 1) * sin[...]).astype(BF16)

    def unit(n, out, parts, partial, prefix):
        start, extent, way = parts[n]
        bufs = [r[f"{prefix}{n}{m}"] for m in range(4)]
        return scatter_part(qkv_wires, at, partial, out, pl.ds(start, extent), way, bufs)

    def keys_and_values():
        yield from unit(0, summed, QKV_PARTS, part, "q")
        shared[at.z, at.y, :, pl.ds(0, HD)] = turned(summed[:, pl.ds(0, HD)])
        shared[at.z, at.y, :, pl.ds(HD, HD)] = summed[:, pl.ds(HD, HD)].astype(BF16)
        yield from gather_small(qkv_wires, at, shared)

    phase("qkv")
    loads["key"].wait()
    loads["value"].wait()
    product_into(part, x, r["key"], 0)
    product_into(part, x, r["value"], HD)
    steps.add(keys_and_values(), "kv")
    loads["query"].wait()
    product_into(part, x, r["query"], 2 * HD)
    phase("qkv_sum")
    for n in range(1, len(QKV_PARTS)):
        steps.add(unit(n, summed, QKV_PARTS, part, "q"), f"q{n}")
    steps.run()
    qkv_wires.drain()

    phase("attend")
    every = r["every"]
    heads = (summed.shape[1] - 2 * HD) // HD
    block = summed.shape[0]
    query = jnp.concatenate(
        [turned(summed[:, (2 + h) * HD : (3 + h) * HD]) for h in range(heads)], axis=0
    )
    keys = shared[:, :, :, 0:HD].reshape(-1, HD)
    values = shared[:, :, :, HD : 2 * HD].reshape(-1, HD)
    scores = lax.dot_general(
        query, keys, (((1,), (1,)), ((), ())), preferred_element_type=F32
    ) * HD ** (-0.5)
    key_at = lax.broadcasted_iota(jnp.int32, scores.shape, 1)
    query_at = lax.broadcasted_iota(jnp.int32, scores.shape, 0) % block + at.cp * block
    allowed = key_at <= query_at
    scores = jnp.where(allowed, scores, masked)
    top = jnp.max(scores, axis=-1, keepdims=True)
    weights = jnp.where(allowed, jnp.exp(scores - top), 0.0)
    total = jnp.sum(weights, axis=-1, keepdims=True)
    mean = jnp.dot(weights.astype(BF16), values, preferred_element_type=F32) / total
    mean = mean.astype(BF16)
    for h in range(heads):
        every[at.z, at.y, :, h * HD : (h + 1) * HD] = mean[h * block : (h + 1) * block]

    phase("gather_att")
    out_part, out_got, out_total, projected = (
        r["out_part"],
        r["out_got"],
        r["out_total"],
        r["projected"],
    )
    loads["out"].wait()
    owners = []

    def out_chunk(c):
        p = jnp.dot(chunk_rows(every, at, c), r["out"][...], preferred_element_type=F32)
        blocks = 2 * NY
        for b in range(blocks):
            for t in range(TP):
                first = b * block + t * local_rows
                out_part[c, t, b] = p[first : first + local_rows].astype(BF16)
        copies = []
        for off in range(1, TP):
            to = (at.tp + off) % TP
            copies.append(out_wires.copy(out_part.at[c, to], out_got.at[c, at.tp], {"tp": to}))
        yield
        out_got[c, at.tp] = out_part[c, at.tp]
        for copy in copies:
            copy.wait_recv()

        def sum_part(b, carry):
            parts = out_got[c, 0, b].astype(F32)
            for t in range(1, TP):
                parts = parts + out_got[c, t, b].astype(F32)
            out_total[c, b] = parts.astype(BF16)
            return carry

        lax.fori_loop(0, blocks, sum_part, 0)
        for n, off in enumerate(CHUNKS[c]):
            for turn in range(NY):
                y = (at.y + turn) % NY
                source = out_total.at[c, n * NY + y]
                if off == 0 and turn == 0:
                    projected[at.cp] = source[...]
                else:
                    to = {"cp": (at.z + off) % NZ * NY + y}
                    owners.append(out_wires.copy(source, projected.at[at.cp], to))

    gather_rows(wires, steps, at, every, GATHER_SPLIT, out_chunk)
    steps.run()
    phase("out_cp")
    for copy in owners:
        copy.wait_recv()
    phase("norm_feed")
    for c in range(CP):
        cols = slice(c * width, (c + 1) * width)
        attended[:, cols] = (tokens[:, cols].astype(F32) + projected[c].astype(F32)).astype(BF16)

    normed = normalize(attended[...].astype(F32), r["feed_gain"][...])
    by_width, got_width, stream = r["by_width"], r["got_width"], r["stream"]
    wide = by_width.shape[-1]
    for t in range(TP):
        by_width[t] = normed[:, t * wide : (t + 1) * wide]

    phase("swap1")
    def keep_width():
        got_width[at.tp] = by_width[at.tp]

    exchange(
        r["s2"],
        r["r2"],
        lambda p: by_width.at[p],
        lambda p: got_width.at[p],
        "tp",
        TP,
        at.tp,
        keep_width,
    )
    phase("gather_feed")
    stream[at.z, at.y] = jnp.concatenate(
        [got_width[t].astype(F32) for t in range(TP)], axis=0
    ).astype(BF16)
    for name in ("gate", "up", "down"):
        loads[name].wait()
    reduced = r["reduced"]
    places = {off: (c, n) for c, chunk in enumerate(CHUNKS) for n, off in enumerate(chunk)}
    finished = far_scatter_parts(
        qkv_wires,
        steps,
        lambda off: r["down_sum"].at[places[off]],
        reduced,
        r["down_far"],
        lambda off: at.along_z((at.z + off) % NZ),
    )
    gather_rows(
        qkv_wires,
        steps,
        at,
        stream,
        GATHER_SPLIT,
        lambda c: feed_chunk(qkv_wires, at, r, c, finished),
    )
    steps.run()
    phase("swap2")
    by_token, lowered = r["by_token"], r["lowered"]
    for t in range(TP):
        by_token[t] = reduced[pl.ds(t * local_rows, local_rows), :].astype(BF16)

    def keep_token():
        lowered[at.tp] = by_token[at.tp]

    exchange(
        r["s1"],
        r["r1"],
        lambda p: by_token.at[p],
        lambda p: lowered.at[p],
        "tp",
        TP,
        at.tp,
        keep_token,
    )
    for t in range(TP):
        cols = slice(t * wide, (t + 1) * wide)
        mixed[:, cols] = (attended[:, cols].astype(F32) + lowered[t].astype(F32)).astype(BF16)
    phase("drain")
    wires.drain()
    qkv_wires.drain()
    phase(None)


VMEM = pl.BlockSpec(memory_space=pltpu.VMEM)
ANY = pl.BlockSpec(memory_space=pl.ANY)
COPIES, COPIES_2 = 128, 112


def dma(count):
    return pltpu.SemaphoreType.DMA((count,))


def on_device(
    tokens,
    attention_gain,
    query_weight,
    key_weight,
    value_weight,
    out_weight,
    feed_gain,
    gate_weight,
    up_weight,
    down_weight,
):
    local_rows, model = tokens.shape
    block = local_rows * TP
    rows = block * CP
    qkv = query_weight.shape[1] + key_weight.shape[1] + value_weight.shape[1]
    units = gate_weight.shape[1]
    wide, width = model // TP, model // CP
    chunks = len(CHUNKS)

    inverse = rope_base ** (-(jnp.arange(HD // 2, dtype=F32) * 2.0 / HD))
    positions = lax.axis_index("cp") * block + jnp.arange(block, dtype=jnp.int32)
    angles = positions.astype(F32)[:, None] * inverse[None, :]
    cosine, sine = jnp.cos(angles), jnp.sin(angles)

    inputs = {
        "tokens": tokens,
        "attention_gain": attention_gain[None],
        "feed_gain": feed_gain[None],
        "cos": jnp.concatenate([cosine, cosine], axis=1),
        "sin": jnp.concatenate([-sine, sine], axis=1),
        "key_weight": key_weight,
        "value_weight": value_weight,
        "query_weight": query_weight,
        "out_weight": out_weight,
        "gate_weight": gate_weight,
        "up_weight": up_weight,
        "down_weight": down_weight,
    }

    def buf(*shape, kind=BF16):
        return pltpu.VMEM(shape, kind)

    scratch = {name: buf(*inputs[name + "_weight"].shape) for name in WEIGHTS}
    scratch |= {
        "slices": buf(CP, local_rows, width),
        "got": buf(CP, local_rows, width),
        "columns": buf(TP, CP, local_rows, width),
        "rows_in": buf(CP, block, width),
        "qkv_part": buf(NZ, NY, block, qkv),
        "summed": buf(block, qkv, kind=F32),
        "shared": buf(NZ, NY, block, 2 * HD),
        "every": buf(NZ, NY, block, wide),
        "out_part": buf(chunks, TP, CP // chunks, local_rows, width),
        "out_got": buf(chunks, TP, CP // chunks, local_rows, width),
        "out_total": buf(chunks, CP // chunks, local_rows, width),
        "projected": buf(CP, local_rows, width),
        "by_width": buf(TP, local_rows, wide),
        "got_width": buf(TP, local_rows, wide),
        "stream": buf(NZ, NY, block, wide),
        "unit_part": buf(chunks, 2, NY, block, 2 * units),
        "held": buf(chunks, NX, block, 2 * units),
        "from_left": buf(chunks, NX // 2, block, 2 * units),
        "from_right": buf(chunks, NX // 2, block, 2 * units),
        "unit_total": buf(chunks, block, 2 * units, kind=F32),
        "hidden": buf(chunks, 2, NX, block, units),
        "down_part": buf(chunks, 2, NY, block, wide),
        "down_left": buf(chunks, NY // 2, 2, block, wide),
        "down_right": buf(chunks, NY // 2, 2, block, wide),
        "down_sum": buf(chunks, 2, block, wide),
        "down_far": buf(8, block, wide),
        "reduced": buf(block, wide, kind=F32),
        "by_token": buf(TP, local_rows, wide),
        "lowered": buf(TP, local_rows, wide),
    }
    scratch |= scatter_scratch("q", QKV_PARTS, block)
    for n, count in enumerate((CP, TP, TP)):
        scratch |= {f"s{n}": dma(count), f"r{n}": dma(count)}
    scratch |= {"load": dma(len(WEIGHTS)), "send": dma(COPIES), "recv": dma(COPIES)}
    scratch |= {"send_2": dma(COPIES_2), "recv_2": dma(COPIES_2)}

    names = (*inputs, "attended", "mixed", *scratch)
    shape = jax.ShapeDtypeStruct(tokens.shape, BF16)
    return pl.pallas_call(
        functools.partial(layer_kernel, names),
        out_shape=(shape, shape),
        in_specs=[ANY if name.endswith("_weight") else VMEM for name in inputs],
        out_specs=(VMEM, VMEM),
        scratch_shapes=list(scratch.values()),
        compiler_params=pltpu.CompilerParams(
            collective_id=0,
            has_side_effects=True,
            vmem_limit_bytes=60 * 1024 * 1024,
        ),
        name="layer",
    )(*inputs.values())


def solution(mesh):
    in_specs = (
        P(("cp", "tp"), None),
        P(),
        P("cp", "tp"),
        P("cp", "tp"),
        P("cp", "tp"),
        P("tp", "cp"),
        P(),
        P("tp", "cp"),
        P("tp", "cp"),
        P("cp", "tp"),
    )
    out_specs = (P(("cp", "tp"), None), P(("cp", "tp"), None))
    return jax.shard_map(
        on_device, mesh=mesh, in_specs=in_specs, out_specs=out_specs, check_vma=False
    )
```

```python
import collections
import functools

import jax
import jax.numpy as jnp
from jax import lax
from jax.experimental import pallas as pl
from jax.experimental.pallas import tpu as pltpu
from jax.sharding import PartitionSpec as P

HD = 128
NZ, NY, NX = 8, 4, 4
CP, TP = NZ * NY, NX * 2
MESH = pl.DeviceIdType.MESH
F32, BF16 = jnp.float32, jnp.bfloat16

epsilon = 1e-05
rope_base = 500000.0
masked = -1e30


class Wires:
    def __init__(self, send, recv):
        self.send, self.recv, self.used, self.sent = send, recv, 0, []

    def copy(self, src, dst, device):
        i = self.used
        self.used += 1
        assert i < self.send.shape[0]
        c = pltpu.make_async_remote_copy(
            src_ref=src,
            dst_ref=dst,
            send_sem=self.send.at[i],
            recv_sem=self.recv.at[i],
            device_id=device,
            device_id_type=MESH,
        )
        c.start()
        self.sent.append(c)
        return c

    def drain(self):
        for c in self.sent:
            c.wait_send()
        self.sent, self.used = [], 0


class Now(list):
    pass


def advance(gen):
    needs = next(gen, None)
    while isinstance(needs, Now):
        for c in needs:
            c.wait_recv()
        needs = next(gen, None)
    return needs


class Steps:
    def __init__(self):
        self.queue = collections.deque()

    def add(self, gen, name="line", step=0):
        with jax.named_scope(f"{name}_{step}"):
            needs = advance(gen)
        if needs is not None:
            self.queue.append((needs, gen, name, step + 1))

    def go_on(self, entry):
        needs, gen, name, step = entry
        with jax.named_scope(f"wait_{name}_{step}"):
            for c in needs:
                c.wait_recv()
        self.add(gen, name, step)

    def run(self, until=lambda: False):
        while self.queue and not until():
            self.go_on(self.queue.popleft())

    def play(self, order, begin=None):
        for name in order.split():
            if name.isupper():
                begin(name)
                continue
            at = next(i for i, entry in enumerate(self.queue) if entry[2] == name)
            entry = self.queue[at]
            del self.queue[at]
            self.go_on(entry)


class Phases:
    def __init__(self):
        self.scope = None

    def __call__(self, name):
        if self.scope:
            self.scope.__exit__(None, None, None)
        self.scope = jax.named_scope(name) if name else None
        if self.scope:
            self.scope.__enter__()


class Place:
    def __init__(self):
        self.cp, self.tp = lax.axis_index("cp"), lax.axis_index("tp")
        self.z, self.y = self.cp // NY, self.cp % NY
        self.x, self.core = self.tp // 2, self.tp % 2

    def along_z(self, z):
        return {"cp": z * NY + self.y}

    def along_y(self, y):
        return {"cp": self.z * NY + y}

    def along_x(self, x):
        return {"tp": x * 2 + self.core}

    def partner(self):
        return {"tp": self.x * 2 + 1 - self.core}


def ring(n, me, device_of):
    return device_of((me + 1) % n), device_of((me + n - 1) % n)


def greet(devices):
    barrier = pltpu.get_barrier_semaphore()
    for device in devices:
        pl.semaphore_signal(barrier, inc=1, device_id=device, device_id_type=MESH)
    return len(devices)


def greet_group(axis, n, me):
    barrier = pltpu.get_barrier_semaphore()

    def signal(off, carry):
        pl.semaphore_signal(
            barrier, inc=1, device_id={axis: (me + off) % n}, device_id_type=MESH
        )
        return carry

    lax.fori_loop(1, n, signal, 0)
    return n - 1


def await_greetings(count):
    pl.semaphore_wait(pltpu.get_barrier_semaphore(), count)


def half_of(ref, h):
    d = ref.shape[0] // 2
    return ref.at[pl.ds(h * d, d)]


def ring_gather(wires, block, n, me, device_of, arrived=None):
    right, left = ring(n, me, device_of)
    last = n // 2 - 1

    def send(k):
        r, l = block((me + n - k) % n), block((me + k) % n)
        if k == last:
            r, l = half_of(r, 0), half_of(l, 1)
        return wires.copy(r, r, right), wires.copy(l, l, left)

    flying = send(0)
    if arrived:
        arrived(me)
    for k in range(1, n // 2 + 1):
        yield flying
        if k <= last:
            flying = send(k)
            if arrived:
                arrived((me + n - k) % n)
                arrived((me + k) % n)
        elif arrived:
            arrived((me + n // 2) % n)


def add_rows(dst, terms, finish=None):
    if len(dst.shape) == 3:
        for i in range(dst.shape[0]):
            add_rows(dst.at[i], [t.at[i] for t in terms])
        return
    rows = dst.shape[0]
    step = min(rows, 16)

    def body(i, carry):
        at = pl.ds(pl.multiple_of(i * step, step), step)
        total = terms[0][at, :].astype(F32)
        for t in terms[1:]:
            total = total + t[at, :].astype(F32)
        dst[at, :] = total.astype(dst.dtype)
        return carry

    lax.fori_loop(0, rows // step, body, 0)


def ring_scatter(wires, own, out, from_left, from_right, n, me, device_of):
    right, left = ring(n, me, device_of)
    m = n // 2
    far = own((me + m) % n)
    r = wires.copy(half_of(far, 0), half_of(from_left.at[0], 0), right)
    l = wires.copy(half_of(far, 1), half_of(from_right.at[0], 1), left)
    for k in range(1, m):
        to_right, to_left = own((me + m - k) % n), own((me + n - m + k) % n)
        got_left, got_right = from_left.at[k - 1], from_right.at[k - 1]
        yield [r]
        if k == 1:
            add_rows(half_of(got_left, 0), [half_of(got_left, 0), half_of(to_right, 0)])
            add_rows(half_of(got_left, 1), [half_of(to_right, 1)])
        else:
            add_rows(got_left, [got_left, to_right])
        r = wires.copy(got_left, from_left.at[k], right)
        yield Now([l])
        if k == 1:
            add_rows(half_of(got_right, 1), [half_of(got_right, 1), half_of(to_left, 1)])
            add_rows(half_of(got_right, 0), [half_of(to_left, 0)])
        else:
            add_rows(got_right, [got_right, to_left])
        l = wires.copy(got_right, from_right.at[k], left)
    yield [r, l]
    add_rows(out, [own(me), from_left.at[m - 1], from_right.at[m - 1]])


def far_gather(wires, block, n, me, device_of, arrived):
    def send(ref, off):
        return wires.copy(ref, ref, device_of((me + n + off) % n))

    def whole(off):
        return block((me + n + off) % n)

    own = block(me)
    p2, m2, p1, m1 = send(own, 2), send(own, -2), send(own, 1), send(own, -1)
    arrived(0)
    yield [p2]
    p3, p4 = send(whole(-2), 1), send(half_of(whole(-2), 0), 2)
    yield Now([m2])
    m3, m4 = send(whole(2), -1), send(half_of(whole(2), 1), -2)
    yield Now([p1])
    arrived(7)
    yield Now([m1])
    for off in (1, 6, 2):
        arrived(off)
    yield [p3]
    arrived(5)
    yield Now([m3])
    arrived(3)
    yield Now([p4, m4])
    arrived(4)


def far_scatter(wires, own, out, bufs, n, me, device_of):
    lines = FarScatter(
        wires,
        lambda off: own((me + off) % n),
        out,
        bufs,
        lambda off: device_of((me + off) % n),
    )
    for off in (4, 3, 5, 1, 7):
        lines.send(off)
    yield from lines.turns("l")
    other = lines.turns("r")
    yield Now(next(other))
    next(other, None)
    yield from lines.last_round()


class FarScatter:
    def __init__(self, wires, own, out, bufs, device_of):
        self.wires, self.own, self.out, self.device_of = wires, own, out, device_of
        self.bufs, self.sent = bufs, {}

    def copy(self, name, src, dst, off):
        self.sent[name] = self.wires.copy(src, dst, self.device_of(off))

    def send(self, off):
        near_l, near_r, turn_l, turn_r, far_l, far_r = [self.bufs.at[i] for i in range(6)]
        term = self.own(off)
        if off == 1:
            self.copy("near_l", term, near_l, 1)
        elif off == 7:
            self.copy("near_r", term, near_r, 7)
        elif off == 3:
            self.copy("turn_l", term, turn_l, 1)
        elif off == 5:
            self.copy("turn_r", term, turn_r, 7)
        elif off == 4:
            self.copy("far_l", half_of(term, 0), half_of(far_l, 0), 2)
            self.copy("far_r", half_of(term, 1), half_of(far_r, 1), 6)

    def turn(self, side):
        n, off, full = (0, 2, 0) if side == "l" else (1, 6, 1)
        turn, far, into = self.bufs.at[2 + n], self.bufs.at[4 + n], self.bufs.at[6 + n]
        mine = self.own(off)
        add_rows(half_of(turn, full), [half_of(x, full) for x in (turn, far, mine)])
        add_rows(half_of(turn, 1 - full), [half_of(x, 1 - full) for x in (turn, mine)])
        self.copy("sum_" + side, turn, into, off)

    def turns(self, side):
        yield [self.sent["turn_" + side], self.sent["far_" + side]]
        self.turn(side)

    def last_round(self):
        yield [self.sent[n] for n in ("near_l", "near_r", "sum_l", "sum_r")]
        near_l, near_r, sum_l, sum_r = [self.bufs.at[i] for i in (0, 1, 6, 7)]
        add_rows(self.out, [self.own(0), near_l, near_r, sum_l, sum_r])


def exchange(send_sem, recv_sem, source, target, axis, n, me, meanwhile=None):
    def copy(off):
        peer = (me + off) % n
        return pltpu.make_async_remote_copy(
            src_ref=source(peer),
            dst_ref=target(me),
            send_sem=send_sem.at[off],
            recv_sem=recv_sem.at[off],
            device_id={axis: peer},
            device_id_type=MESH,
        )

    def start(off, carry):
        copy(off).start()
        return carry

    def wait(off, carry):
        copy(off).wait()
        return carry

    lax.fori_loop(1, n, start, 0)
    if meanwhile:
        meanwhile()
    lax.fori_loop(1, n, wait, 0)


Z_FIRST, Y_FIRST = "z", "y"
QKV_PARTS = ((0, 256, Y_FIRST), (256, 256, Y_FIRST), (512, 384, Y_FIRST), (896, 384, Z_FIRST))
QKV_ORDER = "k a b c k a c k b a k b c a k b c k"
GATHER_SPLIT = 768
DOWN_SPLIT = 768


CHUNKS = ((2, 6), (3, 4), (5, 7), (0, 1))
OUT_CHUNKS = ((0, 7), (1, 6), (2, 5), (3, 4))


def gather_rows(wires, steps, at, out_ref, split, chunks, ready):
    first, rest = pl.ds(0, split), pl.ds(split, out_ref.shape[-1] - split)
    seen = collections.Counter()

    def z_at(off):
        return (at.z + off) % NZ

    def mark(off):
        seen[off] += 1
        for c, chunk in enumerate(chunks):
            if off in chunk and all(seen[o] == 2 for o in chunk):
                steps.add(ready(c), f"chunk{chunks[c][0]}{chunks[c][1]}")

    def y_first():
        yield from ring_gather(
            wires, lambda j: out_ref.at[at.z, j, :, rest], NY, at.y, at.along_y
        )
        yield from far_gather(
            wires, lambda i: out_ref.at[i, :, :, rest], NZ, at.z, at.along_z, mark
        )

    def to_y(off):
        def line():
            yield from ring_gather(
                wires, lambda j: out_ref.at[z_at(off), j, :, first], NY, at.y, at.along_y
            )
            mark(off)

        steps.add(line(), f"y{off}")

    steps.add(y_first(), "yz")
    steps.add(
        far_gather(
            wires, lambda i: out_ref.at[i, at.y, :, first], NZ, at.z, at.along_z, to_y
        ),
        "z",
    )


def gather_small(wires, at, ref):
    handed = []

    def to_y(block):
        for off in (1, 3, 2):
            handed.append(wires.copy(block, block, at.along_y((at.y + off) % NY)))

    own = ref.at[at.z, at.y]
    order = (4, 3, 5, 2, 6, 1, 7)
    copies = {off: wires.copy(own, own, at.along_z((at.z + off) % NZ)) for off in order}
    to_y(own)
    yield []
    for off in (1, 7, 2, 6, 3, 5, 4):
        yield Now([copies[off]])
        to_y(ref.at[(at.z + NZ - off) % NZ, at.y])
    yield handed


def scatter_part(wires, at, part, out, columns, way, bufs):
    if way == Z_FIRST:
        z_bufs, y_left, y_right, y_sum = bufs
        yield from far_scatter(
            wires, lambda i: part.at[i, :, :, columns], y_sum, z_bufs, NZ, at.z, at.along_z
        )
        yield from ring_scatter(
            wires,
            lambda j: y_sum.at[j],
            out.at[:, columns],
            y_left,
            y_right,
            NY,
            at.y,
            at.along_y,
        )
    else:
        z_bufs, y_left, y_right, z_sum = bufs
        yield from ring_scatter(
            wires,
            lambda j: part.at[:, j, :, columns],
            z_sum,
            y_left,
            y_right,
            NY,
            at.y,
            at.along_y,
        )
        yield from far_scatter(
            wires, lambda i: z_sum.at[i], out.at[:, columns], z_bufs, NZ, at.z, at.along_z
        )


def scatter_scratch(prefix, parts, rows):
    scratch = {}
    for n, (_, width, way) in enumerate(parts):
        if way == Z_FIRST:
            shapes = (
                (NZ, NY, rows, width),
                (NY // 2, rows, width),
                (NY // 2, rows, width),
                (NY, rows, width),
            )
        else:
            shapes = (
                (NZ, rows, width),
                (NY // 2, NZ, rows, width),
                (NY // 2, NZ, rows, width),
                (NZ, rows, width),
            )
        for m, shape in enumerate(shapes):
            scratch[f"{prefix}{n}{m}"] = pltpu.VMEM(shape, BF16)
    return scratch


def product_into(part, x, w_ref, start):
    width = w_ref.shape[1]
    tile = min(width, 256)

    def body(i, carry):
        at = pl.multiple_of(i * tile, tile)
        p = jnp.dot(x(), w_ref[:, pl.ds(at, tile)], preferred_element_type=F32)
        part[:, :, :, pl.ds(pl.multiple_of(start + at, 128), tile)] = p.astype(BF16).reshape(
            *part.shape[:3], tile
        )
        return carry

    lax.fori_loop(0, width // tile, body, 0)


def chunk_rows(ref, at, chunk):
    blocks = [ref[(at.z + off) % NZ] for off in chunk]
    return jnp.concatenate([b.reshape(-1, b.shape[-1]) for b in blocks], axis=0)


ORDER = (
    "a B C b D c a d b a c d b a a c d b c a d b b c c "
    "d d a b V v c d W w b T c U d N n t u L n l n"
)


def feed_chunk(wires, at, r, c, produced, finished):
    partner = at.partner()
    units = r["gate"].shape[1]
    part, held, total, hidden = (
        r["unit_part"].at[c],
        r["held"].at[c],
        r["unit_total"].at[c],
        r["hidden"].at[c],
    )
    rows = total.shape[0]

    def tile(w_ref, col, width, start):
        p = jnp.dot(
            chunk_rows(r["stream"], at, CHUNKS[c]), w_ref[:, pl.ds(col, width)], preferred_element_type=F32
        )
        part[:, :, :, pl.ds(start + col, width)] = p.astype(BF16).reshape(2, NY, rows, width)

    def body(t):
        col = t * 256
        tile(r["gate"], col, 256, 0)
        tile(r["up"], col, 256, units)

    for t in range(units // 256):
        body(t)
    if units % 256:
        tile(r["gate"], units // 256 * 256, units % 256, 0)
        tile(r["up"], units // 256 * 256, units % 256, units)
    yield [wires.copy(part.at[1 - at.core], held, partner)]
    add_rows(held, [held, part.at[at.core]])
    yield from ring_scatter(
        wires,
        lambda i: held.at[i],
        total,
        r["from_left"].at[c],
        r["from_right"].at[c],
        NX,
        at.x,
        at.along_x,
    )

    def activate(i, carry):
        here = pl.ds(pl.multiple_of(i * 16, 16), 16)
        gate, up = total[here, pl.ds(0, units)], total[here, pl.ds(units, units)]
        hidden[at.core, at.x, here, :] = (jax.nn.silu(gate) * up).astype(BF16)
        return carry

    lax.fori_loop(0, rows // 16, activate, 0)
    handed = []

    def hand_over(i):
        ref = hidden.at[at.core, i]
        handed.append(wires.copy(ref, ref, partner))

    yield from ring_gather(
        wires, lambda i: hidden.at[at.core, i], NX, at.x, at.along_x, hand_over
    )
    yield handed
    down_part = r["down_part"].at[c]

    def down(i, carry):
        cols = pl.ds(pl.multiple_of(i * 256, 256), 256)
        p = jnp.dot(
            hidden[...].reshape(2 * NX * rows, units), r["down"][:, cols], preferred_element_type=F32
        )
        down_part[:, :, :, cols] = p.astype(BF16).reshape(2, NY, rows, 256)
        return carry

    lax.fori_loop(0, down_part.shape[-1] // 256, down, 0)
    produced(c)
    yield from ring_scatter(
        wires,
        lambda j: down_part.at[:, j, :, pl.ds(0, DOWN_SPLIT)],
        r["down_sum"].at[c],
        r["down_left"].at[c],
        r["down_right"].at[c],
        NY,
        at.y,
        at.along_y,
    )
    finished(c)


def normalize(values, gain):
    mean_square = jnp.mean(values * values, axis=-1, keepdims=True)
    return (values * lax.rsqrt(mean_square + epsilon) * gain).astype(BF16)


WEIGHTS = ("key", "value", "query", "out", "gate", "up", "down")


def layer_kernel(names, *refs):
    r = dict(zip(names, refs))
    at = Place()
    qkv_wires, wires = Wires(r["send"], r["recv"]), Wires(r["send"], r["recv_2"])
    steps = Steps()
    out_wires = wires
    tokens = r["tokens"]
    local_rows, model = tokens.shape
    attended, mixed = r["streams"].at[0], r["streams"].at[1]
    cos, sin = r["cos"], r["sin"]

    phase = Phases()
    phase("greet")
    greeted = greet_group("cp", CP, at.cp) + greet_group("tp", TP, at.tp)
    loads = {}
    for n, name in enumerate(WEIGHTS):
        loads[name] = pltpu.make_async_copy(
            r[name + "_weight"], r[name], r["load"].at[n]
        )
        loads[name].start()

    normed = normalize(tokens[...].astype(F32), r["attention_gain"][...])
    slices, got, columns = r["slices"], r["got"], r["columns"]
    width = slices.shape[-1]
    for c in range(CP):
        slices[c] = normed[:, c * width : (c + 1) * width]
    phase("barrier")
    await_greetings(greeted)

    phase("spread_cp")
    def keep_slice():
        got[at.cp] = slices[at.cp]

    exchange(
        r["send"], r["recv_2"], lambda p: slices.at[p], lambda p: got.at[p], "cp", CP, at.cp, keep_slice
    )

    phase("spread_tp")
    def keep_columns():
        columns[at.tp] = got[...]

    exchange(
        r["send"], r["r0"], lambda p: got, lambda p: columns.at[p], "tp", TP, at.tp, keep_columns
    )
    phase("relayout")
    rows_in = r["rows_in"]

    def in_order(b, carry):
        parts = [columns[t, b].astype(F32) for t in range(TP)]
        rows_in[b] = jnp.concatenate(parts, axis=0).astype(BF16)
        return carry

    lax.fori_loop(0, CP, in_order, 0)

    part, summed, shared = r["qkv_part"], r["summed"], r["shared"]

    def x():
        return rows_in[...].reshape(-1, width)

    def turned(v):
        return (v * cos[...] + pltpu.roll(v, HD // 2, 1) * sin[...]).astype(BF16)

    def unit(n, out, parts, partial, prefix):
        start, extent, way = parts[n]
        bufs = [r[f"{prefix}{n}{m}"] for m in range(4)]
        return scatter_part(qkv_wires, at, partial, out, pl.ds(start, extent), way, bufs)

    def keys_and_values():
        yield from unit(0, summed, QKV_PARTS, part, "q")
        shared[at.z, at.y, :, pl.ds(0, HD)] = turned(summed[:, pl.ds(0, HD)])
        shared[at.z, at.y, :, pl.ds(HD, HD)] = summed[:, pl.ds(HD, HD)].astype(BF16)
        yield from gather_small(qkv_wires, at, shared)

    phase("qkv")
    loads["key"].wait()
    loads["value"].wait()
    product_into(part, x, r["key"], 0)
    product_into(part, x, r["value"], HD)
    steps.add(keys_and_values(), "k")
    loads["query"].wait()
    product_into(part, x, r["query"], 2 * HD)
    phase("qkv_sum")
    for n in range(1, len(QKV_PARTS)):
        steps.add(unit(n, summed, QKV_PARTS, part, "q"), "kabc"[n])
    steps.play(QKV_ORDER)
    steps.run()
    qkv_wires.drain()

    phase("attend")
    every = r["every"]
    heads = (summed.shape[1] - 2 * HD) // HD
    block = summed.shape[0]
    query = jnp.concatenate(
        [turned(summed[:, (2 + h) * HD : (3 + h) * HD]) for h in range(heads)], axis=0
    )
    keys = shared[:, :, :, 0:HD].reshape(-1, HD)
    values = shared[:, :, :, HD : 2 * HD].reshape(-1, HD)
    scores = lax.dot_general(
        query, keys, (((1,), (1,)), ((), ())), preferred_element_type=F32
    ) * HD ** (-0.5)
    key_at = lax.broadcasted_iota(jnp.int32, scores.shape, 1)
    query_at = lax.broadcasted_iota(jnp.int32, scores.shape, 0) % block + at.cp * block
    allowed = key_at <= query_at
    scores = jnp.where(allowed, scores, masked)
    top = jnp.max(scores, axis=-1, keepdims=True)
    weights = jnp.where(allowed, jnp.exp(scores - top), 0.0)
    total = jnp.sum(weights, axis=-1, keepdims=True)
    mean = jnp.dot(weights.astype(BF16), values, preferred_element_type=F32) / total
    mean = mean.astype(BF16)
    for h in range(heads):
        every[at.z, at.y, :, h * HD : (h + 1) * HD] = mean[h * block : (h + 1) * block]

    phase("gather_att")
    out_part, out_got, out_total, projected = (
        r["out_part"],
        r["out_got"],
        r["out_total"],
        r["projected"],
    )
    loads["out"].wait()
    owners = []

    def out_chunk(c):
        p = jnp.dot(chunk_rows(every, at, OUT_CHUNKS[c]), r["out"][...], preferred_element_type=F32)
        blocks = 2 * NY
        for b in range(blocks):
            for t in range(TP):
                first = b * block + t * local_rows
                out_part[c, t, b] = p[first : first + local_rows].astype(BF16)
        copies = []
        for off in range(1, TP):
            to = (at.tp + off) % TP
            copies.append(out_wires.copy(out_part.at[c, to], out_got.at[c, at.tp], {"tp": to}))
        out_got[c, at.tp] = out_part[c, at.tp]
        yield copies

        def sum_part(b, carry):
            parts = out_got[c, 0, b].astype(F32)
            for t in range(1, TP):
                parts = parts + out_got[c, t, b].astype(F32)
            out_total[c, b] = parts.astype(BF16)
            return carry

        lax.fori_loop(0, blocks, sum_part, 0)
        for n, off in enumerate(OUT_CHUNKS[c]):
            for turn in range(NY):
                y = (at.y + turn) % NY
                source = out_total.at[c, n * NY + y]
                if off == 0 and turn == 0:
                    projected[at.cp] = source[...]
                else:
                    to = {"cp": (at.z + off) % NZ * NY + y}
                    owners.append(out_wires.copy(source, projected.at[at.cp], to))

    gather_rows(wires, steps, at, every, GATHER_SPLIT, OUT_CHUNKS, out_chunk)
    steps.run()
    phase("out_cp")
    for c in owners:
        c.wait_recv()
    wires.drain()
    phase("norm_feed")
    for c in range(CP):
        cols = slice(c * width, (c + 1) * width)
        attended[:, cols] = (tokens[:, cols].astype(F32) + projected[c].astype(F32)).astype(BF16)

    normed = normalize(attended[...].astype(F32), r["feed_gain"][...])
    by_width, got_width, stream = r["by_width"], r["got_width"], r["stream"]
    wide = by_width.shape[-1]
    for t in range(TP):
        by_width[t] = normed[:, t * wide : (t + 1) * wide]

    phase("swap1")
    def keep_width():
        got_width[at.tp] = by_width[at.tp]

    exchange(
        r["send"],
        r["r1"],
        lambda p: by_width.at[p],
        lambda p: got_width.at[p],
        "tp",
        TP,
        at.tp,
        keep_width,
    )
    phase("gather_feed")
    stream[at.z, at.y] = jnp.concatenate(
        [got_width[t].astype(F32) for t in range(TP)], axis=0
    ).astype(BF16)
    for name in ("gate", "up", "down"):
        loads[name].wait()
    reduced = r["reduced"]
    places = {off: (c, n) for c, chunk in enumerate(CHUNKS) for n, off in enumerate(chunk)}
    def to_z(off):
        return at.along_z((at.z + off) % NZ)

    lines = FarScatter(
        qkv_wires,
        lambda off: r["down_sum"].at[places[off]],
        reduced.at[:, pl.ds(0, DOWN_SPLIT)],
        r["down_far"],
        to_z,
    )
    rest = pl.ds(DOWN_SPLIT, reduced.shape[1] - DOWN_SPLIT)
    z_lines = FarScatter(
        qkv_wires,
        lambda off: r["down_part"].at[*places[off], :, :, rest],
        r["z_sum"],
        r["z_far"],
        to_z,
    )
    there = {}

    def produced(c):
        for off in CHUNKS[c]:
            z_lines.send(off)

    def finished(c):
        for off in CHUNKS[c]:
            lines.send(off)

    def z_first_end():
        yield from z_lines.last_round()
        yield from ring_scatter(
            qkv_wires,
            lambda j: r["z_sum"].at[j],
            reduced.at[:, rest],
            r["z_left"],
            r["z_right"],
            NY,
            at.y,
            at.along_y,
        )

    later = {
        "T": lambda: lines.turns("l"),
        "U": lambda: lines.turns("r"),
        "V": lambda: z_lines.turns("l"),
        "W": lambda: z_lines.turns("r"),
        "N": z_first_end,
        "L": lines.last_round,
    }

    def begin(letter):
        if letter in later:
            gen = later[letter]()
        else:
            gen = feed_chunk(qkv_wires, at, r, "ABCD".index(letter), produced, finished)
        steps.add(gen, letter.lower())

    def chunk_there(c):
        there[c] = True
        if c == 0:
            begin("A")
        return iter(())

    gather_rows(qkv_wires, steps, at, stream, GATHER_SPLIT, CHUNKS, chunk_there)
    steps.run(lambda: len(there) == len(CHUNKS))
    steps.play(ORDER, begin)
    steps.run()
    phase("swap2")
    qkv_wires.drain()
    by_token, lowered = r["by_token"], r["lowered"]
    for t in range(TP):
        by_token[t] = reduced[pl.ds(t * local_rows, local_rows), :].astype(BF16)

    def keep_token():
        lowered[at.tp] = by_token[at.tp]

    exchange(
        r["send"],
        r["r0"],
        lambda p: by_token.at[p],
        lambda p: lowered.at[p],
        "tp",
        TP,
        at.tp,
        keep_token,
    )
    for t in range(TP):
        cols = slice(t * wide, (t + 1) * wide)
        mixed[:, cols] = (attended[:, cols].astype(F32) + lowered[t].astype(F32)).astype(BF16)
    phase(None)


VMEM = pl.BlockSpec(memory_space=pltpu.VMEM)
ANY = pl.BlockSpec(memory_space=pl.ANY)
COPIES, COPIES_2 = 140, 111


def dma(count):
    return pltpu.SemaphoreType.DMA((count,))


def on_device(
    tokens,
    attention_gain,
    query_weight,
    key_weight,
    value_weight,
    out_weight,
    feed_gain,
    gate_weight,
    up_weight,
    down_weight,
):
    local_rows, model = tokens.shape
    block = local_rows * TP
    rows = block * CP
    qkv = query_weight.shape[1] + key_weight.shape[1] + value_weight.shape[1]
    units = gate_weight.shape[1]
    wide, width = model // TP, model // CP
    chunks = len(CHUNKS)

    inverse = rope_base ** (-(jnp.arange(HD // 2, dtype=F32) * 2.0 / HD))
    positions = lax.axis_index("cp") * block + jnp.arange(block, dtype=jnp.int32)
    angles = positions.astype(F32)[:, None] * inverse[None, :]
    cosine, sine = jnp.cos(angles), jnp.sin(angles)

    inputs = {
        "tokens": tokens,
        "attention_gain": attention_gain[None],
        "feed_gain": feed_gain[None],
        "cos": jnp.concatenate([cosine, cosine], axis=1),
        "sin": jnp.concatenate([-sine, sine], axis=1),
        "key_weight": key_weight,
        "value_weight": value_weight,
        "query_weight": query_weight,
        "out_weight": out_weight,
        "gate_weight": gate_weight,
        "up_weight": up_weight,
        "down_weight": down_weight,
    }

    def buf(*shape, kind=BF16):
        return pltpu.VMEM(shape, kind)

    scratch = {name: buf(*inputs[name + "_weight"].shape) for name in WEIGHTS}
    scratch |= {
        "slices": buf(CP, local_rows, width),
        "got": buf(CP, local_rows, width),
        "columns": buf(TP, CP, local_rows, width),
        "rows_in": buf(CP, block, width),
        "qkv_part": buf(NZ, NY, block, qkv),
        "summed": buf(block, qkv, kind=F32),
        "shared": buf(NZ, NY, block, 2 * HD),
        "every": buf(NZ, NY, block, wide),
        "out_part": buf(chunks, TP, CP // chunks, local_rows, width),
        "out_got": buf(chunks, TP, CP // chunks, local_rows, width),
        "out_total": buf(chunks, CP // chunks, local_rows, width),
        "projected": buf(CP, local_rows, width),
        "by_width": buf(TP, local_rows, wide),
        "got_width": buf(TP, local_rows, wide),
        "stream": buf(NZ, NY, block, wide),
        "unit_part": buf(chunks, 2, NY, block, 2 * units),
        "held": buf(chunks, NX, block, 2 * units),
        "from_left": buf(chunks, NX // 2, block, 2 * units),
        "from_right": buf(chunks, NX // 2, block, 2 * units),
        "unit_total": buf(chunks, block, 2 * units, kind=F32),
        "hidden": buf(chunks, 2, NX, block, units),
        "down_part": buf(chunks, 2, NY, block, wide),
        "down_left": buf(chunks, NY // 2, 2, block, DOWN_SPLIT),
        "down_right": buf(chunks, NY // 2, 2, block, DOWN_SPLIT),
        "down_sum": buf(chunks, 2, block, DOWN_SPLIT),
        "down_far": buf(8, block, DOWN_SPLIT),
        "z_far": buf(8, NY, block, wide - DOWN_SPLIT),
        "z_sum": buf(NY, block, wide - DOWN_SPLIT),
        "z_left": buf(NY // 2, block, wide - DOWN_SPLIT),
        "z_right": buf(NY // 2, block, wide - DOWN_SPLIT),
        "reduced": buf(block, wide, kind=F32),
        "by_token": buf(TP, local_rows, wide),
        "lowered": buf(TP, local_rows, wide),
    }
    scratch |= scatter_scratch("q", QKV_PARTS, block)
    scratch |= {f"r{n}": dma(TP) for n in range(2)}
    scratch |= {"load": dma(len(WEIGHTS)), "send": dma(COPIES), "recv": dma(COPIES)}
    scratch |= {"recv_2": dma(COPIES_2)}

    names = (*inputs, "streams", *scratch)
    streams = pl.pallas_call(
        functools.partial(layer_kernel, names),
        out_shape=jax.ShapeDtypeStruct((2, *tokens.shape), BF16),
        in_specs=[ANY if name.endswith("_weight") else VMEM for name in inputs],
        out_specs=VMEM,
        scratch_shapes=list(scratch.values()),
        compiler_params=pltpu.CompilerParams(
            collective_id=0,
            has_side_effects=True,
            vmem_limit_bytes=60 * 1024 * 1024,
        ),
        name="layer",
    )(*inputs.values())
    return streams[0], streams[1]


def solution(mesh):
    in_specs = (
        P(("cp", "tp"), None),
        P(),
        P("cp", "tp"),
        P("cp", "tp"),
        P("cp", "tp"),
        P("tp", "cp"),
        P(),
        P("tp", "cp"),
        P("tp", "cp"),
        P("cp", "tp"),
    )
    out_specs = (P(("cp", "tp"), None), P(("cp", "tp"), None))
    return jax.shard_map(
        on_device, mesh=mesh, in_specs=in_specs, out_specs=out_specs, check_vma=False
    )
```

```python
import collections
import functools

import jax
import jax.numpy as jnp
from jax import lax
from jax.experimental import pallas as pl
from jax.experimental.pallas import tpu as pltpu
from jax.sharding import PartitionSpec as P

HD = 128
NZ, NY, NX = 8, 4, 4
CP, TP = NZ * NY, NX * 2
MESH = pl.DeviceIdType.MESH
F32, BF16 = jnp.float32, jnp.bfloat16

epsilon = 1e-05
rope_base = 500000.0
masked = -1e30


class Wires:
    def __init__(self, send, recv):
        self.send, self.recv, self.used, self.sent = send, recv, 0, []

    def copy(self, src, dst, device):
        i, slots = self.used, self.send.shape[0]
        self.used += 1
        assert i < self.recv.shape[0]
        if i >= slots:
            self.sent[i - slots].wait_send()
        c = pltpu.make_async_remote_copy(
            src_ref=src,
            dst_ref=dst,
            send_sem=self.send.at[i % slots],
            recv_sem=self.recv.at[i],
            device_id=device,
            device_id_type=MESH,
        )
        c.start()
        self.sent.append(c)
        return c

    def drain(self):
        for c in self.sent[-self.send.shape[0] :]:
            c.wait_send()
        self.sent, self.used = [], 0


class Now(list):
    pass


def advance(gen):
    needs = next(gen, None)
    while isinstance(needs, Now):
        for c in needs:
            c.wait_recv()
        needs = next(gen, None)
    return needs


class Steps:
    def __init__(self):
        self.queue, self.begun = collections.deque(), set()

    def add(self, gen, name="line", step=0):
        with jax.named_scope(f"{name}_{step}"):
            needs = advance(gen)
        if needs is not None:
            self.queue.append((needs, gen, name, step + 1))

    def go_on(self, entry):
        needs, gen, name, step = entry
        with jax.named_scope(f"wait_{name}_{step}"):
            for c in needs:
                c.wait_recv()
        self.add(gen, name, step)

    def run(self, until=lambda: False):
        while self.queue and not until():
            self.go_on(self.queue.popleft())

    def play(self, order, begin):
        for word in order.split():
            if word.isupper():
                if word not in self.begun:
                    self.begun.add(word)
                    begin(word)
                continue
            name, step = word.split("/") if "/" in word else (word[0], word[1:])
            step = int(step)
            while True:
                found = [i for i, e in enumerate(self.queue) if e[2] == name]
                if not found or self.queue[found[0]][3] > step:
                    break
                entry = self.queue[found[0]]
                del self.queue[found[0]]
                self.go_on(entry)


class Phases:
    def __init__(self):
        self.scope = None

    def __call__(self, name):
        if self.scope:
            self.scope.__exit__(None, None, None)
        self.scope = jax.named_scope(name) if name else None
        if self.scope:
            self.scope.__enter__()


class Place:
    def __init__(self):
        self.cp, self.tp = lax.axis_index("cp"), lax.axis_index("tp")
        self.z, self.y = self.cp // NY, self.cp % NY
        self.x, self.core = self.tp // 2, self.tp % 2

    def along_z(self, z):
        return {"cp": z * NY + self.y}

    def along_y(self, y):
        return {"cp": self.z * NY + y}

    def along_x(self, x):
        return {"tp": x * 2 + self.core}

    def partner(self):
        return {"tp": self.x * 2 + 1 - self.core}


def ring(n, me, device_of):
    return device_of((me + 1) % n), device_of((me + n - 1) % n)


def greet(devices):
    barrier = pltpu.get_barrier_semaphore()
    for device in devices:
        pl.semaphore_signal(barrier, inc=1, device_id=device, device_id_type=MESH)
    return len(devices)


def greet_group(axis, n, me):
    barrier = pltpu.get_barrier_semaphore()

    def signal(off, carry):
        pl.semaphore_signal(
            barrier, inc=1, device_id={axis: (me + off) % n}, device_id_type=MESH
        )
        return carry

    lax.fori_loop(1, n, signal, 0)
    return n - 1


def await_greetings(count):
    pl.semaphore_wait(pltpu.get_barrier_semaphore(), count)


def half_of(ref, h):
    d = ref.shape[0] // 2
    if d:
        return ref.at[pl.ds(h * d, d)]
    width = ref.shape[-1]
    d = -(-width // 256) * 128
    cols = pl.ds(0, d) if h == 0 else pl.ds(d, width - d)
    return ref.at[(slice(None),) * (len(ref.shape) - 1) + (cols,)]


def ring_gather(wires, block, n, me, device_of, arrived=None):
    right, left = ring(n, me, device_of)
    last = n // 2 - 1

    def send(k):
        r, l = block((me + n - k) % n), block((me + k) % n)
        if k == last:
            r, l = half_of(r, 0), half_of(l, 1)
        return wires.copy(r, r, right), wires.copy(l, l, left)

    flying = send(0)
    if arrived:
        arrived(me)
    for k in range(1, n // 2 + 1):
        yield flying
        if k <= last:
            flying = send(k)
            if arrived:
                arrived((me + n - k) % n)
                arrived((me + k) % n)
        elif arrived:
            arrived((me + n // 2) % n)


def add_rows(dst, terms, finish=None):
    if len(dst.shape) > 2:
        for i in range(dst.shape[0]):
            add_rows(dst.at[i], [t.at[i] for t in terms])
        return
    rows = dst.shape[0]
    step = min(rows, 16)

    def body(i, carry):
        at = pl.ds(pl.multiple_of(i * step, step), step)
        total = terms[0][at, :].astype(F32)
        for t in terms[1:]:
            total = total + t[at, :].astype(F32)
        dst[at, :] = total.astype(dst.dtype)
        return carry

    lax.fori_loop(0, rows // step, body, 0)


def ring_scatter(wires, own, out, from_left, from_right, n, me, device_of):
    right, left = ring(n, me, device_of)
    m = n // 2
    far = own((me + m) % n)
    r = wires.copy(half_of(far, 0), half_of(from_left.at[0], 0), right)
    l = wires.copy(half_of(far, 1), half_of(from_right.at[0], 1), left)
    for k in range(1, m):
        to_right, to_left = own((me + m - k) % n), own((me + n - m + k) % n)
        got_left, got_right = from_left.at[k - 1], from_right.at[k - 1]
        yield [r]
        if k == 1:
            add_rows(half_of(got_left, 0), [half_of(got_left, 0), half_of(to_right, 0)])
            add_rows(half_of(got_left, 1), [half_of(to_right, 1)])
        else:
            add_rows(got_left, [got_left, to_right])
        r = wires.copy(got_left, from_left.at[k], right)
        yield Now([l])
        if k == 1:
            add_rows(half_of(got_right, 1), [half_of(got_right, 1), half_of(to_left, 1)])
            add_rows(half_of(got_right, 0), [half_of(to_left, 0)])
        else:
            add_rows(got_right, [got_right, to_left])
        l = wires.copy(got_right, from_right.at[k], left)
    yield [r, l]
    add_rows(out, [own(me), from_left.at[m - 1], from_right.at[m - 1]])


def far_gather(wires, block, n, me, device_of, arrived):
    def send(ref, off):
        return wires.copy(ref, ref, device_of((me + n + off) % n))

    def whole(off):
        return block((me + n + off) % n)

    own = block(me)
    p2, m2, p1, m1 = send(own, 2), send(own, -2), send(own, 1), send(own, -1)
    arrived(0)
    yield [p2]
    p3, p4 = send(whole(-2), 1), send(half_of(whole(-2), 0), 2)
    yield Now([m2])
    m3, m4 = send(whole(2), -1), send(half_of(whole(2), 1), -2)
    yield Now([p1])
    arrived(7)
    yield Now([m1])
    for off in (1, 6, 2):
        arrived(off)
    yield [p3]
    arrived(5)
    yield Now([m3])
    arrived(3)
    yield Now([p4, m4])
    arrived(4)


def far_scatter(wires, own, out, bufs, n, me, device_of):
    lines = FarScatter(
        wires,
        lambda off: own((me + off) % n),
        out,
        bufs,
        lambda off: device_of((me + off) % n),
    )
    for off in (4, 3, 5, 1, 7):
        lines.send(off)
    yield from lines.turns("l")
    other = lines.turns("r")
    yield Now(next(other))
    next(other, None)
    yield from lines.last_round()


class FarScatter:
    def __init__(self, wires, own, out, bufs, device_of):
        self.wires, self.own, self.out, self.device_of = wires, own, out, device_of
        self.bufs, self.sent = bufs, {}

    def copy(self, name, src, dst, off):
        self.sent[name] = self.wires.copy(src, dst, self.device_of(off))

    def send(self, off):
        near_l, near_r, turn_l, turn_r, far_l, far_r = [self.bufs.at[i] for i in range(6)]
        term = self.own(off)
        if off == 1:
            self.copy("near_l", term, near_l, 1)
        elif off == 7:
            self.copy("near_r", term, near_r, 7)
        elif off == 3:
            self.copy("turn_l", term, turn_l, 1)
        elif off == 5:
            self.copy("turn_r", term, turn_r, 7)
        elif off == 4:
            self.copy("far_l", half_of(term, 0), half_of(far_l, 0), 2)
            self.copy("far_r", half_of(term, 1), half_of(far_r, 1), 6)

    def turn(self, side):
        n, off, full = (0, 2, 0) if side == "l" else (1, 6, 1)
        turn, far, into = self.bufs.at[2 + n], self.bufs.at[4 + n], self.bufs.at[6 + n]
        mine = self.own(off)
        add_rows(half_of(turn, full), [half_of(x, full) for x in (turn, far, mine)])
        add_rows(half_of(turn, 1 - full), [half_of(x, 1 - full) for x in (turn, mine)])
        self.copy("sum_" + side, turn, into, off)

    def turns(self, side):
        yield [self.sent["turn_" + side], self.sent["far_" + side]]
        self.turn(side)

    def last_round(self):
        yield [self.sent[n] for n in ("near_l", "near_r", "sum_l", "sum_r")]
        near_l, near_r, sum_l, sum_r = [self.bufs.at[i] for i in (0, 1, 6, 7)]
        add_rows(self.out, [self.own(0), near_l, near_r, sum_l, sum_r])


def exchange(send_sem, recv_sem, source, target, axis, n, me, meanwhile=None):
    def copy(off):
        peer = (me + off) % n
        return pltpu.make_async_remote_copy(
            src_ref=source(peer),
            dst_ref=target(me),
            send_sem=send_sem.at[off],
            recv_sem=recv_sem.at[off],
            device_id={axis: peer},
            device_id_type=MESH,
        )

    def start(off, carry):
        copy(off).start()
        return carry

    def wait(off, carry):
        copy(off).wait()
        return carry

    lax.fori_loop(1, n, start, 0)
    if meanwhile:
        meanwhile()
    lax.fori_loop(1, n, wait, 0)


Z_FIRST, Y_FIRST = "z", "y"
QKV_PARTS = ((0, 256, Y_FIRST), (256, 256, Y_FIRST), (512, 384, Y_FIRST), (896, 384, Z_FIRST))
QKV_ORDER = "k1 A B k2 c1 a1 k3 b1 a2 c2 k4 a3 b2 c3 a4 c4 b3 k5 o1 b4 k6"
GATHER_SPLIT = 768
DOWN_SPLIT = 768


CHUNKS = {"e": (0,), "b": (2, 6), "c": (3, 4), "d": (5,), "a": (1, 7)}
OUT_CHUNKS = {0: (0, 7, 1, 6, 2), 1: (5, 3, 4)}


def gather_rows(wires, steps, at, out_ref, split, chunks, ready):
    first, rest = pl.ds(0, split), pl.ds(split, out_ref.shape[-1] - split)
    seen = collections.Counter()

    def z_at(off):
        return (at.z + off) % NZ

    def mark(off):
        seen[off] += 1
        for c, chunk in chunks.items():
            if off in chunk and all(seen[o] == 2 for o in chunk):
                steps.add(ready(c), f"chunk{c}")

    def y_first():
        yield from ring_gather(
            wires, lambda j: out_ref.at[at.z, j, :, rest], NY, at.y, at.along_y
        )
        yield from far_gather(
            wires, lambda i: out_ref.at[i, :, :, rest], NZ, at.z, at.along_z, mark
        )

    def to_y(off):
        def line():
            yield from ring_gather(
                wires, lambda j: out_ref.at[z_at(off), j, :, first], NY, at.y, at.along_y
            )
            mark(off)

        steps.add(line(), f"y{off}")

    steps.add(y_first(), "yz")
    steps.add(
        far_gather(
            wires, lambda i: out_ref.at[i, at.y, :, first], NZ, at.z, at.along_z, to_y
        ),
        "z",
    )


def gather_small(wires, at, ref):
    handed = []

    def to_y(block):
        for off in (1, 3, 2):
            handed.append(wires.copy(block, block, at.along_y((at.y + off) % NY)))

    own = ref.at[at.z, at.y]
    order = (4, 3, 5, 2, 6, 1, 7)
    copies = {off: wires.copy(own, own, at.along_z((at.z + off) % NZ)) for off in order}
    to_y(own)
    yield []
    for off in (1, 7, 2, 6, 3, 5, 4):
        yield Now([copies[off]])
        to_y(ref.at[(at.z + NZ - off) % NZ, at.y])
    yield handed


def scatter_part(wires, at, part, out, columns, way, bufs):
    if way == Z_FIRST:
        z_bufs, y_left, y_right, y_sum = bufs
        yield from far_scatter(
            wires, lambda i: part.at[i, :, :, columns], y_sum, z_bufs, NZ, at.z, at.along_z
        )
        yield from ring_scatter(
            wires,
            lambda j: y_sum.at[j],
            out.at[:, columns],
            y_left,
            y_right,
            NY,
            at.y,
            at.along_y,
        )
    else:
        z_bufs, y_left, y_right, z_sum = bufs
        yield from ring_scatter(
            wires,
            lambda j: part.at[:, j, :, columns],
            z_sum,
            y_left,
            y_right,
            NY,
            at.y,
            at.along_y,
        )
        yield from far_scatter(
            wires, lambda i: z_sum.at[i], out.at[:, columns], z_bufs, NZ, at.z, at.along_z
        )


def scatter_scratch(prefix, parts, rows):
    scratch = {}
    for n, (_, width, way) in enumerate(parts):
        if way == Z_FIRST:
            shapes = (
                (NZ, NY, rows, width),
                (NY // 2, rows, width),
                (NY // 2, rows, width),
                (NY, rows, width),
            )
        else:
            shapes = (
                (NZ, rows, width),
                (NY // 2, NZ, rows, width),
                (NY // 2, NZ, rows, width),
                (NZ, rows, width),
            )
        for m, shape in enumerate(shapes):
            scratch[f"{prefix}{n}{m}"] = pltpu.VMEM(shape, BF16)
    return scratch


def product_into(part, x, w_ref, start):
    width = w_ref.shape[1]
    tile = min(width, 256)

    def body(i, carry):
        at = pl.multiple_of(i * tile, tile)
        p = jnp.dot(x(), w_ref[:, pl.ds(at, tile)], preferred_element_type=F32)
        part[:, :, :, pl.ds(pl.multiple_of(start + at, 128), tile)] = p.astype(BF16).reshape(
            *part.shape[:3], tile
        )
        return carry

    lax.fori_loop(0, width // tile, body, 0)


def chunk_rows(ref, at, chunk):
    blocks = [ref[(at.z + off) % NZ] for off in chunk]
    return jnp.concatenate([b.reshape(-1, b.shape[-1]) for b in blocks], axis=0)


GATHER_ORDER = """yz/1 y0/1 z/1 yz/2 y0/2 E y7/1 y1/1 e1 y6/1 y2/1 z/2 yz/3 y7/2 e2 y1/2 y6/2 y2/2 B y5/1 y3/1 y4/1 yz/4 b1 e3 y5/2 y3/2 e4 y4/2"""
ORDER = """b2 C D c1 d1 A b3 a1 c2 d2 b4 e5 a2 c3 d3 b5 e6 a3 b6 c4 d4 e7 a4 c5 c6 b7 d5 d6 a5 a6 e8 b8 c7 V v1 W w1 d7 a7 c8 d8 T U a8 N n1 t1 u1 n2 L l1 n3"""


def feed_chunk(wires, at, r, c, produced, finished):
    partner = at.partner()
    units = r["gate"].shape[1]
    part, held, total, hidden, down_part = (
        r[f"{name}_{c}"] for name in ("unit_part", "held", "unit_total", "hidden", "down_part")
    )

    def tile(w_ref, col, width, start):
        p = jnp.dot(
            chunk_rows(r["stream"], at, CHUNKS[c]), w_ref[:, pl.ds(col, width)], preferred_element_type=F32
        )
        cols = pl.ds(start + col, width)
        part[:, :, :, :, cols] = p.astype(BF16).reshape(*part.shape[:4], width)

    for t in range(units // 256):
        tile(r["gate"], t * 256, 256, 0)
        tile(r["up"], t * 256, 256, units)
    if units % 256:
        tile(r["gate"], units // 256 * 256, units % 256, 0)
        tile(r["up"], units // 256 * 256, units % 256, units)
    yield [wires.copy(part.at[:, :, 1 - at.core], held, partner)]
    add_rows(held, [held, part.at[:, :, at.core]])
    yield from ring_scatter(
        wires,
        lambda i: held.at[:, i],
        total,
        r[f"from_left_{c}"],
        r[f"from_right_{c}"],
        NX,
        at.x,
        at.along_x,
    )
    for n in range(total.shape[0]):
        gate, up = total[n, :, pl.ds(0, units)], total[n, :, pl.ds(units, units)]
        hidden[n, at.x, at.core] = (jax.nn.silu(gate) * up).astype(BF16)
    handed = []

    def hand_over(i):
        ref = hidden.at[:, i, at.core]
        handed.append(wires.copy(ref, ref, partner))

    yield from ring_gather(
        wires, lambda i: hidden.at[:, i, at.core], NX, at.x, at.along_x, hand_over
    )
    yield handed

    def down(i, carry):
        cols = pl.ds(pl.multiple_of(i * 256, 256), 256)
        p = jnp.dot(
            hidden[...].reshape(-1, units), r["down"][:, cols], preferred_element_type=F32
        )
        down_part[:, :, :, cols] = p.astype(BF16).reshape(*down_part.shape[:3], 256)
        return carry

    lax.fori_loop(0, down_part.shape[-1] // 256, down, 0)
    produced(c)
    yield from ring_scatter(
        wires,
        lambda j: down_part.at[:, j, :, pl.ds(0, DOWN_SPLIT)],
        r[f"down_sum_{c}"],
        r[f"down_left_{c}"],
        r[f"down_right_{c}"],
        NY,
        at.y,
        at.along_y,
    )
    finished(c)


def normalize(values, gain):
    mean_square = jnp.mean(values * values, axis=-1, keepdims=True)
    return (values * lax.rsqrt(mean_square + epsilon) * gain).astype(BF16)


WEIGHTS = ("out", "key", "value", "query", "gate", "up", "down")


def layer_kernel(names, *refs):
    r = dict(zip(names, refs))
    at = Place()
    qkv_wires, wires = Wires(r["send"], r["recv"]), Wires(r["send"], r["recv_2"])
    steps = Steps()
    tokens = r["tokens"]
    local_rows, model = tokens.shape
    attended, mixed = r["streams"].at[0], r["streams"].at[1]
    cos, sin = r["cos"], r["sin"]

    phase = Phases()
    phase("greet")
    greeted = greet_group("cp", CP, at.cp) + greet_group("tp", TP, at.tp)
    loads = {}
    for n, name in enumerate(WEIGHTS):
        held = r["out"].at[at.y] if name == "out" else r[name]
        loads[name] = pltpu.make_async_copy(r[name + "_weight"], held, r["load"].at[n])
        loads[name].start()

    block = cos.shape[0]
    positions = at.cp * block + lax.broadcasted_iota(jnp.int32, (block, HD), 0)
    angles = positions.astype(F32) * r["inverse"][...]
    first_half = lax.broadcasted_iota(jnp.int32, (block, HD), 1) < HD // 2
    cos[...] = jnp.cos(angles)
    sin[...] = jnp.where(first_half, -jnp.sin(angles), jnp.sin(angles))

    normed = normalize(tokens[...].astype(F32), r["attention_gain"][...])
    slices, got, columns = r["slices"], r["got"], r["columns"]
    width = slices.shape[-1]
    for c in range(CP):
        slices[c] = normed[:, c * width : (c + 1) * width]
    phase("barrier")
    await_greetings(greeted)

    phase("spread_cp")
    weight_wires = Wires(r["send_w"], r["recv_w"])
    weight_ring = ring_gather(weight_wires, lambda j: r["out"].at[j], NY, at.y, at.along_y)
    weight_flights = []

    def out_weights():
        yield weight_flights
        yield advance(weight_ring)

    def keep_slice():
        loads["out"].wait()
        weight_flights.extend(advance(weight_ring))
        got[at.cp] = slices[at.cp]

    exchange(
        r["send"], r["recv_2"], lambda p: slices.at[p], lambda p: got.at[p], "cp", CP, at.cp, keep_slice
    )

    phase("spread_tp")
    def keep_columns():
        columns[at.tp] = got[...]

    exchange(
        r["send"], r["r0"], lambda p: got, lambda p: columns.at[p], "tp", TP, at.tp, keep_columns
    )
    phase("relayout")
    rows_in = r["rows_in"]

    def in_order(b, carry):
        parts = [columns[t, b].astype(F32) for t in range(TP)]
        rows_in[b] = jnp.concatenate(parts, axis=0).astype(BF16)
        return carry

    lax.fori_loop(0, CP, in_order, 0)

    part, summed, shared = r["qkv_part"], r["summed"], r["shared"]

    def x():
        return rows_in[...].reshape(-1, width)

    def turned(v):
        return (v * cos[...] + pltpu.roll(v, HD // 2, 1) * sin[...]).astype(BF16)

    def unit(n, out, parts, partial, prefix):
        start, extent, way = parts[n]
        bufs = [r[f"{prefix}{n}{m}"] for m in range(4)]
        return scatter_part(qkv_wires, at, partial, out, pl.ds(start, extent), way, bufs)

    def keys_and_values():
        yield from unit(0, summed, QKV_PARTS, part, "q")
        shared[at.z, at.y, :, pl.ds(0, HD)] = turned(summed[:, pl.ds(0, HD)])
        shared[at.z, at.y, :, pl.ds(HD, HD)] = summed[:, pl.ds(HD, HD)].astype(BF16)
        yield from gather_small(qkv_wires, at, shared)

    phase("qkv")
    loads["key"].wait()
    loads["value"].wait()
    product_into(part, x, r["key"], 0)
    product_into(part, x, r["value"], HD)
    steps.add(keys_and_values(), "k")
    loads["query"].wait()
    product_into(part, x, r["query"], 2 * HD)
    phase("qkv_sum")
    def query_part(letter):
        n = "KABC".index(letter)
        steps.add(unit(n, summed, QKV_PARTS, part, "q"), letter.lower())

    steps.play("C", query_part)
    steps.add(out_weights(), "o")
    steps.play(QKV_ORDER, query_part)
    steps.begun.clear()
    qkv_wires.drain()

    phase("attend")
    every = r["every"]
    heads = (summed.shape[1] - 2 * HD) // HD
    block = summed.shape[0]
    query = jnp.concatenate(
        [turned(summed[:, (2 + h) * HD : (3 + h) * HD]) for h in range(heads)], axis=0
    )
    keys = shared[:, :, :, 0:HD].reshape(-1, HD)
    values = shared[:, :, :, HD : 2 * HD].reshape(-1, HD)
    scores = lax.dot_general(
        query, keys, (((1,), (1,)), ((), ())), preferred_element_type=F32
    ) * HD ** (-0.5)
    key_at = lax.broadcasted_iota(jnp.int32, scores.shape, 1)
    query_at = lax.broadcasted_iota(jnp.int32, scores.shape, 0) % block + at.cp * block
    allowed = key_at <= query_at
    scores = jnp.where(allowed, scores, masked)
    top = jnp.max(scores, axis=-1, keepdims=True)
    weights = jnp.where(allowed, jnp.exp(scores - top), 0.0)
    total = jnp.sum(weights, axis=-1, keepdims=True)
    mean = jnp.dot(weights.astype(BF16), values, preferred_element_type=F32) / total
    mean = mean.astype(BF16)
    for h in range(heads):
        every[at.z, :, h * HD : (h + 1) * HD] = mean[h * block : (h + 1) * block]

    phase("gather_att")
    projected = r["projected"]
    owners, seen = [], set()

    def out_chunk(c):
        chunk = OUT_CHUNKS[c]
        part, arrived, total = r[f"out_part_{c}"], r[f"out_got_{c}"], r[f"out_total_{c}"]
        x = jnp.concatenate([every[(at.z + off) % NZ] for off in chunk], axis=0)
        for y in range(NY):
            p = jnp.dot(x, r["out"][y], preferred_element_type=F32)
            for n in range(len(chunk)):
                for t in range(TP):
                    first = n * block + t * local_rows
                    part[t, n, :, y * width : (y + 1) * width] = p[
                        first : first + local_rows
                    ].astype(BF16)
        copies = []
        for off in range(1, TP):
            to = (at.tp + off) % TP
            copies.append(wires.copy(part.at[to], arrived.at[at.tp], {"tp": to}))
        arrived[at.tp] = part[at.tp]
        yield copies
        for n, off in enumerate(chunk):
            sums = arrived[0, n].astype(F32)
            for t in range(1, TP):
                sums = sums + arrived[t, n].astype(F32)
            total[n] = sums.astype(BF16)
            if off == 0:
                projected[at.z] = total[n]
            else:
                to = at.along_z((at.z + off) % NZ)
                owners.append(wires.copy(total.at[n], projected.at[at.z], to))

    def att_there(off):
        seen.add(off)
        for c, chunk in OUT_CHUNKS.items():
            if off in chunk and seen >= set(chunk):
                steps.play("o2", None)
                steps.add(out_chunk(c), f"out{c}")

    steps.add(
        far_gather(wires, lambda i: every.at[i], NZ, at.z, at.along_z, att_there), "z"
    )
    steps.run()
    phase("out_cp")
    for c in owners:
        c.wait_recv()
    wires.drain()
    weight_wires.drain()
    phase("norm_feed")
    wide = projected.shape[-1]
    for z in range(NZ):
        cols = slice(z * wide, (z + 1) * wide)
        attended[:, cols] = (tokens[:, cols].astype(F32) + projected[z].astype(F32)).astype(BF16)

    normed = normalize(attended[...].astype(F32), r["feed_gain"][...])
    by_width, got_width, stream = r["by_width"], r["got_width"], r["stream"]
    wide = by_width.shape[-1]
    for t in range(TP):
        by_width[t] = normed[:, t * wide : (t + 1) * wide]

    phase("swap1")
    def keep_width():
        got_width[at.tp] = by_width[at.tp]

    exchange(
        r["send"],
        r["r1"],
        lambda p: by_width.at[p],
        lambda p: got_width.at[p],
        "tp",
        TP,
        at.tp,
        keep_width,
    )
    phase("gather_feed")
    stream[at.z, at.y] = jnp.concatenate(
        [got_width[t].astype(F32) for t in range(TP)], axis=0
    ).astype(BF16)
    for name in ("gate", "up", "down"):
        loads[name].wait()
    reduced = r["reduced"]
    places = {off: (c, n) for c, chunk in CHUNKS.items() for n, off in enumerate(chunk)}

    def piece(name, off):
        c, n = places[off]
        return r[f"{name}_{c}"].at[n]

    def to_z(off):
        return at.along_z((at.z + off) % NZ)

    lines = FarScatter(
        qkv_wires,
        lambda off: piece("down_sum", off),
        reduced.at[:, pl.ds(0, DOWN_SPLIT)],
        r["down_far"],
        to_z,
    )
    rest = pl.ds(DOWN_SPLIT, reduced.shape[1] - DOWN_SPLIT)
    z_lines = FarScatter(
        qkv_wires,
        lambda off: piece("down_part", off).at[:, :, rest],
        r["z_sum"],
        r["z_far"],
        to_z,
    )
    there = {}

    def produced(c):
        for off in CHUNKS[c]:
            z_lines.send(off)

    def finished(c):
        for off in CHUNKS[c]:
            lines.send(off)

    def z_first_end():
        yield from z_lines.last_round()
        yield from ring_scatter(
            qkv_wires,
            lambda j: r["z_sum"].at[j],
            reduced.at[:, rest],
            r["z_left"],
            r["z_right"],
            NY,
            at.y,
            at.along_y,
        )

    later = {
        "T": lambda: lines.turns("l"),
        "U": lambda: lines.turns("r"),
        "V": lambda: z_lines.turns("l"),
        "W": lambda: z_lines.turns("r"),
        "N": z_first_end,
        "L": lines.last_round,
    }

    def begin(letter):
        if letter in later:
            gen = later[letter]()
        else:
            assert letter.lower() in there
            gen = feed_chunk(qkv_wires, at, r, letter.lower(), produced, finished)
        steps.add(gen, letter.lower())

    def chunk_there(c):
        there[c] = True
        return iter(())

    gather_rows(qkv_wires, steps, at, stream, GATHER_SPLIT, CHUNKS, chunk_there)
    steps.play(GATHER_ORDER, begin)
    assert len(there) == len(CHUNKS)
    steps.play(ORDER, begin)
    assert not steps.queue
    phase("swap2")
    qkv_wires.drain()
    by_token, lowered = r["by_token"], r["lowered"]
    for t in range(TP):
        by_token[t] = reduced[pl.ds(t * local_rows, local_rows), :].astype(BF16)

    def keep_token():
        lowered[at.tp] = by_token[at.tp]

    exchange(
        r["send"],
        r["r0"],
        lambda p: by_token.at[p],
        lambda p: lowered.at[p],
        "tp",
        TP,
        at.tp,
        keep_token,
    )
    for t in range(TP):
        cols = slice(t * wide, (t + 1) * wide)
        mixed[:, cols] = (attended[:, cols].astype(F32) + lowered[t].astype(F32)).astype(BF16)
    phase(None)


VMEM = pl.BlockSpec(memory_space=pltpu.VMEM)
ANY = pl.BlockSpec(memory_space=pl.ANY)
COPIES, COPIES_2, SLOTS = 157, CP, 48


def dma(count):
    return pltpu.SemaphoreType.DMA((count,))


def on_device(
    tokens,
    attention_gain,
    query_weight,
    key_weight,
    value_weight,
    out_weight,
    feed_gain,
    gate_weight,
    up_weight,
    down_weight,
):
    local_rows, model = tokens.shape
    block = local_rows * TP
    rows = block * CP
    qkv = query_weight.shape[1] + key_weight.shape[1] + value_weight.shape[1]
    units = gate_weight.shape[1]
    wide, width = model // TP, model // CP

    pair = jnp.arange(HD, dtype=F32)[None] % (HD // 2)
    inverse = rope_base ** (-(pair * 2.0 / HD))

    inputs = {
        "tokens": tokens,
        "attention_gain": attention_gain[None],
        "feed_gain": feed_gain[None],
        "inverse": inverse,
        "key_weight": key_weight,
        "value_weight": value_weight,
        "query_weight": query_weight,
        "out_weight": out_weight,
        "gate_weight": gate_weight,
        "up_weight": up_weight,
        "down_weight": down_weight,
    }

    def buf(*shape, kind=BF16):
        return pltpu.VMEM(shape, kind)

    scratch = {name: buf(*inputs[name + "_weight"].shape) for name in WEIGHTS}
    scratch |= {
        "cos": buf(block, HD, kind=F32),
        "sin": buf(block, HD, kind=F32),
        "slices": buf(CP, local_rows, width),
        "got": buf(CP, local_rows, width),
        "columns": buf(TP, CP, local_rows, width),
        "rows_in": buf(CP, block, width),
        "qkv_part": buf(NZ, NY, block, qkv),
        "summed": buf(block, qkv, kind=F32),
        "shared": buf(NZ, NY, block, 2 * HD),
        "every": buf(NZ, block, wide),
        "projected": buf(NZ, local_rows, wide),
        "by_width": buf(TP, local_rows, wide),
        "got_width": buf(TP, local_rows, wide),
        "stream": buf(NZ, NY, block, wide),
        "down_far": buf(8, block, DOWN_SPLIT),
        "z_far": buf(8, NY, block, wide - DOWN_SPLIT),
        "z_sum": buf(NY, block, wide - DOWN_SPLIT),
        "z_left": buf(NY // 2, block, wide - DOWN_SPLIT),
        "z_right": buf(NY // 2, block, wide - DOWN_SPLIT),
        "reduced": buf(block, wide, kind=F32),
        "by_token": buf(TP, local_rows, wide),
        "lowered": buf(TP, local_rows, wide),
    }
    scratch["out"] = buf(NY, *out_weight.shape)
    for c, chunk in OUT_CHUNKS.items():
        scratch |= {
            f"out_part_{c}": buf(TP, len(chunk), local_rows, wide),
            f"out_got_{c}": buf(TP, len(chunk), local_rows, wide),
            f"out_total_{c}": buf(len(chunk), local_rows, wide),
        }
    for c, chunk in CHUNKS.items():
        n, half = len(chunk), block // 2
        scratch |= {
            f"unit_part_{c}": buf(n, NX, 2, half, 2 * units),
            f"held_{c}": buf(n, NX, half, 2 * units),
            f"from_left_{c}": buf(NX // 2, n, half, 2 * units),
            f"from_right_{c}": buf(NX // 2, n, half, 2 * units),
            f"unit_total_{c}": buf(n, half, 2 * units, kind=F32),
            f"hidden_{c}": buf(n, NX, 2, half, units),
            f"down_part_{c}": buf(n, NY, block, wide),
            f"down_left_{c}": buf(NY // 2, n, block, DOWN_SPLIT),
            f"down_right_{c}": buf(NY // 2, n, block, DOWN_SPLIT),
            f"down_sum_{c}": buf(n, block, DOWN_SPLIT),
        }
    scratch |= scatter_scratch("q", QKV_PARTS, block)
    scratch |= {f"r{n}": dma(TP) for n in range(2)}
    scratch |= {"load": dma(len(WEIGHTS)), "send": dma(SLOTS), "recv": dma(COPIES)}
    scratch |= {"recv_2": dma(COPIES_2), "send_w": dma(4), "recv_w": dma(4)}

    names = (*inputs, "streams", *scratch)
    streams = pl.pallas_call(
        functools.partial(layer_kernel, names),
        out_shape=jax.ShapeDtypeStruct((2, *tokens.shape), BF16),
        in_specs=[ANY if name.endswith("_weight") else VMEM for name in inputs],
        out_specs=VMEM,
        scratch_shapes=list(scratch.values()),
        compiler_params=pltpu.CompilerParams(
            collective_id=0,
            has_side_effects=True,
            vmem_limit_bytes=60 * 1024 * 1024,
        ),
        name="layer",
    )(*inputs.values())
    return streams[0], streams[1]


def solution(mesh):
    in_specs = (
        P(("cp", "tp"), None),
        P(),
        P("cp", "tp"),
        P("cp", "tp"),
        P("cp", "tp"),
        P("tp", "cp"),
        P(),
        P("tp", "cp"),
        P("tp", "cp"),
        P("cp", "tp"),
    )
    out_specs = (P(("cp", "tp"), None), P(("cp", "tp"), None))
    return jax.shard_map(
        on_device, mesh=mesh, in_specs=in_specs, out_specs=out_specs, check_vma=False
    )
```

```python
import collections
import functools

import jax
import jax.numpy as jnp
from jax import lax
from jax.experimental import pallas as pl
from jax.experimental.pallas import tpu as pltpu
from jax.sharding import PartitionSpec as P

HD = 128
NZ, NY, NX = 8, 4, 4
CP, TP = NZ * NY, NX * 2
MESH = pl.DeviceIdType.MESH
F32, BF16 = jnp.float32, jnp.bfloat16

epsilon = 1e-05
rope_base = 500000.0
masked = -1e30


class Wires:
    def __init__(self, send, recv):
        self.send, self.recv, self.used, self.sent = send, recv, 0, []

    def copy(self, src, dst, device):
        i, slots = self.used, self.send.shape[0]
        self.used += 1
        assert i < self.recv.shape[0]
        if i >= slots:
            self.sent[i - slots].wait_send()
        c = pltpu.make_async_remote_copy(
            src_ref=src,
            dst_ref=dst,
            send_sem=self.send.at[i % slots],
            recv_sem=self.recv.at[i],
            device_id=device,
            device_id_type=MESH,
        )
        c.start()
        self.sent.append(c)
        return c

    def drain(self):
        for c in self.sent[-self.send.shape[0] :]:
            c.wait_send()
        self.sent, self.used = [], 0


class Now(list):
    pass


def advance(gen):
    needs = next(gen, None)
    while isinstance(needs, Now):
        for c in needs:
            c.wait_recv()
        needs = next(gen, None)
    return needs


class Steps:
    def __init__(self):
        self.queue, self.begun = collections.deque(), set()

    def add(self, gen, name="line", step=0):
        with jax.named_scope(f"{name}_{step}"):
            needs = advance(gen)
        if needs is not None:
            self.queue.append((needs, gen, name, step + 1))

    def go_on(self, entry):
        needs, gen, name, step = entry
        with jax.named_scope(f"wait_{name}_{step}"):
            for c in needs:
                c.wait_recv()
        self.add(gen, name, step)

    def run(self, until=lambda: False):
        while self.queue and not until():
            self.go_on(self.queue.popleft())

    def play(self, order, begin):
        for word in order.split():
            if word.isupper():
                if word not in self.begun:
                    self.begun.add(word)
                    begin(word)
                continue
            name, step = word.split("/") if "/" in word else (word[0], word[1:])
            step = int(step)
            while True:
                found = [i for i, e in enumerate(self.queue) if e[2] == name]
                if not found or self.queue[found[0]][3] > step:
                    break
                entry = self.queue[found[0]]
                del self.queue[found[0]]
                self.go_on(entry)


class Phases:
    def __init__(self):
        self.scope = None

    def __call__(self, name):
        if self.scope:
            self.scope.__exit__(None, None, None)
        self.scope = jax.named_scope(name) if name else None
        if self.scope:
            self.scope.__enter__()


class Place:
    def __init__(self):
        self.cp, self.tp = lax.axis_index("cp"), lax.axis_index("tp")
        self.z, self.y = self.cp // NY, self.cp % NY
        self.x, self.core = self.tp // 2, self.tp % 2

    def along_z(self, z):
        return {"cp": z * NY + self.y}

    def along_y(self, y):
        return {"cp": self.z * NY + y}

    def along_x(self, x):
        return {"tp": x * 2 + self.core}

    def partner(self):
        return {"tp": self.x * 2 + 1 - self.core}


def ring(n, me, device_of):
    return device_of((me + 1) % n), device_of((me + n - 1) % n)


def greet(devices):
    barrier = pltpu.get_barrier_semaphore()
    for device in devices:
        pl.semaphore_signal(barrier, inc=1, device_id=device, device_id_type=MESH)
    return len(devices)


def greet_group(axis, n, me):
    barrier = pltpu.get_barrier_semaphore()

    def signal(off, carry):
        pl.semaphore_signal(
            barrier, inc=1, device_id={axis: (me + off) % n}, device_id_type=MESH
        )
        return carry

    lax.fori_loop(1, n, signal, 0)
    return n - 1


def await_greetings(count):
    pl.semaphore_wait(pltpu.get_barrier_semaphore(), count)


def half_of(ref, h):
    d = ref.shape[0] // 2
    if d:
        return ref.at[pl.ds(h * d, d)]
    width = ref.shape[-1]
    d = -(-width // 256) * 128
    cols = pl.ds(0, d) if h == 0 else pl.ds(d, width - d)
    return ref.at[(slice(None),) * (len(ref.shape) - 1) + (cols,)]


def ring_gather(wires, block, n, me, device_of, arrived=None):
    right, left = ring(n, me, device_of)
    last = n // 2 - 1

    def send(k):
        r, l = block((me + n - k) % n), block((me + k) % n)
        if k == last:
            r, l = half_of(r, 0), half_of(l, 1)
        return wires.copy(r, r, right), wires.copy(l, l, left)

    flying = send(0)
    if arrived:
        arrived(me)
    for k in range(1, n // 2 + 1):
        yield flying
        if k <= last:
            flying = send(k)
            if arrived:
                arrived((me + n - k) % n)
                arrived((me + k) % n)
        elif arrived:
            arrived((me + n // 2) % n)


def add_rows(dst, terms, finish=None):
    if len(dst.shape) > 2:
        for i in range(dst.shape[0]):
            add_rows(dst.at[i], [t.at[i] for t in terms])
        return
    rows = dst.shape[0]
    step = min(rows, 16)

    def body(i, carry):
        at = pl.ds(pl.multiple_of(i * step, step), step)
        total = terms[0][at, :].astype(F32)
        for t in terms[1:]:
            total = total + t[at, :].astype(F32)
        dst[at, :] = total.astype(dst.dtype)
        return carry

    lax.fori_loop(0, rows // step, body, 0)


def ring_scatter(wires, own, out, from_left, from_right, n, me, device_of):
    right, left = ring(n, me, device_of)
    m = n // 2
    far = own((me + m) % n)
    r = wires.copy(half_of(far, 0), half_of(from_left.at[0], 0), right)
    l = wires.copy(half_of(far, 1), half_of(from_right.at[0], 1), left)
    for k in range(1, m):
        to_right, to_left = own((me + m - k) % n), own((me + n - m + k) % n)
        got_left, got_right = from_left.at[k - 1], from_right.at[k - 1]
        yield [r]
        if k == 1:
            add_rows(half_of(got_left, 0), [half_of(got_left, 0), half_of(to_right, 0)])
            add_rows(half_of(got_left, 1), [half_of(to_right, 1)])
        else:
            add_rows(got_left, [got_left, to_right])
        r = wires.copy(got_left, from_left.at[k], right)
        yield Now([l])
        if k == 1:
            add_rows(half_of(got_right, 1), [half_of(got_right, 1), half_of(to_left, 1)])
            add_rows(half_of(got_right, 0), [half_of(to_left, 0)])
        else:
            add_rows(got_right, [got_right, to_left])
        l = wires.copy(got_right, from_right.at[k], left)
    yield [r, l]
    add_rows(out, [own(me), from_left.at[m - 1], from_right.at[m - 1]])


def far_gather(wires, block, n, me, device_of, arrived):
    def send(ref, off):
        return wires.copy(ref, ref, device_of((me + n + off) % n))

    def whole(off):
        return block((me + n + off) % n)

    own = block(me)
    p2, m2, p1, m1 = send(own, 2), send(own, -2), send(own, 1), send(own, -1)
    arrived(0)
    yield [p2]
    p3, p4 = send(whole(-2), 1), send(half_of(whole(-2), 0), 2)
    yield Now([m2])
    m3, m4 = send(whole(2), -1), send(half_of(whole(2), 1), -2)
    yield Now([p1])
    arrived(7)
    yield Now([m1])
    for off in (1, 6, 2):
        arrived(off)
    yield [p3]
    arrived(5)
    yield Now([m3])
    arrived(3)
    yield Now([p4, m4])
    arrived(4)


def far_scatter(wires, own, out, bufs, n, me, device_of):
    lines = FarScatter(
        wires,
        lambda off: own((me + off) % n),
        out,
        bufs,
        lambda off: device_of((me + off) % n),
    )
    for off in (4, 3, 5, 1, 7):
        lines.send(off)
    yield from lines.turns("l")
    other = lines.turns("r")
    yield Now(next(other))
    next(other, None)
    yield from lines.last_round()


class FarScatter:
    def __init__(self, wires, own, out, bufs, device_of):
        self.wires, self.own, self.out, self.device_of = wires, own, out, device_of
        self.bufs, self.sent = bufs, {}

    def copy(self, name, src, dst, off):
        self.sent[name] = self.wires.copy(src, dst, self.device_of(off))

    def send(self, off):
        near_l, near_r, turn_l, turn_r, far_l, far_r = [self.bufs.at[i] for i in range(6)]
        term = self.own(off)
        if off == 1:
            self.copy("near_l", term, near_l, 1)
        elif off == 7:
            self.copy("near_r", term, near_r, 7)
        elif off == 3:
            self.copy("turn_l", term, turn_l, 1)
        elif off == 5:
            self.copy("turn_r", term, turn_r, 7)
        elif off == 4:
            self.copy("far_l", half_of(term, 0), half_of(far_l, 0), 2)
            self.copy("far_r", half_of(term, 1), half_of(far_r, 1), 6)

    def turn(self, side):
        n, off, full = (0, 2, 0) if side == "l" else (1, 6, 1)
        turn, far, into = self.bufs.at[2 + n], self.bufs.at[4 + n], self.bufs.at[6 + n]
        mine = self.own(off)
        add_rows(half_of(turn, full), [half_of(x, full) for x in (turn, far, mine)])
        add_rows(half_of(turn, 1 - full), [half_of(x, 1 - full) for x in (turn, mine)])
        self.copy("sum_" + side, turn, into, off)

    def turns(self, side):
        yield [self.sent["turn_" + side], self.sent["far_" + side]]
        self.turn(side)

    def last_round(self):
        yield [self.sent[n] for n in ("near_l", "near_r", "sum_l", "sum_r")]
        near_l, near_r, sum_l, sum_r = [self.bufs.at[i] for i in (0, 1, 6, 7)]
        add_rows(self.out, [self.own(0), near_l, near_r, sum_l, sum_r])


def exchange(send_sem, recv_sem, source, target, axis, n, me, meanwhile=None):
    def copy(off):
        peer = (me + off) % n
        return pltpu.make_async_remote_copy(
            src_ref=source(peer),
            dst_ref=target(me),
            send_sem=send_sem.at[off],
            recv_sem=recv_sem.at[off],
            device_id=axis(peer) if callable(axis) else {axis: peer},
            device_id_type=MESH,
        )

    def start(off, carry):
        copy(off).start()
        return carry

    def wait(off, carry):
        copy(off).wait()
        return carry

    lax.fori_loop(1, n, start, 0)
    if meanwhile:
        meanwhile()
    lax.fori_loop(1, n, wait, 0)


QKV_PARTS = ((0, 256), (256, 512), (768, 512))
QKV_ORDER = "g2 K k1 q1 O p2 A k2 q2 B a1 k3 b1 o1 H a2 b2 k4"
GATHER_SPLIT = 768
DOWN_SPLIT = 768


CHUNKS = {"e": (0,), "b": (2, 6), "c": (3, 4), "d": (5,), "a": (1, 7)}
OUT_CHUNKS = {0: (0, 7, 1, 6, 2), 1: (5, 3, 4)}


def gather_rows(wires, steps, at, out_ref, split, chunks, ready):
    first, rest = pl.ds(0, split), pl.ds(split, out_ref.shape[-1] - split)
    seen = collections.Counter()

    def z_at(off):
        return (at.z + off) % NZ

    def mark(off):
        seen[off] += 1
        for c, chunk in chunks.items():
            if off in chunk and all(seen[o] == 2 for o in chunk):
                steps.add(ready(c), f"chunk{c}")

    def y_first():
        yield from ring_gather(
            wires, lambda j: out_ref.at[at.z, j, :, rest], NY, at.y, at.along_y
        )
        yield from far_gather(
            wires, lambda i: out_ref.at[i, :, :, rest], NZ, at.z, at.along_z, mark
        )

    def to_y(off):
        def line():
            yield from ring_gather(
                wires, lambda j: out_ref.at[z_at(off), j, :, first], NY, at.y, at.along_y
            )
            mark(off)

        steps.add(line(), f"y{off}")

    steps.add(y_first(), "yz")
    steps.add(
        far_gather(
            wires, lambda i: out_ref.at[i, at.y, :, first], NZ, at.z, at.along_z, to_y
        ),
        "z",
    )


def gather_small(wires, at, ref):
    handed = []

    def to_y(block):
        for off in (1, 3, 2):
            handed.append(wires.copy(block, block, at.along_y((at.y + off) % NY)))

    own = ref.at[at.z, at.y]
    order = (4, 3, 5, 2, 6, 1, 7)
    copies = {off: wires.copy(own, own, at.along_z((at.z + off) % NZ)) for off in order}
    to_y(own)
    yield []
    for off in (1, 7, 2, 6, 3, 5, 4):
        yield Now([copies[off]])
        to_y(ref.at[(at.z + NZ - off) % NZ, at.y])
    yield handed


def chunk_rows(ref, at, chunk):
    blocks = [ref[(at.z + off) % NZ] for off in chunk]
    return jnp.concatenate([b.reshape(-1, b.shape[-1]) for b in blocks], axis=0)


GATHER_ORDER = """yz/1 y0/1 z/1 yz/2 y0/2 E y7/1 y1/1 e1 y6/1 y2/1 z/2 yz/3 y7/2 e2 y1/2 y6/2 y2/2 B y5/1 y3/1 y4/1 yz/4 b1 e3 y5/2 y3/2 e4 y4/2"""
ORDER = """b2 C D c1 d1 A b3 a1 c2 d2 b4 e5 a2 c3 d3 b5 e6 a3 b6 c4 d4 e7 a4 c5 c6 b7 d5 d6 a5 a6 e8 b8 c7 V v1 W w1 d7 a7 c8 d8 T U a8 N n1 t1 u1 n2 L l1 n3"""


def feed_chunk(wires, at, r, c, produced, finished):
    partner = at.partner()
    units = r["gate"].shape[1]
    part, held, total, hidden, down_part = (
        r[f"{name}_{c}"] for name in ("unit_part", "held", "unit_total", "hidden", "down_part")
    )

    def tile(w_ref, col, width, start):
        p = jnp.dot(
            chunk_rows(r["stream"], at, CHUNKS[c]), w_ref[:, pl.ds(col, width)], preferred_element_type=F32
        )
        cols = pl.ds(start + col, width)
        part[:, :, :, :, cols] = p.astype(BF16).reshape(*part.shape[:4], width)

    for t in range(units // 256):
        tile(r["gate"], t * 256, 256, 0)
        tile(r["up"], t * 256, 256, units)
    if units % 256:
        tile(r["gate"], units // 256 * 256, units % 256, 0)
        tile(r["up"], units // 256 * 256, units % 256, units)
    yield [wires.copy(part.at[:, :, 1 - at.core], held, partner)]
    add_rows(held, [held, part.at[:, :, at.core]])
    yield from ring_scatter(
        wires,
        lambda i: held.at[:, i],
        total,
        r[f"from_left_{c}"],
        r[f"from_right_{c}"],
        NX,
        at.x,
        at.along_x,
    )
    for n in range(total.shape[0]):
        gate, up = total[n, :, pl.ds(0, units)], total[n, :, pl.ds(units, units)]
        hidden[n, at.x, at.core] = (jax.nn.silu(gate) * up).astype(BF16)
    handed = []

    def hand_over(i):
        ref = hidden.at[:, i, at.core]
        handed.append(wires.copy(ref, ref, partner))

    yield from ring_gather(
        wires, lambda i: hidden.at[:, i, at.core], NX, at.x, at.along_x, hand_over
    )
    yield handed

    def down(i, carry):
        cols = pl.ds(pl.multiple_of(i * 256, 256), 256)
        p = jnp.dot(
            hidden[...].reshape(-1, units), r["down"][:, cols], preferred_element_type=F32
        )
        down_part[:, :, :, cols] = p.astype(BF16).reshape(*down_part.shape[:3], 256)
        return carry

    lax.fori_loop(0, down_part.shape[-1] // 256, down, 0)
    produced(c)
    yield from ring_scatter(
        wires,
        lambda j: down_part.at[:, j, :, pl.ds(0, DOWN_SPLIT)],
        r[f"down_sum_{c}"],
        r[f"down_left_{c}"],
        r[f"down_right_{c}"],
        NY,
        at.y,
        at.along_y,
    )
    finished(c)


def normalize(values, gain):
    mean_square = jnp.mean(values * values, axis=-1, keepdims=True)
    return (values * lax.rsqrt(mean_square + epsilon) * gain).astype(BF16)


WEIGHTS = ("key", "value", "query", "out", "gate", "up", "down")
ALONG_Y = ("key", "value", "query", "out")


def layer_kernel(names, *refs):
    r = dict(zip(names, refs))
    at = Place()
    qkv_wires, wires = Wires(r["send"], r["recv"]), Wires(r["send"], r["recv_2"])
    steps = Steps()
    tokens = r["tokens"]
    local_rows, model = tokens.shape
    attended, mixed = r["streams"].at[0], r["streams"].at[1]
    cos, sin = r["cos"], r["sin"]

    phase = Phases()
    phase("greet")
    greeted = greet_group("cp", CP, at.cp) + greet_group("tp", TP, at.tp)
    loads = {}
    for n, name in enumerate(WEIGHTS):
        held = r[name].at[at.y] if name in ALONG_Y else r[name]
        loads[name] = pltpu.make_async_copy(r[name + "_weight"], held, r["load"].at[n])
        loads[name].start()

    block = cos.shape[0]
    positions = at.cp * block + lax.broadcasted_iota(jnp.int32, (block, HD), 0)
    angles = positions.astype(F32) * r["inverse"][...]
    first_half = lax.broadcasted_iota(jnp.int32, (block, HD), 1) < HD // 2
    cos[...] = jnp.cos(angles)
    sin[...] = jnp.where(first_half, -jnp.sin(angles), jnp.sin(angles))

    normed = normalize(tokens[...].astype(F32), r["attention_gain"][...])
    slices, got, columns = r["slices"], r["got"], r["columns"]
    wide = slices.shape[-1]
    for z in range(NZ):
        slices[z] = normed[:, z * wide : (z + 1) * wide]
    phase("barrier")
    await_greetings(greeted)

    phase("spread_cp")
    weight_wires = Wires(r["send_w"], r["recv_w"])
    query_cols, out_cols = r["query"].shape[-1] // 2, r["out"].shape[-1] // 2

    def gathered(*blocks):
        rings = [ring_gather(weight_wires, b, NY, at.y, at.along_y) for b in blocks]
        while True:
            flights = [advance(g) for g in rings]
            if flights[0] is None:
                return
            yield [c for some in flights for c in some]

    weight_parts = {
        "G": lambda: gathered(lambda j: r["key"].at[j], lambda j: r["value"].at[j]),
        "P": lambda: gathered(lambda j: r["query"].at[j, :, pl.ds(0, query_cols)]),
        "Q": lambda: gathered(lambda j: r["query"].at[j, :, pl.ds(query_cols, query_cols)]),
        "O": lambda: gathered(lambda j: r["out"].at[j, :, pl.ds(0, out_cols)]),
        "H": lambda: gathered(lambda j: r["out"].at[j, :, pl.ds(out_cols, out_cols)]),
    }

    def begin_weights(letter):
        steps.add(weight_parts[letter](), letter.lower())

    def keep_slice():
        for name in ALONG_Y:
            loads[name].wait()
        steps.play("G P", begin_weights)
        got[at.z] = slices[at.z]

    exchange(
        r["send"], r["recv_2"], lambda p: slices.at[p], lambda p: got.at[p], at.along_z, NZ, at.z, keep_slice
    )
    steps.play("g1 Q", begin_weights)

    phase("spread_tp")
    def keep_columns():
        columns[at.tp] = got[...]

    exchange(
        r["send"], r["r0"], lambda p: got, lambda p: columns.at[p], "tp", TP, at.tp, keep_columns
    )
    phase("relayout")
    rows_in = r["rows_in"]

    def in_order(b, carry):
        parts = [columns[t, b].astype(F32) for t in range(TP)]
        rows_in[b] = jnp.concatenate(parts, axis=0).astype(BF16)
        return carry

    steps.play("p1", begin_weights)
    lax.fori_loop(0, NZ, in_order, 0)

    part, summed, shared = r["qkv_part"], r["summed"], r["shared"]

    def product(name, cols, start):
        x = rows_in[...].reshape(-1, wide)
        w = r[name][:, :, cols].reshape(wide, -1)
        p = jnp.dot(x, w, preferred_element_type=F32)
        part[:, :, start : start + p.shape[1]] = p.astype(BF16).reshape(NZ, block, -1)

    def turned(v):
        return (v * cos[...] + pltpu.roll(v, HD // 2, 1) * sin[...]).astype(BF16)

    def unit(n):
        start, extent = QKV_PARTS[n]
        cols = pl.ds(start, extent)
        return far_scatter(
            qkv_wires,
            lambda i: part.at[i, :, cols],
            summed.at[:, cols],
            r[f"sum_{n}"],
            NZ,
            at.z,
            at.along_z,
        )

    def keys_and_values():
        yield from unit(0)
        shared[at.z, at.y, :, pl.ds(0, HD)] = turned(summed[:, pl.ds(0, HD)])
        shared[at.z, at.y, :, pl.ds(HD, HD)] = summed[:, pl.ds(HD, HD)].astype(BF16)
        yield from gather_small(qkv_wires, at, shared)

    def begin_part(letter):
        if letter == "K":
            product("key", slice(None), 0)
            product("value", slice(None), HD)
            steps.add(keys_and_values(), "k")
        elif letter in "AB":
            n = "KAB".index(letter)
            start, extent = QKV_PARTS[n]
            for col in range(0, extent, 256):
                at_col = start - 2 * HD + col
                product("query", slice(at_col, at_col + 256), start + col)
            steps.add(unit(n), letter.lower())
        else:
            begin_weights(letter)

    phase("qkv_sum")
    steps.play(QKV_ORDER, begin_part)
    steps.begun.clear()
    qkv_wires.drain()

    phase("attend")
    every = r["every"]
    heads = (summed.shape[1] - 2 * HD) // HD
    block = summed.shape[0]
    query = jnp.concatenate(
        [turned(summed[:, (2 + h) * HD : (3 + h) * HD]) for h in range(heads)], axis=0
    )
    keys = shared[:, :, :, 0:HD].reshape(-1, HD)
    values = shared[:, :, :, HD : 2 * HD].reshape(-1, HD)
    scores = lax.dot_general(
        query, keys, (((1,), (1,)), ((), ())), preferred_element_type=F32
    ) * HD ** (-0.5)
    key_at = lax.broadcasted_iota(jnp.int32, scores.shape, 1)
    query_at = lax.broadcasted_iota(jnp.int32, scores.shape, 0) % block + at.cp * block
    allowed = key_at <= query_at
    scores = jnp.where(allowed, scores, masked)
    top = jnp.max(scores, axis=-1, keepdims=True)
    weights = jnp.where(allowed, jnp.exp(scores - top), 0.0)
    total = jnp.sum(weights, axis=-1, keepdims=True)
    mean = jnp.dot(weights.astype(BF16), values, preferred_element_type=F32) / total
    mean = mean.astype(BF16)
    for h in range(heads):
        every[at.z, :, h * HD : (h + 1) * HD] = mean[h * block : (h + 1) * block]

    phase("gather_att")
    projected = r["projected"]
    owners, seen = [], set()

    def out_chunk(c):
        chunk = OUT_CHUNKS[c]
        part, arrived, total = r[f"out_part_{c}"], r[f"out_got_{c}"], r[f"out_total_{c}"]
        x = jnp.concatenate([every[(at.z + off) % NZ] for off in chunk], axis=0)
        cols = r["out"].shape[-1]
        for y in range(NY):
            p = jnp.dot(x, r["out"][y], preferred_element_type=F32)
            for n in range(len(chunk)):
                for t in range(TP):
                    first = n * block + t * local_rows
                    part[t, n, :, y * cols : (y + 1) * cols] = p[
                        first : first + local_rows
                    ].astype(BF16)
        copies = []
        for off in range(1, TP):
            to = (at.tp + off) % TP
            copies.append(wires.copy(part.at[to], arrived.at[at.tp], {"tp": to}))
        arrived[at.tp] = part[at.tp]
        yield copies
        for n, off in enumerate(chunk):
            sums = arrived[0, n].astype(F32)
            for t in range(1, TP):
                sums = sums + arrived[t, n].astype(F32)
            total[n] = sums.astype(BF16)
            if off == 0:
                projected[at.z] = total[n]
            else:
                to = at.along_z((at.z + off) % NZ)
                owners.append(wires.copy(total.at[n], projected.at[at.z], to))

    def att_there(off):
        seen.add(off)
        for c, chunk in OUT_CHUNKS.items():
            if off in chunk and seen >= set(chunk):
                steps.play("o2 h1 h2", None)
                steps.add(out_chunk(c), f"out{c}")

    steps.add(
        far_gather(wires, lambda i: every.at[i], NZ, at.z, at.along_z, att_there), "z"
    )
    steps.play("h1 z/1 z/2", None)
    steps.run()
    phase("out_cp")
    for c in owners:
        c.wait_recv()
    wires.drain()
    weight_wires.drain()
    phase("norm_feed")
    wide = projected.shape[-1]
    for z in range(NZ):
        cols = slice(z * wide, (z + 1) * wide)
        attended[:, cols] = (tokens[:, cols].astype(F32) + projected[z].astype(F32)).astype(BF16)

    normed = normalize(attended[...].astype(F32), r["feed_gain"][...])
    by_width, got_width, stream = r["by_width"], r["got_width"], r["stream"]
    wide = by_width.shape[-1]
    for t in range(TP):
        by_width[t] = normed[:, t * wide : (t + 1) * wide]

    phase("swap1")
    def keep_width():
        got_width[at.tp] = by_width[at.tp]

    exchange(
        r["send"],
        r["r1"],
        lambda p: by_width.at[p],
        lambda p: got_width.at[p],
        "tp",
        TP,
        at.tp,
        keep_width,
    )
    phase("gather_feed")
    stream[at.z, at.y] = jnp.concatenate(
        [got_width[t].astype(F32) for t in range(TP)], axis=0
    ).astype(BF16)
    for name in ("gate", "up", "down"):
        loads[name].wait()
    reduced = r["reduced"]
    places = {off: (c, n) for c, chunk in CHUNKS.items() for n, off in enumerate(chunk)}

    def piece(name, off):
        c, n = places[off]
        return r[f"{name}_{c}"].at[n]

    def to_z(off):
        return at.along_z((at.z + off) % NZ)

    lines = FarScatter(
        qkv_wires,
        lambda off: piece("down_sum", off),
        reduced.at[:, pl.ds(0, DOWN_SPLIT)],
        r["down_far"],
        to_z,
    )
    rest = pl.ds(DOWN_SPLIT, reduced.shape[1] - DOWN_SPLIT)
    z_lines = FarScatter(
        qkv_wires,
        lambda off: piece("down_part", off).at[:, :, rest],
        r["z_sum"],
        r["z_far"],
        to_z,
    )
    there = {}

    def produced(c):
        for off in CHUNKS[c]:
            z_lines.send(off)

    def finished(c):
        for off in CHUNKS[c]:
            lines.send(off)

    def z_first_end():
        yield from z_lines.last_round()
        yield from ring_scatter(
            qkv_wires,
            lambda j: r["z_sum"].at[j],
            reduced.at[:, rest],
            r["z_left"],
            r["z_right"],
            NY,
            at.y,
            at.along_y,
        )

    later = {
        "T": lambda: lines.turns("l"),
        "U": lambda: lines.turns("r"),
        "V": lambda: z_lines.turns("l"),
        "W": lambda: z_lines.turns("r"),
        "N": z_first_end,
        "L": lines.last_round,
    }

    def begin(letter):
        if letter in later:
            gen = later[letter]()
        else:
            assert letter.lower() in there
            gen = feed_chunk(qkv_wires, at, r, letter.lower(), produced, finished)
        steps.add(gen, letter.lower())

    def chunk_there(c):
        there[c] = True
        return iter(())

    gather_rows(qkv_wires, steps, at, stream, GATHER_SPLIT, CHUNKS, chunk_there)
    steps.play(GATHER_ORDER, begin)
    assert len(there) == len(CHUNKS)
    steps.play(ORDER, begin)
    assert not steps.queue
    phase("swap2")
    qkv_wires.drain()
    by_token, lowered = r["by_token"], r["lowered"]
    for t in range(TP):
        by_token[t] = reduced[pl.ds(t * local_rows, local_rows), :].astype(BF16)

    def keep_token():
        lowered[at.tp] = by_token[at.tp]

    exchange(
        r["send"],
        r["r0"],
        lambda p: by_token.at[p],
        lambda p: lowered.at[p],
        "tp",
        TP,
        at.tp,
        keep_token,
    )
    for t in range(TP):
        cols = slice(t * wide, (t + 1) * wide)
        mixed[:, cols] = (attended[:, cols].astype(F32) + lowered[t].astype(F32)).astype(BF16)
    phase(None)


VMEM = pl.BlockSpec(memory_space=pltpu.VMEM)
ANY = pl.BlockSpec(memory_space=pl.ANY)
COPIES, COPIES_2, SLOTS = 157, CP, 48


def dma(count):
    return pltpu.SemaphoreType.DMA((count,))


def on_device(
    tokens,
    attention_gain,
    query_weight,
    key_weight,
    value_weight,
    out_weight,
    feed_gain,
    gate_weight,
    up_weight,
    down_weight,
):
    local_rows, model = tokens.shape
    block = local_rows * TP
    rows = block * CP
    qkv = query_weight.shape[1] + key_weight.shape[1] + value_weight.shape[1]
    units = gate_weight.shape[1]
    wide = model // TP

    pair = jnp.arange(HD, dtype=F32)[None] % (HD // 2)
    inverse = rope_base ** (-(pair * 2.0 / HD))

    inputs = {
        "tokens": tokens,
        "attention_gain": attention_gain[None],
        "feed_gain": feed_gain[None],
        "inverse": inverse,
        "key_weight": key_weight,
        "value_weight": value_weight,
        "query_weight": query_weight,
        "out_weight": out_weight,
        "gate_weight": gate_weight,
        "up_weight": up_weight,
        "down_weight": down_weight,
    }

    def buf(*shape, kind=BF16):
        return pltpu.VMEM(shape, kind)

    scratch = {name: buf(*inputs[name + "_weight"].shape) for name in WEIGHTS}
    scratch |= {
        "cos": buf(block, HD, kind=F32),
        "sin": buf(block, HD, kind=F32),
        "slices": buf(NZ, local_rows, wide),
        "got": buf(NZ, local_rows, wide),
        "columns": buf(TP, NZ, local_rows, wide),
        "rows_in": buf(NZ, block, wide),
        "qkv_part": buf(NZ, block, qkv),
        "summed": buf(block, qkv, kind=F32),
        "shared": buf(NZ, NY, block, 2 * HD),
        "every": buf(NZ, block, wide),
        "projected": buf(NZ, local_rows, wide),
        "by_width": buf(TP, local_rows, wide),
        "got_width": buf(TP, local_rows, wide),
        "stream": buf(NZ, NY, block, wide),
        "down_far": buf(8, block, DOWN_SPLIT),
        "z_far": buf(8, NY, block, wide - DOWN_SPLIT),
        "z_sum": buf(NY, block, wide - DOWN_SPLIT),
        "z_left": buf(NY // 2, block, wide - DOWN_SPLIT),
        "z_right": buf(NY // 2, block, wide - DOWN_SPLIT),
        "reduced": buf(block, wide, kind=F32),
        "by_token": buf(TP, local_rows, wide),
        "lowered": buf(TP, local_rows, wide),
    }
    for name in ALONG_Y:
        scratch[name] = buf(NY, *inputs[name + "_weight"].shape)
    for c, chunk in OUT_CHUNKS.items():
        scratch |= {
            f"out_part_{c}": buf(TP, len(chunk), local_rows, wide),
            f"out_got_{c}": buf(TP, len(chunk), local_rows, wide),
            f"out_total_{c}": buf(len(chunk), local_rows, wide),
        }
    for c, chunk in CHUNKS.items():
        n, half = len(chunk), block // 2
        scratch |= {
            f"unit_part_{c}": buf(n, NX, 2, half, 2 * units),
            f"held_{c}": buf(n, NX, half, 2 * units),
            f"from_left_{c}": buf(NX // 2, n, half, 2 * units),
            f"from_right_{c}": buf(NX // 2, n, half, 2 * units),
            f"unit_total_{c}": buf(n, half, 2 * units, kind=F32),
            f"hidden_{c}": buf(n, NX, 2, half, units),
            f"down_part_{c}": buf(n, NY, block, wide),
            f"down_left_{c}": buf(NY // 2, n, block, DOWN_SPLIT),
            f"down_right_{c}": buf(NY // 2, n, block, DOWN_SPLIT),
            f"down_sum_{c}": buf(n, block, DOWN_SPLIT),
        }
    for n, (_, extent) in enumerate(QKV_PARTS):
        scratch[f"sum_{n}"] = buf(NZ, block, extent)
    scratch |= {f"r{n}": dma(TP) for n in range(2)}
    scratch |= {"load": dma(len(WEIGHTS)), "send": dma(SLOTS), "recv": dma(COPIES)}
    scratch |= {"recv_2": dma(COPIES_2), "send_w": dma(24), "recv_w": dma(24)}

    names = (*inputs, "streams", *scratch)
    streams = pl.pallas_call(
        functools.partial(layer_kernel, names),
        out_shape=jax.ShapeDtypeStruct((2, *tokens.shape), BF16),
        in_specs=[ANY if name.endswith("_weight") else VMEM for name in inputs],
        out_specs=VMEM,
        scratch_shapes=list(scratch.values()),
        compiler_params=pltpu.CompilerParams(
            collective_id=0,
            has_side_effects=True,
            vmem_limit_bytes=60 * 1024 * 1024,
        ),
        name="layer",
    )(*inputs.values())
    return streams[0], streams[1]


def solution(mesh):
    in_specs = (
        P(("cp", "tp"), None),
        P(),
        P("cp", "tp"),
        P("cp", "tp"),
        P("cp", "tp"),
        P("tp", "cp"),
        P(),
        P("tp", "cp"),
        P("tp", "cp"),
        P("cp", "tp"),
    )
    out_specs = (P(("cp", "tp"), None), P(("cp", "tp"), None))
    return jax.shard_map(
        on_device, mesh=mesh, in_specs=in_specs, out_specs=out_specs, check_vma=False
    )
```

```python
import collections
import functools

import jax
import jax.numpy as jnp
import numpy as np
from jax import lax
from jax.experimental import pallas as pl
from jax.experimental.pallas import tpu as pltpu
from jax.sharding import PartitionSpec as P

HD = 128
NZ, NY, NX = 8, 4, 4
CP, TP = NZ * NY, NX * 2
MESH = pl.DeviceIdType.MESH
F32, BF16 = jnp.float32, jnp.bfloat16

epsilon = 1e-05
rope_base = 500000.0
masked = -1e30


class Wires:
    def __init__(self, send, recv):
        self.send, self.recv, self.used, self.sent = send, recv, 0, []

    def copy(self, src, dst, device):
        i, slots = self.used, self.send.shape[0]
        self.used += 1
        assert i < self.recv.shape[0]
        if i >= slots:
            self.sent[i - slots].wait_send()
        c = pltpu.make_async_remote_copy(
            src_ref=src,
            dst_ref=dst,
            send_sem=self.send.at[i % slots],
            recv_sem=self.recv.at[i],
            device_id=device,
            device_id_type=MESH,
        )
        c.start()
        self.sent.append(c)
        return c

    def drain(self):
        for c in self.sent[-self.send.shape[0] :]:
            c.wait_send()
        self.sent, self.used = [], 0


class Now(list):
    pass


def advance(gen):
    needs = next(gen, None)
    while isinstance(needs, Now):
        for c in needs:
            c.wait_recv()
        needs = next(gen, None)
    return needs


class Steps:
    def __init__(self):
        self.queue, self.begun = collections.deque(), set()

    def add(self, gen, name="line", step=0):
        with jax.named_scope(f"{name}_{step}"):
            needs = advance(gen)
        if needs is not None:
            self.queue.append((needs, gen, name, step + 1))

    def go_on(self, entry):
        needs, gen, name, step = entry
        with jax.named_scope(f"wait_{name}_{step}"):
            for c in needs:
                c.wait_recv()
        self.add(gen, name, step)

    def run(self, until=lambda: False):
        while self.queue and not until():
            self.go_on(self.queue.popleft())

    def play(self, order, begin):
        for word in order.split():
            if word.isupper():
                if word not in self.begun:
                    self.begun.add(word)
                    begin(word)
                continue
            name, step = word.split("/") if "/" in word else (word[0], word[1:])
            step = int(step)
            while True:
                found = [i for i, e in enumerate(self.queue) if e[2] == name]
                if not found or self.queue[found[0]][3] > step:
                    break
                entry = self.queue[found[0]]
                del self.queue[found[0]]
                self.go_on(entry)


class Phases:
    def __init__(self):
        self.scope = None

    def __call__(self, name):
        if self.scope:
            self.scope.__exit__(None, None, None)
        self.scope = jax.named_scope(name) if name else None
        if self.scope:
            self.scope.__enter__()


class Place:
    def __init__(self):
        self.cp, self.tp = lax.axis_index("cp"), lax.axis_index("tp")
        self.z, self.y = self.cp // NY, self.cp % NY
        self.x, self.core = self.tp // 2, self.tp % 2

    def along_z(self, z):
        return {"cp": z * NY + self.y}

    def along_y(self, y):
        return {"cp": self.z * NY + y}

    def along_x(self, x):
        return {"tp": x * 2 + self.core}

    def partner(self):
        return {"tp": self.x * 2 + 1 - self.core}


def ring(n, me, device_of):
    return device_of((me + 1) % n), device_of((me + n - 1) % n)


def greet(devices):
    barrier = pltpu.get_barrier_semaphore()
    for device in devices:
        pl.semaphore_signal(barrier, inc=1, device_id=device, device_id_type=MESH)
    return len(devices)


def greet_group(axis, n, me):
    barrier = pltpu.get_barrier_semaphore()

    def signal(off, carry):
        pl.semaphore_signal(
            barrier, inc=1, device_id={axis: (me + off) % n}, device_id_type=MESH
        )
        return carry

    lax.fori_loop(1, n, signal, 0)
    return n - 1


def await_greetings(count):
    pl.semaphore_wait(pltpu.get_barrier_semaphore(), count)


def half_of(ref, h):
    d = ref.shape[0] // 2
    if d:
        return ref.at[pl.ds(h * d, d)]
    width = ref.shape[-1]
    d = -(-width // 256) * 128
    cols = pl.ds(0, d) if h == 0 else pl.ds(d, width - d)
    return ref.at[(slice(None),) * (len(ref.shape) - 1) + (cols,)]


def ring_gather(wires, block, n, me, device_of, arrived=None):
    right, left = ring(n, me, device_of)
    last = n // 2 - 1

    def send(k):
        r, l = block((me + n - k) % n), block((me + k) % n)
        if k == last:
            r, l = half_of(r, 0), half_of(l, 1)
        return wires.copy(r, r, right), wires.copy(l, l, left)

    flying = send(0)
    if arrived:
        arrived(me)
    for k in range(1, n // 2 + 1):
        yield flying
        if k <= last:
            flying = send(k)
            if arrived:
                arrived((me + n - k) % n)
                arrived((me + k) % n)
        elif arrived:
            arrived((me + n // 2) % n)


def add_rows(dst, terms, finish=None):
    if len(dst.shape) > 2:
        for i in range(dst.shape[0]):
            add_rows(dst.at[i], [t.at[i] for t in terms])
        return
    rows = dst.shape[0]
    step = min(rows, 16)

    def body(i, carry):
        at = pl.ds(pl.multiple_of(i * step, step), step)
        total = terms[0][at, :].astype(F32)
        for t in terms[1:]:
            total = total + t[at, :].astype(F32)
        dst[at, :] = total.astype(dst.dtype)
        return carry

    lax.fori_loop(0, rows // step, body, 0)


def ring_scatter(wires, own, out, from_left, from_right, n, me, device_of):
    right, left = ring(n, me, device_of)
    m = n // 2
    far = own((me + m) % n)
    r = wires.copy(half_of(far, 0), half_of(from_left.at[0], 0), right)
    l = wires.copy(half_of(far, 1), half_of(from_right.at[0], 1), left)
    for k in range(1, m):
        to_right, to_left = own((me + m - k) % n), own((me + n - m + k) % n)
        got_left, got_right = from_left.at[k - 1], from_right.at[k - 1]
        yield [r]
        if k == 1:
            add_rows(half_of(got_left, 0), [half_of(got_left, 0), half_of(to_right, 0)])
            add_rows(half_of(got_left, 1), [half_of(to_right, 1)])
        else:
            add_rows(got_left, [got_left, to_right])
        r = wires.copy(got_left, from_left.at[k], right)
        yield Now([l])
        if k == 1:
            add_rows(half_of(got_right, 1), [half_of(got_right, 1), half_of(to_left, 1)])
            add_rows(half_of(got_right, 0), [half_of(to_left, 0)])
        else:
            add_rows(got_right, [got_right, to_left])
        l = wires.copy(got_right, from_right.at[k], left)
    yield [r, l]
    add_rows(out, [own(me), from_left.at[m - 1], from_right.at[m - 1]])


def far_gather(wires, block, n, me, device_of, arrived):
    def send(ref, off):
        return wires.copy(ref, ref, device_of((me + n + off) % n))

    def whole(off):
        return block((me + n + off) % n)

    own = block(me)
    p2, m2, p1, m1 = send(own, 2), send(own, -2), send(own, 1), send(own, -1)
    arrived(0)
    yield [p2]
    p3, p4 = send(whole(-2), 1), send(half_of(whole(-2), 0), 2)
    yield Now([m2])
    m3, m4 = send(whole(2), -1), send(half_of(whole(2), 1), -2)
    yield Now([p1])
    arrived(7)
    yield Now([m1])
    for off in (1, 6, 2):
        arrived(off)
    yield [p3]
    arrived(5)
    yield Now([m3])
    arrived(3)
    yield Now([p4, m4])
    arrived(4)


def far_scatter(wires, own, out, bufs, n, me, device_of):
    lines = FarScatter(
        wires,
        lambda off: own((me + off) % n),
        out,
        bufs,
        lambda off: device_of((me + off) % n),
    )
    for off in (4, 3, 5, 1, 7):
        lines.send(off)
    yield from lines.turns("l")
    other = lines.turns("r")
    yield Now(next(other))
    next(other, None)
    yield from lines.last_round()


class FarScatter:
    def __init__(self, wires, own, out, bufs, device_of):
        self.wires, self.own, self.out, self.device_of = wires, own, out, device_of
        self.bufs, self.sent = bufs, {}

    def copy(self, name, src, dst, off):
        self.sent[name] = self.wires.copy(src, dst, self.device_of(off))

    def send(self, off):
        near_l, near_r, turn_l, turn_r, far_l, far_r = [self.bufs.at[i] for i in range(6)]
        term = self.own(off)
        if off == 1:
            self.copy("near_l", term, near_l, 1)
        elif off == 7:
            self.copy("near_r", term, near_r, 7)
        elif off == 3:
            self.copy("turn_l", term, turn_l, 1)
        elif off == 5:
            self.copy("turn_r", term, turn_r, 7)
        elif off == 4:
            self.copy("far_l", half_of(term, 0), half_of(far_l, 0), 2)
            self.copy("far_r", half_of(term, 1), half_of(far_r, 1), 6)

    def turn(self, side):
        n, off, full = (0, 2, 0) if side == "l" else (1, 6, 1)
        turn, far, into = self.bufs.at[2 + n], self.bufs.at[4 + n], self.bufs.at[6 + n]
        mine = self.own(off)
        add_rows(half_of(turn, full), [half_of(x, full) for x in (turn, far, mine)])
        add_rows(half_of(turn, 1 - full), [half_of(x, 1 - full) for x in (turn, mine)])
        self.copy("sum_" + side, turn, into, off)

    def turns(self, side):
        yield [self.sent["turn_" + side], self.sent["far_" + side]]
        self.turn(side)

    def last_round(self):
        yield [self.sent[n] for n in ("near_l", "near_r", "sum_l", "sum_r")]
        near_l, near_r, sum_l, sum_r = [self.bufs.at[i] for i in (0, 1, 6, 7)]
        add_rows(self.out, [self.own(0), near_l, near_r, sum_l, sum_r])


def exchange(send_sem, recv_sem, source, target, axis, n, me, meanwhile=None):
    def copy(off):
        peer = (me + off) % n
        return pltpu.make_async_remote_copy(
            src_ref=source(peer),
            dst_ref=target(me),
            send_sem=send_sem.at[off],
            recv_sem=recv_sem.at[off],
            device_id=axis(peer) if callable(axis) else {axis: peer},
            device_id_type=MESH,
        )

    def start(off, carry):
        copy(off).start()
        return carry

    def wait(off, carry):
        copy(off).wait()
        return carry

    lax.fori_loop(1, n, start, 0)
    if meanwhile:
        meanwhile()
    lax.fori_loop(1, n, wait, 0)


QKV_PARTS = ((0, 256), (256, 512), (768, 512))
QKV_ORDER = "g2 K k1 q1 O p2 A k2 q2 B a1 k3 b1 o1 H a2 b2 k4"
GATHER_SPLIT = 768
DOWN_SPLIT = 640


CHUNKS = {"e": (0,), "b": (1, 7), "c": (3, 4), "d": (5,), "a": (2, 6)}
OUT_CHUNKS = {0: (0, 7, 1, 6, 2), 1: (5, 3, 4)}


def gather_rows(wires, steps, at, out_ref, split, chunks, ready):
    first, rest = pl.ds(0, split), pl.ds(split, out_ref.shape[-1] - split)
    seen = collections.Counter()

    def z_at(off):
        return (at.z + off) % NZ

    def mark(off):
        seen[off] += 1
        for c, chunk in chunks.items():
            if off in chunk and all(seen[o] == 2 for o in chunk):
                steps.add(ready(c), f"chunk{c}")

    def y_first():
        yield from ring_gather(
            wires, lambda j: out_ref.at[at.z, j, :, rest], NY, at.y, at.along_y
        )
        yield from far_gather(
            wires, lambda i: out_ref.at[i, :, :, rest], NZ, at.z, at.along_z, mark
        )

    def to_y(off):
        def line():
            yield from ring_gather(
                wires, lambda j: out_ref.at[z_at(off), j, :, first], NY, at.y, at.along_y
            )
            mark(off)

        steps.add(line(), f"y{off}")

    steps.add(y_first(), "yz")
    steps.add(
        far_gather(
            wires, lambda i: out_ref.at[i, at.y, :, first], NZ, at.z, at.along_z, to_y
        ),
        "z",
    )


def gather_small(wires, at, ref):
    handed = []

    def to_y(block):
        for off in (1, 3, 2):
            handed.append(wires.copy(block, block, at.along_y((at.y + off) % NY)))

    own = ref.at[at.z, at.y]
    order = (4, 3, 5, 2, 6, 1, 7)
    copies = {off: wires.copy(own, own, at.along_z((at.z + off) % NZ)) for off in order}
    to_y(own)
    yield []
    for off in (1, 7, 2, 6, 3, 5, 4):
        yield Now([copies[off]])
        to_y(ref.at[(at.z + NZ - off) % NZ, at.y])
    yield handed


def chunk_rows(ref, at, chunk):
    blocks = [ref[(at.z + off) % NZ] for off in chunk]
    return jnp.concatenate([b.reshape(-1, b.shape[-1]) for b in blocks], axis=0)


GATHER_ORDER = """yz/1 y0/1 z/1 yz/2 y0/2 E y7/1 y1/1 e1 y6/1 y2/1 z/2 yz/3 y7/2 y1/2 B e2 y6/2 y2/2 b1 y5/1 y3/1 y4/1 yz/4 e3 y5/2 y3/2 y4/2"""
ORDER = """b2 C e4 D A c1 d1 a1 b3 e5 c2 d2 a2 b4 c3 d3 b5 e6 a3 b6 c4 d4 e7 a4 c5 c6 b7 d5 d6 a5 a6 e8 b8 c7 V v1 W w1 d7 a7 c8 d8 a8 T U N n1 t1 u1 n2 L l1 n3"""


def feed_chunk(wires, at, r, c, produced, finished):
    partner = at.partner()
    units = r["gate"].shape[1]
    part, held, total, hidden, down_part = (
        r[f"{name}_{c}"] for name in ("unit_part", "held", "unit_total", "hidden", "down_part")
    )

    def tile(w_ref, col, width, start):
        p = jnp.dot(
            chunk_rows(r["stream"], at, CHUNKS[c]), w_ref[:, pl.ds(col, width)], preferred_element_type=F32
        )
        cols = pl.ds(start + col, width)
        part[:, :, :, :, cols] = p.astype(BF16).reshape(*part.shape[:4], width)

    for t in range(units // 256):
        tile(r["gate"], t * 256, 256, 0)
        tile(r["up"], t * 256, 256, units)
    if units % 256:
        tile(r["gate"], units // 256 * 256, units % 256, 0)
        tile(r["up"], units // 256 * 256, units % 256, units)
    yield [wires.copy(part.at[:, :, 1 - at.core], held, partner)]
    add_rows(held, [held, part.at[:, :, at.core]])
    yield from ring_scatter(
        wires,
        lambda i: held.at[:, i],
        total,
        r[f"from_left_{c}"],
        r[f"from_right_{c}"],
        NX,
        at.x,
        at.along_x,
    )
    for n in range(total.shape[0]):
        gate, up = total[n, :, pl.ds(0, units)], total[n, :, pl.ds(units, units)]
        hidden[n, at.x, at.core] = (jax.nn.silu(gate) * up).astype(BF16)
    handed = []

    def hand_over(i):
        ref = hidden.at[:, i, at.core]
        handed.append(wires.copy(ref, ref, partner))

    yield from ring_gather(
        wires, lambda i: hidden.at[:, i, at.core], NX, at.x, at.along_x, hand_over
    )
    yield handed

    def down(i, carry):
        cols = pl.ds(pl.multiple_of(i * 256, 256), 256)
        p = jnp.dot(
            hidden[...].reshape(-1, units), r["down"][:, cols], preferred_element_type=F32
        )
        down_part[:, :, :, cols] = p.astype(BF16).reshape(*down_part.shape[:3], 256)
        return carry

    lax.fori_loop(0, down_part.shape[-1] // 256, down, 0)
    produced(c)
    yield from ring_scatter(
        wires,
        lambda j: down_part.at[:, j, :, pl.ds(0, DOWN_SPLIT)],
        r[f"down_sum_{c}"],
        r[f"down_left_{c}"],
        r[f"down_right_{c}"],
        NY,
        at.y,
        at.along_y,
    )
    finished(c)


def normalize(values, gain):
    mean_square = jnp.mean(values * values, axis=-1, keepdims=True)
    return (values * lax.rsqrt(mean_square + epsilon) * gain).astype(BF16)


WEIGHTS = ("key", "value", "query", "out", "gate", "up", "down")
SMALL = ("tokens", "attention_gain", "feed_gain")
ALONG_Y = ("key", "value", "query", "out")


def layer_kernel(names, *refs):
    r = dict(zip(names, refs))
    at = Place()
    qkv_wires, wires = Wires(r["send"], r["recv"]), Wires(r["send"], r["recv_2"])
    steps = Steps()
    tokens = r["tokens_held"]
    local_rows, model = tokens.shape
    attended, mixed = r["streams"].at[0], r["streams"].at[1]
    cos, sin = r["cos"], r["sin"]

    phase = Phases()
    phase("greet")
    greeted = greet_group("cp", CP, at.cp) + greet_group("tp", TP, at.tp)
    loads = {}
    for n, name in enumerate(SMALL):
        held = r[name + "_held"]
        loads[name] = pltpu.make_async_copy(r[name], held, r["load"].at[len(WEIGHTS) + n])
        loads[name].start()
    for n, name in enumerate(WEIGHTS):
        held = r[name].at[at.y] if name in ALONG_Y else r[name]
        loads[name] = pltpu.make_async_copy(r[name + "_weight"], held, r["load"].at[n])
        loads[name].start()

    block = cos.shape[0]
    positions = at.cp * block + lax.broadcasted_iota(jnp.int32, (block, HD), 0)
    angles = positions.astype(F32) * r["inverse"][...]
    first_half = lax.broadcasted_iota(jnp.int32, (block, HD), 1) < HD // 2
    cos[...] = jnp.cos(angles)
    sin[...] = jnp.where(first_half, -jnp.sin(angles), jnp.sin(angles))

    for name in SMALL:
        loads[name].wait()
    normed = normalize(tokens[...].astype(F32), r["attention_gain_held"][...])
    slices, got, columns = r["slices"], r["got"], r["columns"]
    wide = slices.shape[-1]
    for z in range(NZ):
        slices[z] = normed[:, z * wide : (z + 1) * wide]
    phase("barrier")
    await_greetings(greeted)

    phase("spread_cp")
    weight_wires = Wires(r["send_w"], r["recv_w"])
    query_cols, out_cols = r["query"].shape[-1] // 2, r["out"].shape[-1] // 2

    def gathered(*blocks):
        rings = [ring_gather(weight_wires, b, NY, at.y, at.along_y) for b in blocks]
        while True:
            flights = [advance(g) for g in rings]
            if flights[0] is None:
                return
            yield [c for some in flights for c in some]

    weight_parts = {
        "G": lambda: gathered(lambda j: r["key"].at[j], lambda j: r["value"].at[j]),
        "P": lambda: gathered(lambda j: r["query"].at[j, :, pl.ds(0, query_cols)]),
        "Q": lambda: gathered(lambda j: r["query"].at[j, :, pl.ds(query_cols, query_cols)]),
        "O": lambda: gathered(lambda j: r["out"].at[j, :, pl.ds(0, out_cols)]),
        "H": lambda: gathered(lambda j: r["out"].at[j, :, pl.ds(out_cols, out_cols)]),
    }

    def begin_weights(letter):
        steps.add(weight_parts[letter](), letter.lower())

    def keep_slice():
        for name in ALONG_Y:
            loads[name].wait()
        steps.play("G P", begin_weights)
        got[at.z] = slices[at.z]

    exchange(
        r["send"], r["recv_2"], lambda p: slices.at[p], lambda p: got.at[p], at.along_z, NZ, at.z, keep_slice
    )
    steps.play("g1 Q", begin_weights)

    phase("spread_tp")
    def keep_columns():
        columns[at.tp] = got[...]

    exchange(
        r["send"], r["r0"], lambda p: got, lambda p: columns.at[p], "tp", TP, at.tp, keep_columns
    )
    phase("relayout")
    rows_in = r["rows_in"]

    def in_order(b, carry):
        parts = [columns[t, b].astype(F32) for t in range(TP)]
        rows_in[b] = jnp.concatenate(parts, axis=0).astype(BF16)
        return carry

    steps.play("p1", begin_weights)
    lax.fori_loop(0, NZ, in_order, 0)

    part, summed, shared = r["qkv_part"], r["summed"], r["shared"]

    def product(name, cols, start):
        x = rows_in[...].reshape(-1, wide)
        w = r[name][:, :, cols].reshape(wide, -1)
        p = jnp.dot(x, w, preferred_element_type=F32)
        part[:, :, start : start + p.shape[1]] = p.astype(BF16).reshape(NZ, block, -1)

    def turned(v):
        return (v * cos[...] + pltpu.roll(v, HD // 2, 1) * sin[...]).astype(BF16)

    def unit(n):
        start, extent = QKV_PARTS[n]
        cols = pl.ds(start, extent)
        return far_scatter(
            qkv_wires,
            lambda i: part.at[i, :, cols],
            summed.at[:, cols],
            r[f"sum_{n}"],
            NZ,
            at.z,
            at.along_z,
        )

    def keys_and_values():
        yield from unit(0)
        shared[at.z, at.y, :, pl.ds(0, HD)] = turned(summed[:, pl.ds(0, HD)])
        shared[at.z, at.y, :, pl.ds(HD, HD)] = summed[:, pl.ds(HD, HD)].astype(BF16)
        yield from gather_small(qkv_wires, at, shared)

    def begin_part(letter):
        if letter == "K":
            product("key", slice(None), 0)
            product("value", slice(None), HD)
            steps.add(keys_and_values(), "k")
        elif letter in "AB":
            n = "KAB".index(letter)
            start, extent = QKV_PARTS[n]
            for col in range(0, extent, 256):
                at_col = start - 2 * HD + col
                product("query", slice(at_col, at_col + 256), start + col)
            steps.add(unit(n), letter.lower())
        else:
            begin_weights(letter)

    phase("qkv_sum")
    steps.play(QKV_ORDER, begin_part)
    steps.begun.clear()
    qkv_wires.drain()

    phase("attend")
    every = r["every"]
    heads = (summed.shape[1] - 2 * HD) // HD
    block = summed.shape[0]
    query = jnp.concatenate(
        [turned(summed[:, (2 + h) * HD : (3 + h) * HD]) for h in range(heads)], axis=0
    )
    keys = shared[:, :, :, 0:HD].reshape(-1, HD)
    values = shared[:, :, :, HD : 2 * HD].reshape(-1, HD)
    scores = lax.dot_general(
        query, keys, (((1,), (1,)), ((), ())), preferred_element_type=F32
    ) * HD ** (-0.5)
    key_at = lax.broadcasted_iota(jnp.int32, scores.shape, 1)
    query_at = lax.broadcasted_iota(jnp.int32, scores.shape, 0) % block + at.cp * block
    allowed = key_at <= query_at
    scores = jnp.where(allowed, scores, masked)
    top = jnp.max(scores, axis=-1, keepdims=True)
    weights = jnp.where(allowed, jnp.exp(scores - top), 0.0)
    total = jnp.sum(weights, axis=-1, keepdims=True)
    mean = jnp.dot(weights.astype(BF16), values, preferred_element_type=F32) / total
    mean = mean.astype(BF16)
    for h in range(heads):
        every[at.z, :, h * HD : (h + 1) * HD] = mean[h * block : (h + 1) * block]

    phase("gather_att")
    projected = r["projected"]
    owners, seen = [], set()

    def out_chunk(c):
        chunk = OUT_CHUNKS[c]
        part, arrived, total = r[f"out_part_{c}"], r[f"out_got_{c}"], r[f"out_total_{c}"]
        x = jnp.concatenate([every[(at.z + off) % NZ] for off in chunk], axis=0)
        cols = r["out"].shape[-1]
        for y in range(NY):
            p = jnp.dot(x, r["out"][y], preferred_element_type=F32)
            for n in range(len(chunk)):
                for t in range(TP):
                    first = n * block + t * local_rows
                    part[t, n, :, y * cols : (y + 1) * cols] = p[
                        first : first + local_rows
                    ].astype(BF16)
        copies = []
        for off in range(1, TP):
            to = (at.tp + off) % TP
            copies.append(wires.copy(part.at[to], arrived.at[at.tp], {"tp": to}))
        arrived[at.tp] = part[at.tp]
        yield copies
        for n, off in enumerate(chunk):
            sums = arrived[0, n].astype(F32)
            for t in range(1, TP):
                sums = sums + arrived[t, n].astype(F32)
            total[n] = sums.astype(BF16)
            if off == 0:
                projected[at.z] = total[n]
            else:
                to = at.along_z((at.z + off) % NZ)
                owners.append(wires.copy(total.at[n], projected.at[at.z], to))

    def att_there(off):
        seen.add(off)
        for c, chunk in OUT_CHUNKS.items():
            if off in chunk and seen >= set(chunk):
                steps.play("o2 h1 h2", None)
                steps.add(out_chunk(c), f"out{c}")

    steps.add(
        far_gather(wires, lambda i: every.at[i], NZ, at.z, at.along_z, att_there), "z"
    )
    steps.play("h1 z/1 z/2", None)
    steps.run()
    phase("out_cp")
    for c in owners:
        c.wait_recv()
    wires.drain()
    weight_wires.drain()
    phase("norm_feed")
    wide = projected.shape[-1]
    for z in range(NZ):
        cols = slice(z * wide, (z + 1) * wide)
        attended[:, cols] = (tokens[:, cols].astype(F32) + projected[z].astype(F32)).astype(BF16)

    normed = normalize(attended[...].astype(F32), r["feed_gain_held"][...])
    by_width, got_width, stream = r["by_width"], r["got_width"], r["stream"]
    wide = by_width.shape[-1]
    for t in range(TP):
        by_width[t] = normed[:, t * wide : (t + 1) * wide]

    phase("swap1")
    def keep_width():
        got_width[at.tp] = by_width[at.tp]

    exchange(
        r["send"],
        r["r1"],
        lambda p: by_width.at[p],
        lambda p: got_width.at[p],
        "tp",
        TP,
        at.tp,
        keep_width,
    )
    phase("gather_feed")
    stream[at.z, at.y] = jnp.concatenate(
        [got_width[t].astype(F32) for t in range(TP)], axis=0
    ).astype(BF16)
    for name in ("gate", "up", "down"):
        loads[name].wait()
    reduced = r["reduced"]
    places = {off: (c, n) for c, chunk in CHUNKS.items() for n, off in enumerate(chunk)}

    def piece(name, off):
        c, n = places[off]
        return r[f"{name}_{c}"].at[n]

    def to_z(off):
        return at.along_z((at.z + off) % NZ)

    lines = FarScatter(
        qkv_wires,
        lambda off: piece("down_sum", off),
        reduced.at[:, pl.ds(0, DOWN_SPLIT)],
        r["down_far"],
        to_z,
    )
    rest = pl.ds(DOWN_SPLIT, reduced.shape[1] - DOWN_SPLIT)
    z_lines = FarScatter(
        qkv_wires,
        lambda off: piece("down_part", off).at[:, :, rest],
        r["z_sum"],
        r["z_far"],
        to_z,
    )
    there = {}

    def produced(c):
        for off in CHUNKS[c]:
            z_lines.send(off)

    def finished(c):
        for off in CHUNKS[c]:
            lines.send(off)

    def z_first_end():
        yield from z_lines.last_round()
        yield from ring_scatter(
            qkv_wires,
            lambda j: r["z_sum"].at[j],
            reduced.at[:, rest],
            r["z_left"],
            r["z_right"],
            NY,
            at.y,
            at.along_y,
        )

    later = {
        "T": lambda: lines.turns("l"),
        "U": lambda: lines.turns("r"),
        "V": lambda: z_lines.turns("l"),
        "W": lambda: z_lines.turns("r"),
        "N": z_first_end,
        "L": lines.last_round,
    }

    def begin(letter):
        if letter in later:
            gen = later[letter]()
        else:
            assert letter.lower() in there
            gen = feed_chunk(qkv_wires, at, r, letter.lower(), produced, finished)
        steps.add(gen, letter.lower())

    def chunk_there(c):
        there[c] = True
        return iter(())

    gather_rows(qkv_wires, steps, at, stream, GATHER_SPLIT, CHUNKS, chunk_there)
    steps.play(GATHER_ORDER, begin)
    assert len(there) == len(CHUNKS)
    steps.play(ORDER, begin)
    assert not steps.queue
    phase("swap2")
    qkv_wires.drain()
    by_token, lowered = r["by_token"], r["lowered"]
    for t in range(TP):
        by_token[t] = reduced[pl.ds(t * local_rows, local_rows), :].astype(BF16)

    def keep_token():
        lowered[at.tp] = by_token[at.tp]

    exchange(
        r["send"],
        r["r0"],
        lambda p: by_token.at[p],
        lambda p: lowered.at[p],
        "tp",
        TP,
        at.tp,
        keep_token,
    )
    for t in range(TP):
        cols = slice(t * wide, (t + 1) * wide)
        mixed[:, cols] = (attended[:, cols].astype(F32) + lowered[t].astype(F32)).astype(BF16)
    phase(None)


VMEM = pl.BlockSpec(memory_space=pltpu.VMEM)
ANY = pl.BlockSpec(memory_space=pl.ANY)
COPIES, COPIES_2, SLOTS = 157, CP, 48


def dma(count):
    return pltpu.SemaphoreType.DMA((count,))


def on_device(
    tokens,
    attention_gain,
    query_weight,
    key_weight,
    value_weight,
    out_weight,
    feed_gain,
    gate_weight,
    up_weight,
    down_weight,
):
    local_rows, model = tokens.shape
    block = local_rows * TP
    rows = block * CP
    qkv = query_weight.shape[1] + key_weight.shape[1] + value_weight.shape[1]
    units = gate_weight.shape[1]
    wide = model // TP

    pair = np.arange(HD, dtype=np.float32)[None] % (HD // 2)
    inverse = (np.float64(rope_base) ** (-(pair * 2.0 / HD))).astype(np.float32)

    inputs = {
        "tokens": tokens,
        "attention_gain": attention_gain[None],
        "feed_gain": feed_gain[None],
        "inverse": jnp.asarray(inverse),
        "key_weight": key_weight,
        "value_weight": value_weight,
        "query_weight": query_weight,
        "out_weight": out_weight,
        "gate_weight": gate_weight,
        "up_weight": up_weight,
        "down_weight": down_weight,
    }

    def buf(*shape, kind=BF16):
        return pltpu.VMEM(shape, kind)

    scratch = {name: buf(*inputs[name + "_weight"].shape) for name in WEIGHTS}
    scratch |= {
        "cos": buf(block, HD, kind=F32),
        "sin": buf(block, HD, kind=F32),
        "slices": buf(NZ, local_rows, wide),
        "got": buf(NZ, local_rows, wide),
        "columns": buf(TP, NZ, local_rows, wide),
        "rows_in": buf(NZ, block, wide),
        "qkv_part": buf(NZ, block, qkv),
        "summed": buf(block, qkv, kind=F32),
        "shared": buf(NZ, NY, block, 2 * HD),
        "every": buf(NZ, block, wide),
        "projected": buf(NZ, local_rows, wide),
        "by_width": buf(TP, local_rows, wide),
        "got_width": buf(TP, local_rows, wide),
        "stream": buf(NZ, NY, block, wide),
        "down_far": buf(8, block, DOWN_SPLIT),
        "z_far": buf(8, NY, block, wide - DOWN_SPLIT),
        "z_sum": buf(NY, block, wide - DOWN_SPLIT),
        "z_left": buf(NY // 2, block, wide - DOWN_SPLIT),
        "z_right": buf(NY // 2, block, wide - DOWN_SPLIT),
        "reduced": buf(block, wide, kind=F32),
        "by_token": buf(TP, local_rows, wide),
        "lowered": buf(TP, local_rows, wide),
    }
    for name in SMALL:
        scratch[name + "_held"] = buf(*inputs[name].shape, kind=inputs[name].dtype)
    for name in ALONG_Y:
        scratch[name] = buf(NY, *inputs[name + "_weight"].shape)
    for c, chunk in OUT_CHUNKS.items():
        scratch |= {
            f"out_part_{c}": buf(TP, len(chunk), local_rows, wide),
            f"out_got_{c}": buf(TP, len(chunk), local_rows, wide),
            f"out_total_{c}": buf(len(chunk), local_rows, wide),
        }
    for c, chunk in CHUNKS.items():
        n, half = len(chunk), block // 2
        scratch |= {
            f"unit_part_{c}": buf(n, NX, 2, half, 2 * units),
            f"held_{c}": buf(n, NX, half, 2 * units),
            f"from_left_{c}": buf(NX // 2, n, half, 2 * units),
            f"from_right_{c}": buf(NX // 2, n, half, 2 * units),
            f"unit_total_{c}": buf(n, half, 2 * units, kind=F32),
            f"hidden_{c}": buf(n, NX, 2, half, units),
            f"down_part_{c}": buf(n, NY, block, wide),
            f"down_left_{c}": buf(NY // 2, n, block, DOWN_SPLIT),
            f"down_right_{c}": buf(NY // 2, n, block, DOWN_SPLIT),
            f"down_sum_{c}": buf(n, block, DOWN_SPLIT),
        }
    for n, (_, extent) in enumerate(QKV_PARTS):
        scratch[f"sum_{n}"] = buf(NZ, block, extent)
    scratch |= {f"r{n}": dma(TP) for n in range(2)}
    scratch |= {"load": dma(len(WEIGHTS) + len(SMALL)), "send": dma(SLOTS), "recv": dma(COPIES)}
    scratch |= {"recv_2": dma(COPIES_2), "send_w": dma(24), "recv_w": dma(24)}

    names = (*inputs, "streams", *scratch)
    streams = pl.pallas_call(
        functools.partial(layer_kernel, names),
        out_shape=jax.ShapeDtypeStruct((2, *tokens.shape), BF16),
        in_specs=[VMEM if name == "inverse" else ANY for name in inputs],
        out_specs=VMEM,
        scratch_shapes=list(scratch.values()),
        compiler_params=pltpu.CompilerParams(
            collective_id=0,
            has_side_effects=True,
            vmem_limit_bytes=60 * 1024 * 1024,
        ),
        name="layer",
    )(*inputs.values())
    return streams[0], streams[1]


def solution(mesh):
    in_specs = (
        P(("cp", "tp"), None),
        P(),
        P("cp", "tp"),
        P("cp", "tp"),
        P("cp", "tp"),
        P("tp", "cp"),
        P(),
        P("tp", "cp"),
        P("tp", "cp"),
        P("cp", "tp"),
    )
    out_specs = (P(("cp", "tp"), None), P(("cp", "tp"), None))
    return jax.shard_map(
        on_device, mesh=mesh, in_specs=in_specs, out_specs=out_specs, check_vma=False
    )
```

```python
import collections
import functools

import jax
import jax.numpy as jnp
import numpy as np
from jax import lax
from jax.experimental import pallas as pl
from jax.experimental.pallas import tpu as pltpu
from jax.sharding import PartitionSpec as P

HD = 128
NZ, NY, NX = 8, 4, 4
CP, TP = NZ * NY, NX * 2
MESH = pl.DeviceIdType.MESH
F32, BF16 = jnp.float32, jnp.bfloat16

epsilon = 1e-05
rope_base = 500000.0
masked = -1e30


class Wires:
    def __init__(self, send, recv):
        self.send, self.recv, self.used, self.sent = send, recv, 0, []

    def copy(self, src, dst, device):
        i, slots = self.used, self.send.shape[0]
        self.used += 1
        assert i < self.recv.shape[0]
        if i >= slots:
            self.sent[i - slots].wait_send()
        c = pltpu.make_async_remote_copy(
            src_ref=src,
            dst_ref=dst,
            send_sem=self.send.at[i % slots],
            recv_sem=self.recv.at[i],
            device_id=device,
            device_id_type=MESH,
        )
        c.start()
        self.sent.append(c)
        return c

    def drain(self):
        for c in self.sent[-self.send.shape[0] :]:
            c.wait_send()
        self.sent, self.used = [], 0


class Now(list):
    pass


def advance(gen):
    needs = next(gen, None)
    while isinstance(needs, Now):
        for c in needs:
            c.wait_recv()
        needs = next(gen, None)
    return needs


class Steps:
    def __init__(self):
        self.queue, self.begun = collections.deque(), set()

    def add(self, gen, name="line", step=0):
        with jax.named_scope(f"{name}_{step}"):
            needs = advance(gen)
        if needs is not None:
            self.queue.append((needs, gen, name, step + 1))

    def go_on(self, entry):
        needs, gen, name, step = entry
        with jax.named_scope(f"wait_{name}_{step}"):
            for c in needs:
                c.wait_recv()
        self.add(gen, name, step)

    def run(self, until=lambda: False):
        while self.queue and not until():
            self.go_on(self.queue.popleft())

    def play(self, order, begin):
        for word in order.split():
            if word.isupper():
                if word not in self.begun:
                    self.begun.add(word)
                    begin(word)
                continue
            name, step = word.split("/") if "/" in word else (word[0], word[1:])
            step = int(step)
            while True:
                found = [i for i, e in enumerate(self.queue) if e[2] == name]
                if not found or self.queue[found[0]][3] > step:
                    break
                entry = self.queue[found[0]]
                del self.queue[found[0]]
                self.go_on(entry)


class Phases:
    def __init__(self):
        self.scope = None

    def __call__(self, name):
        if self.scope:
            self.scope.__exit__(None, None, None)
        self.scope = jax.named_scope(name) if name else None
        if self.scope:
            self.scope.__enter__()


class Place:
    def __init__(self):
        self.cp, self.tp = lax.axis_index("cp"), lax.axis_index("tp")
        self.z, self.y = self.cp // NY, self.cp % NY
        self.x, self.core = self.tp // 2, self.tp % 2

    def along_z(self, z):
        return {"cp": z * NY + self.y}

    def along_y(self, y):
        return {"cp": self.z * NY + y}

    def along_x(self, x):
        return {"tp": x * 2 + self.core}

    def partner(self):
        return {"tp": self.x * 2 + 1 - self.core}


def ring(n, me, device_of):
    return device_of((me + 1) % n), device_of((me + n - 1) % n)


def greet(devices):
    barrier = pltpu.get_barrier_semaphore()
    for device in devices:
        pl.semaphore_signal(barrier, inc=1, device_id=device, device_id_type=MESH)
    return len(devices)


def greet_group(axis, n, me):
    barrier = pltpu.get_barrier_semaphore()

    def signal(off, carry):
        pl.semaphore_signal(
            barrier, inc=1, device_id={axis: (me + off) % n}, device_id_type=MESH
        )
        return carry

    lax.fori_loop(1, n, signal, 0)
    return n - 1


def await_greetings(count):
    pl.semaphore_wait(pltpu.get_barrier_semaphore(), count)


def half_of(ref, h):
    d = ref.shape[0] // 2
    if d:
        return ref.at[pl.ds(h * d, d)]
    width = ref.shape[-1]
    d = -(-width // 256) * 128
    cols = pl.ds(0, d) if h == 0 else pl.ds(d, width - d)
    return ref.at[(slice(None),) * (len(ref.shape) - 1) + (cols,)]


def ring_gather(wires, block, n, me, device_of, arrived=None):
    right, left = ring(n, me, device_of)
    last = n // 2 - 1

    def send(k):
        r, l = block((me + n - k) % n), block((me + k) % n)
        if k == last:
            r, l = half_of(r, 0), half_of(l, 1)
        return wires.copy(r, r, right), wires.copy(l, l, left)

    flying = send(0)
    if arrived:
        arrived(me)
    for k in range(1, n // 2 + 1):
        yield flying
        if k <= last:
            flying = send(k)
            if arrived:
                arrived((me + n - k) % n)
                arrived((me + k) % n)
        elif arrived:
            arrived((me + n // 2) % n)


def add_rows(dst, terms, finish=None):
    if len(dst.shape) > 2:
        for i in range(dst.shape[0]):
            add_rows(dst.at[i], [t.at[i] for t in terms])
        return
    rows = dst.shape[0]
    step = min(rows, 16)

    def body(i, carry):
        at = pl.ds(pl.multiple_of(i * step, step), step)
        total = terms[0][at, :].astype(F32)
        for t in terms[1:]:
            total = total + t[at, :].astype(F32)
        dst[at, :] = total.astype(dst.dtype)
        return carry

    lax.fori_loop(0, rows // step, body, 0)


def ring_scatter(wires, own, out, from_left, from_right, n, me, device_of):
    right, left = ring(n, me, device_of)
    m = n // 2
    far = own((me + m) % n)
    r = wires.copy(half_of(far, 0), half_of(from_left.at[0], 0), right)
    l = wires.copy(half_of(far, 1), half_of(from_right.at[0], 1), left)
    for k in range(1, m):
        to_right, to_left = own((me + m - k) % n), own((me + n - m + k) % n)
        got_left, got_right = from_left.at[k - 1], from_right.at[k - 1]
        yield [r]
        if k == 1:
            add_rows(half_of(got_left, 0), [half_of(got_left, 0), half_of(to_right, 0)])
            add_rows(half_of(got_left, 1), [half_of(to_right, 1)])
        else:
            add_rows(got_left, [got_left, to_right])
        r = wires.copy(got_left, from_left.at[k], right)
        yield Now([l])
        if k == 1:
            add_rows(half_of(got_right, 1), [half_of(got_right, 1), half_of(to_left, 1)])
            add_rows(half_of(got_right, 0), [half_of(to_left, 0)])
        else:
            add_rows(got_right, [got_right, to_left])
        l = wires.copy(got_right, from_right.at[k], left)
    yield [r, l]
    add_rows(out, [own(me), from_left.at[m - 1], from_right.at[m - 1]])


def far_gather(wires, block, n, me, device_of, arrived):
    def send(ref, off):
        return wires.copy(ref, ref, device_of((me + n + off) % n))

    def whole(off):
        return block((me + n + off) % n)

    own = block(me)
    p2, m2, p1, m1 = send(own, 2), send(own, -2), send(own, 1), send(own, -1)
    arrived(0)
    yield [p2]
    p3, p4 = send(whole(-2), 1), send(half_of(whole(-2), 0), 2)
    yield Now([m2])
    m3, m4 = send(whole(2), -1), send(half_of(whole(2), 1), -2)
    yield Now([p1])
    arrived(7)
    yield Now([m1])
    for off in (1, 6, 2):
        arrived(off)
    yield [p3]
    arrived(5)
    yield Now([m3])
    arrived(3)
    yield Now([p4, m4])
    arrived(4)


def far_scatter(wires, own, out, bufs, n, me, device_of):
    lines = FarScatter(
        wires,
        lambda off: own((me + off) % n),
        out,
        bufs,
        lambda off: device_of((me + off) % n),
    )
    for off in (4, 3, 5, 1, 7):
        lines.send(off)
    yield from lines.turns("l")
    other = lines.turns("r")
    yield Now(next(other))
    next(other, None)
    yield from lines.last_round()


class FarScatter:
    def __init__(self, wires, own, out, bufs, device_of):
        self.wires, self.own, self.out, self.device_of = wires, own, out, device_of
        self.bufs, self.sent = bufs, {}

    def copy(self, name, src, dst, off):
        self.sent[name] = self.wires.copy(src, dst, self.device_of(off))

    def send(self, off):
        near_l, near_r, turn_l, turn_r, far_l, far_r = [self.bufs.at[i] for i in range(6)]
        term = self.own(off)
        if off == 1:
            self.copy("near_l", term, near_l, 1)
        elif off == 7:
            self.copy("near_r", term, near_r, 7)
        elif off == 3:
            self.copy("turn_l", term, turn_l, 1)
        elif off == 5:
            self.copy("turn_r", term, turn_r, 7)
        elif off == 4:
            self.copy("far_l", half_of(term, 0), half_of(far_l, 0), 2)
            self.copy("far_r", half_of(term, 1), half_of(far_r, 1), 6)

    def turn(self, side):
        n, off, full = (0, 2, 0) if side == "l" else (1, 6, 1)
        turn, far, into = self.bufs.at[2 + n], self.bufs.at[4 + n], self.bufs.at[6 + n]
        mine = self.own(off)
        add_rows(half_of(turn, full), [half_of(x, full) for x in (turn, far, mine)])
        add_rows(half_of(turn, 1 - full), [half_of(x, 1 - full) for x in (turn, mine)])
        self.copy("sum_" + side, turn, into, off)

    def turns(self, side):
        yield [self.sent["turn_" + side], self.sent["far_" + side]]
        self.turn(side)

    def last_round(self):
        yield [self.sent[n] for n in ("near_l", "near_r", "sum_l", "sum_r")]
        near_l, near_r, sum_l, sum_r = [self.bufs.at[i] for i in (0, 1, 6, 7)]
        add_rows(self.out, [self.own(0), near_l, near_r, sum_l, sum_r])


def exchange(send_sem, recv_sem, source, target, axis, n, me, meanwhile=None):
    def copy(off):
        peer = (me + off) % n
        return pltpu.make_async_remote_copy(
            src_ref=source(peer),
            dst_ref=target(me),
            send_sem=send_sem.at[off],
            recv_sem=recv_sem.at[off],
            device_id=axis(peer) if callable(axis) else {axis: peer},
            device_id_type=MESH,
        )

    def start(off, carry):
        copy(off).start()
        return carry

    def wait(off, carry):
        copy(off).wait()
        return carry

    lax.fori_loop(1, n, start, 0)
    if meanwhile:
        meanwhile()
    lax.fori_loop(1, n, wait, 0)


QKV_PARTS = ((0, 256), (256, 512), (768, 512))
QKV_ORDER = "g2 K k1 q1 O p2 A k2 q2 B a1 k3 b1 o1 H a2 b2 k4"
GATHER_SPLIT = 768
DOWN_SPLIT = 640


CHUNKS = {"e": (0,), "b": (1, 7), "c": (3, 4), "d": (5,), "a": (2, 6)}
OUT_CHUNKS = {0: (0, 7, 1, 6, 2), 1: (5, 3, 4)}


def gather_rows(wires, steps, at, out_ref, split, chunks, ready):
    first, rest = pl.ds(0, split), pl.ds(split, out_ref.shape[-1] - split)
    seen = collections.Counter()

    def z_at(off):
        return (at.z + off) % NZ

    def mark(off):
        seen[off] += 1
        for c, chunk in chunks.items():
            if off in chunk and all(seen[o] == 2 for o in chunk):
                steps.add(ready(c), f"chunk{c}")

    def y_first():
        yield from ring_gather(
            wires, lambda j: out_ref.at[at.z, j, :, rest], NY, at.y, at.along_y
        )
        yield from far_gather(
            wires, lambda i: out_ref.at[i, :, :, rest], NZ, at.z, at.along_z, mark
        )

    def to_y(off):
        def line():
            yield from ring_gather(
                wires, lambda j: out_ref.at[z_at(off), j, :, first], NY, at.y, at.along_y
            )
            mark(off)

        steps.add(line(), f"y{off}")

    steps.add(y_first(), "yz")
    steps.add(
        far_gather(
            wires, lambda i: out_ref.at[i, at.y, :, first], NZ, at.z, at.along_z, to_y
        ),
        "z",
    )


def gather_small(wires, at, ref):
    handed = []

    def to_y(block):
        for off in (1, 3, 2):
            handed.append(wires.copy(block, block, at.along_y((at.y + off) % NY)))

    own = ref.at[at.z, at.y]
    order = (4, 3, 5, 2, 6, 1, 7)
    copies = {off: wires.copy(own, own, at.along_z((at.z + off) % NZ)) for off in order}
    to_y(own)
    yield []
    for off in (1, 7, 2, 6, 3, 5, 4):
        yield Now([copies[off]])
        to_y(ref.at[(at.z + NZ - off) % NZ, at.y])
    yield handed


def chunk_rows(ref, at, chunk):
    blocks = [ref[(at.z + off) % NZ] for off in chunk]
    return jnp.concatenate([b.reshape(-1, b.shape[-1]) for b in blocks], axis=0)


GATHER_ORDER = """yz/1 y0/1 z/1 yz/2 y0/2 E y7/1 y1/1 e1 y6/1 y2/1 z/2 yz/3 y7/2 y1/2 B e2 y6/2 y2/2 b1 y5/1 y3/1 y4/1 yz/4 e3 y5/2 y3/2 y4/2"""
ORDER = """b2 C D A e4 c1 d1 a1 b3 c2 e5 d2 a2 b4 c3 d3 b5 e6 a3 b6 c4 d4 e7 a4 c5 c6 b7 d5 d6 a5 a6 b8 e8 c7 V v1 W w1 d7 a7 c8 d8 a8 T U N n1 t1 u1 n2 L l1"""


def feed_chunk(wires, at, r, c, produced, finished):
    partner = at.partner()
    units = r["gate"].shape[1]
    part, held, total, hidden, down_part = (
        r[f"{name}_{c}"] for name in ("unit_part", "held", "unit_total", "hidden", "down_part")
    )

    def tile(w_ref, col, width, start):
        p = jnp.dot(
            chunk_rows(r["stream"], at, CHUNKS[c]), w_ref[:, pl.ds(col, width)], preferred_element_type=F32
        )
        cols = pl.ds(start + col, width)
        part[:, :, :, :, cols] = p.astype(BF16).reshape(*part.shape[:4], width)

    for t in range(units // 256):
        tile(r["gate"], t * 256, 256, 0)
        tile(r["up"], t * 256, 256, units)
    if units % 256:
        tile(r["gate"], units // 256 * 256, units % 256, 0)
        tile(r["up"], units // 256 * 256, units % 256, units)
    yield [wires.copy(part.at[:, :, 1 - at.core], held, partner)]
    add_rows(held, [held, part.at[:, :, at.core]])
    yield from ring_scatter(
        wires,
        lambda i: held.at[:, i],
        total,
        r[f"from_left_{c}"],
        r[f"from_right_{c}"],
        NX,
        at.x,
        at.along_x,
    )
    for n in range(total.shape[0]):
        gate, up = total[n, :, pl.ds(0, units)], total[n, :, pl.ds(units, units)]
        hidden[n, at.x, at.core] = (jax.nn.silu(gate) * up).astype(BF16)
    handed = []

    def hand_over(i):
        ref = hidden.at[:, i, at.core]
        handed.append(wires.copy(ref, ref, partner))

    yield from ring_gather(
        wires, lambda i: hidden.at[:, i, at.core], NX, at.x, at.along_x, hand_over
    )
    yield handed

    def down(i, carry):
        cols = pl.ds(pl.multiple_of(i * 256, 256), 256)
        p = jnp.dot(
            hidden[...].reshape(-1, units), r["down"][:, cols], preferred_element_type=F32
        )
        down_part[:, :, :, cols] = p.astype(BF16).reshape(*down_part.shape[:3], 256)
        return carry

    lax.fori_loop(0, down_part.shape[-1] // 256, down, 0)
    produced(c)
    yield from ring_scatter(
        wires,
        lambda j: down_part.at[:, j, :, pl.ds(0, DOWN_SPLIT)],
        r[f"down_sum_{c}"],
        r[f"down_left_{c}"],
        r[f"down_right_{c}"],
        NY,
        at.y,
        at.along_y,
    )
    finished(c)


def normalize(values, gain):
    mean_square = jnp.mean(values * values, axis=-1, keepdims=True)
    return (values * lax.rsqrt(mean_square + epsilon) * gain).astype(BF16)


WEIGHTS = ("key", "value", "query", "out", "gate", "up", "down")
SMALL = ("tokens", "attention_gain", "feed_gain")
ALONG_Y = ("key", "value", "query", "out")


def layer_kernel(names, *refs):
    r = dict(zip(names, refs))
    at = Place()
    qkv_wires, wires = Wires(r["send"], r["recv"]), Wires(r["send"], r["recv_2"])
    steps = Steps()
    tokens = r["tokens_held"]
    local_rows, model = tokens.shape
    attended, mixed = r["held_out"].at[0], r["held_out"].at[1]
    cos, sin = r["cos"], r["sin"]

    phase = Phases()
    phase("greet")
    greeted = greet_group("cp", CP, at.cp) + greet_group("tp", TP, at.tp)
    loads = {}
    for n, name in enumerate(SMALL):
        held = r[name + "_held"]
        loads[name] = pltpu.make_async_copy(r[name], held, r["load"].at[len(WEIGHTS) + n])
        loads[name].start()
    for n, name in enumerate(WEIGHTS):
        held = r[name].at[at.y] if name in ALONG_Y else r[name]
        loads[name] = pltpu.make_async_copy(r[name + "_weight"], held, r["load"].at[n])
        loads[name].start()

    block = cos.shape[0]
    positions = at.cp * block + lax.broadcasted_iota(jnp.int32, (block, HD), 0)
    angles = positions.astype(F32) * r["inverse"][...]
    first_half = lax.broadcasted_iota(jnp.int32, (block, HD), 1) < HD // 2
    cos[...] = jnp.cos(angles)
    sin[...] = jnp.where(first_half, -jnp.sin(angles), jnp.sin(angles))

    for name in SMALL:
        loads[name].wait()
    normed = normalize(tokens[...].astype(F32), r["attention_gain_held"][...])
    slices, got, columns = r["slices"], r["got"], r["columns"]
    wide = slices.shape[-1]
    for z in range(NZ):
        slices[z] = normed[:, z * wide : (z + 1) * wide]
    phase("barrier")
    await_greetings(greeted)

    phase("spread_cp")
    weight_wires = Wires(r["send_w"], r["recv_w"])
    query_cols, out_cols = r["query"].shape[-1] // 2, r["out"].shape[-1] // 2

    def gathered(*blocks):
        rings = [ring_gather(weight_wires, b, NY, at.y, at.along_y) for b in blocks]
        while True:
            flights = [advance(g) for g in rings]
            if flights[0] is None:
                return
            yield [c for some in flights for c in some]

    weight_parts = {
        "G": lambda: gathered(lambda j: r["key"].at[j], lambda j: r["value"].at[j]),
        "P": lambda: gathered(lambda j: r["query"].at[j, :, pl.ds(0, query_cols)]),
        "Q": lambda: gathered(lambda j: r["query"].at[j, :, pl.ds(query_cols, query_cols)]),
        "O": lambda: gathered(lambda j: r["out"].at[j, :, pl.ds(0, out_cols)]),
        "H": lambda: gathered(lambda j: r["out"].at[j, :, pl.ds(out_cols, out_cols)]),
    }

    def begin_weights(letter):
        steps.add(weight_parts[letter](), letter.lower())

    def keep_slice():
        for name in ALONG_Y:
            loads[name].wait()
        steps.play("G P", begin_weights)
        got[at.z] = slices[at.z]

    exchange(
        r["send"], r["recv_2"], lambda p: slices.at[p], lambda p: got.at[p], at.along_z, NZ, at.z, keep_slice
    )
    steps.play("g1 Q", begin_weights)

    phase("spread_tp")
    def keep_columns():
        columns[at.tp] = got[...]

    exchange(
        r["send"], r["r0"], lambda p: got, lambda p: columns.at[p], "tp", TP, at.tp, keep_columns
    )
    phase("relayout")
    rows_in = r["rows_in"]

    def in_order(b, carry):
        parts = [columns[t, b].astype(F32) for t in range(TP)]
        rows_in[b] = jnp.concatenate(parts, axis=0).astype(BF16)
        return carry

    steps.play("p1", begin_weights)
    lax.fori_loop(0, NZ, in_order, 0)

    part, summed, shared = r["qkv_part"], r["summed"], r["shared"]

    def product(name, cols, start):
        x = rows_in[...].reshape(-1, wide)
        w = r[name][:, :, cols].reshape(wide, -1)
        p = jnp.dot(x, w, preferred_element_type=F32)
        part[:, :, start : start + p.shape[1]] = p.astype(BF16).reshape(NZ, block, -1)

    def turned(v):
        return (v * cos[...] + pltpu.roll(v, HD // 2, 1) * sin[...]).astype(BF16)

    def unit(n):
        start, extent = QKV_PARTS[n]
        cols = pl.ds(start, extent)
        return far_scatter(
            qkv_wires,
            lambda i: part.at[i, :, cols],
            summed.at[:, cols],
            r[f"sum_{n}"],
            NZ,
            at.z,
            at.along_z,
        )

    def keys_and_values():
        yield from unit(0)
        shared[at.z, at.y, :, pl.ds(0, HD)] = turned(summed[:, pl.ds(0, HD)])
        shared[at.z, at.y, :, pl.ds(HD, HD)] = summed[:, pl.ds(HD, HD)].astype(BF16)
        yield from gather_small(qkv_wires, at, shared)

    def begin_part(letter):
        if letter == "K":
            product("key", slice(None), 0)
            product("value", slice(None), HD)
            steps.add(keys_and_values(), "k")
        elif letter in "AB":
            n = "KAB".index(letter)
            start, extent = QKV_PARTS[n]
            for col in range(0, extent, 256):
                at_col = start - 2 * HD + col
                product("query", slice(at_col, at_col + 256), start + col)
            steps.add(unit(n), letter.lower())
        else:
            begin_weights(letter)

    phase("qkv_sum")
    steps.play(QKV_ORDER, begin_part)
    steps.begun.clear()
    qkv_wires.drain()

    phase("attend")
    every = r["every"]
    heads = (summed.shape[1] - 2 * HD) // HD
    block = summed.shape[0]
    query = jnp.concatenate(
        [turned(summed[:, (2 + h) * HD : (3 + h) * HD]) for h in range(heads)], axis=0
    )
    keys = shared[:, :, :, 0:HD].reshape(-1, HD)
    values = shared[:, :, :, HD : 2 * HD].reshape(-1, HD)
    scores = lax.dot_general(
        query, keys, (((1,), (1,)), ((), ())), preferred_element_type=F32
    ) * HD ** (-0.5)
    key_at = lax.broadcasted_iota(jnp.int32, scores.shape, 1)
    query_at = lax.broadcasted_iota(jnp.int32, scores.shape, 0) % block + at.cp * block
    allowed = key_at <= query_at
    scores = jnp.where(allowed, scores, masked)
    top = jnp.max(scores, axis=-1, keepdims=True)
    weights = jnp.where(allowed, jnp.exp(scores - top), 0.0)
    total = jnp.sum(weights, axis=-1, keepdims=True)
    mean = jnp.dot(weights.astype(BF16), values, preferred_element_type=F32) / total
    mean = mean.astype(BF16)
    for h in range(heads):
        every[at.z, :, h * HD : (h + 1) * HD] = mean[h * block : (h + 1) * block]

    phase("gather_att")
    projected = r["projected"]
    owners, seen = [], set()

    def out_chunk(c):
        chunk = OUT_CHUNKS[c]
        part, arrived, total = r[f"out_part_{c}"], r[f"out_got_{c}"], r[f"out_total_{c}"]
        x = jnp.concatenate([every[(at.z + off) % NZ] for off in chunk], axis=0)
        cols = r["out"].shape[-1]
        for y in range(NY):
            p = jnp.dot(x, r["out"][y], preferred_element_type=F32)
            for n in range(len(chunk)):
                for t in range(TP):
                    first = n * block + t * local_rows
                    part[t, n, :, y * cols : (y + 1) * cols] = p[
                        first : first + local_rows
                    ].astype(BF16)
        copies = []
        for off in range(1, TP):
            to = (at.tp + off) % TP
            copies.append(wires.copy(part.at[to], arrived.at[at.tp], {"tp": to}))
        arrived[at.tp] = part[at.tp]
        yield copies
        for n, off in enumerate(chunk):
            sums = arrived[0, n].astype(F32)
            for t in range(1, TP):
                sums = sums + arrived[t, n].astype(F32)
            total[n] = sums.astype(BF16)
            if off == 0:
                projected[at.z] = total[n]
            else:
                to = at.along_z((at.z + off) % NZ)
                owners.append(wires.copy(total.at[n], projected.at[at.z], to))

    def att_there(off):
        seen.add(off)
        for c, chunk in OUT_CHUNKS.items():
            if off in chunk and seen >= set(chunk):
                steps.play("o2 h1 h2", None)
                steps.add(out_chunk(c), f"out{c}")

    steps.add(
        far_gather(wires, lambda i: every.at[i], NZ, at.z, at.along_z, att_there), "z"
    )
    steps.play("h1 z/1 z/2", None)
    steps.run()
    phase("out_cp")
    for c in owners:
        c.wait_recv()
    wires.drain()
    weight_wires.drain()
    phase("norm_feed")
    wide = projected.shape[-1]
    for z in range(NZ):
        cols = slice(z * wide, (z + 1) * wide)
        attended[:, cols] = (tokens[:, cols].astype(F32) + projected[z].astype(F32)).astype(BF16)

    leaving = [
        pltpu.make_async_copy(r["held_out"].at[n], r["streams"].at[n], r["leave"].at[n])
        for n in range(2)
    ]
    leaving[0].start()

    normed = normalize(attended[...].astype(F32), r["feed_gain_held"][...])
    by_width, got_width, stream = r["by_width"], r["got_width"], r["stream"]
    wide = by_width.shape[-1]
    for t in range(TP):
        by_width[t] = normed[:, t * wide : (t + 1) * wide]

    phase("swap1")
    def keep_width():
        got_width[at.tp] = by_width[at.tp]

    exchange(
        r["send"],
        r["r1"],
        lambda p: by_width.at[p],
        lambda p: got_width.at[p],
        "tp",
        TP,
        at.tp,
        keep_width,
    )
    phase("gather_feed")
    stream[at.z, at.y] = jnp.concatenate(
        [got_width[t].astype(F32) for t in range(TP)], axis=0
    ).astype(BF16)
    for name in ("gate", "up", "down"):
        loads[name].wait()
    reduced = r["reduced"]
    places = {off: (c, n) for c, chunk in CHUNKS.items() for n, off in enumerate(chunk)}

    def piece(name, off):
        c, n = places[off]
        return r[f"{name}_{c}"].at[n]

    def to_z(off):
        return at.along_z((at.z + off) % NZ)

    lines = FarScatter(
        qkv_wires,
        lambda off: piece("down_sum", off),
        reduced.at[:, pl.ds(0, DOWN_SPLIT)],
        r["down_far"],
        to_z,
    )
    rest = pl.ds(DOWN_SPLIT, reduced.shape[1] - DOWN_SPLIT)
    z_lines = FarScatter(
        qkv_wires,
        lambda off: piece("down_part", off).at[:, :, rest],
        r["z_sum"],
        r["z_far"],
        to_z,
    )
    there = {}

    def produced(c):
        for off in CHUNKS[c]:
            z_lines.send(off)

    def finished(c):
        for off in CHUNKS[c]:
            lines.send(off)

    def z_first_end():
        yield from z_lines.last_round()
        terms, beside = r["z_sum"], []
        for off in (2, 1, 3):
            y = (at.y + off) % NY
            beside.append(qkv_wires.copy(terms.at[y], r["z_got"].at[off], at.along_y(y)))
        yield beside
        arrived = [r["z_got"].at[off] for off in range(1, NY)]
        add_rows(reduced.at[:, rest], [terms.at[at.y], *arrived])

    later = {
        "T": lambda: lines.turns("l"),
        "U": lambda: lines.turns("r"),
        "V": lambda: z_lines.turns("l"),
        "W": lambda: z_lines.turns("r"),
        "N": z_first_end,
        "L": lines.last_round,
    }

    def begin(letter):
        if letter in later:
            gen = later[letter]()
        else:
            assert letter.lower() in there
            gen = feed_chunk(qkv_wires, at, r, letter.lower(), produced, finished)
        steps.add(gen, letter.lower())

    def chunk_there(c):
        there[c] = True
        return iter(())

    gather_rows(qkv_wires, steps, at, stream, GATHER_SPLIT, CHUNKS, chunk_there)
    steps.play(GATHER_ORDER, begin)
    assert len(there) == len(CHUNKS)
    steps.play(ORDER, begin)
    assert not steps.queue
    phase("swap2")
    qkv_wires.drain()
    by_token, lowered = r["by_token"], r["lowered"]
    for t in range(TP):
        by_token[t] = reduced[pl.ds(t * local_rows, local_rows), :].astype(BF16)

    def keep_token():
        lowered[at.tp] = by_token[at.tp]

    exchange(
        r["send"],
        r["r0"],
        lambda p: by_token.at[p],
        lambda p: lowered.at[p],
        "tp",
        TP,
        at.tp,
        keep_token,
    )
    for t in range(TP):
        cols = slice(t * wide, (t + 1) * wide)
        mixed[:, cols] = (attended[:, cols].astype(F32) + lowered[t].astype(F32)).astype(BF16)
    leaving[1].start()
    for c in leaving:
        c.wait()
    phase(None)


VMEM = pl.BlockSpec(memory_space=pltpu.VMEM)
ANY = pl.BlockSpec(memory_space=pl.ANY)
COPIES, COPIES_2, SLOTS = 157, NZ + 2 * (TP - 1) + NZ - 1, 36


def dma(count):
    return pltpu.SemaphoreType.DMA((count,))


def on_device(
    tokens,
    attention_gain,
    query_weight,
    key_weight,
    value_weight,
    out_weight,
    feed_gain,
    gate_weight,
    up_weight,
    down_weight,
):
    local_rows, model = tokens.shape
    block = local_rows * TP
    rows = block * CP
    qkv = query_weight.shape[1] + key_weight.shape[1] + value_weight.shape[1]
    units = gate_weight.shape[1]
    wide = model // TP

    pair = np.arange(HD, dtype=np.float32)[None] % (HD // 2)
    inverse = (np.float64(rope_base) ** (-(pair * 2.0 / HD))).astype(np.float32)

    inputs = {
        "tokens": tokens,
        "attention_gain": attention_gain[None],
        "feed_gain": feed_gain[None],
        "inverse": jnp.asarray(inverse),
        "key_weight": key_weight,
        "value_weight": value_weight,
        "query_weight": query_weight,
        "out_weight": out_weight,
        "gate_weight": gate_weight,
        "up_weight": up_weight,
        "down_weight": down_weight,
    }

    def buf(*shape, kind=BF16):
        return pltpu.VMEM(shape, kind)

    scratch = {name: buf(*inputs[name + "_weight"].shape) for name in WEIGHTS}
    scratch |= {
        "cos": buf(block, HD, kind=F32),
        "sin": buf(block, HD, kind=F32),
        "slices": buf(NZ, local_rows, wide),
        "got": buf(NZ, local_rows, wide),
        "columns": buf(TP, NZ, local_rows, wide),
        "rows_in": buf(NZ, block, wide),
        "qkv_part": buf(NZ, block, qkv),
        "summed": buf(block, qkv, kind=F32),
        "shared": buf(NZ, NY, block, 2 * HD),
        "every": buf(NZ, block, wide),
        "projected": buf(NZ, local_rows, wide),
        "by_width": buf(TP, local_rows, wide),
        "got_width": buf(TP, local_rows, wide),
        "stream": buf(NZ, NY, block, wide),
        "down_far": buf(8, block, DOWN_SPLIT),
        "z_far": buf(8, NY, block, wide - DOWN_SPLIT),
        "z_sum": buf(NY, block, wide - DOWN_SPLIT),
        "z_got": buf(NY, block, wide - DOWN_SPLIT),
        "reduced": buf(block, wide, kind=F32),
        "by_token": buf(TP, local_rows, wide),
        "lowered": buf(TP, local_rows, wide),
    }
    for name in SMALL:
        scratch[name + "_held"] = buf(*inputs[name].shape, kind=inputs[name].dtype)
    for name in ALONG_Y:
        scratch[name] = buf(NY, *inputs[name + "_weight"].shape)
    for c, chunk in OUT_CHUNKS.items():
        scratch |= {
            f"out_part_{c}": buf(TP, len(chunk), local_rows, wide),
            f"out_got_{c}": buf(TP, len(chunk), local_rows, wide),
            f"out_total_{c}": buf(len(chunk), local_rows, wide),
        }
    for c, chunk in CHUNKS.items():
        n, half = len(chunk), block // 2
        scratch |= {
            f"unit_part_{c}": buf(n, NX, 2, half, 2 * units),
            f"held_{c}": buf(n, NX, half, 2 * units),
            f"from_left_{c}": buf(NX // 2, n, half, 2 * units),
            f"from_right_{c}": buf(NX // 2, n, half, 2 * units),
            f"unit_total_{c}": buf(n, half, 2 * units, kind=F32),
            f"hidden_{c}": buf(n, NX, 2, half, units),
            f"down_part_{c}": buf(n, NY, block, wide),
            f"down_left_{c}": buf(NY // 2, n, block, DOWN_SPLIT),
            f"down_right_{c}": buf(NY // 2, n, block, DOWN_SPLIT),
            f"down_sum_{c}": buf(n, block, DOWN_SPLIT),
        }
    for n, (_, extent) in enumerate(QKV_PARTS):
        scratch[f"sum_{n}"] = buf(NZ, block, extent)
    scratch |= {f"r{n}": dma(TP) for n in range(2)}
    scratch |= {"load": dma(len(WEIGHTS) + len(SMALL)), "send": dma(SLOTS), "recv": dma(COPIES)}
    scratch |= {"held_out": buf(2, *tokens.shape), "leave": dma(2)}
    scratch |= {"recv_2": dma(COPIES_2), "send_w": dma(8), "recv_w": dma(24)}

    names = (*inputs, "streams", *scratch)
    streams = pl.pallas_call(
        functools.partial(layer_kernel, names),
        out_shape=jax.ShapeDtypeStruct((2, *tokens.shape), BF16),
        in_specs=[VMEM if name == "inverse" else ANY for name in inputs],
        out_specs=ANY,
        scratch_shapes=list(scratch.values()),
        compiler_params=pltpu.CompilerParams(
            collective_id=0,
            has_side_effects=True,
            vmem_limit_bytes=60 * 1024 * 1024,
        ),
        name="layer",
    )(*inputs.values())
    return streams[0], streams[1]


def solution(mesh):
    in_specs = (
        P(("cp", "tp"), None),
        P(),
        P("cp", "tp"),
        P("cp", "tp"),
        P("cp", "tp"),
        P("tp", "cp"),
        P(),
        P("tp", "cp"),
        P("tp", "cp"),
        P("cp", "tp"),
    )
    out_specs = (P(("cp", "tp"), None), P(("cp", "tp"), None))
    return jax.shard_map(
        on_device, mesh=mesh, in_specs=in_specs, out_specs=out_specs, check_vma=False
    )
```

```python
import collections
import functools

import jax
import jax.numpy as jnp
import numpy as np
from jax import lax
from jax.experimental import pallas as pl
from jax.experimental.pallas import tpu as pltpu
from jax.sharding import PartitionSpec as P

HD = 128
NZ, NY, NX = 8, 4, 4
CP, TP = NZ * NY, NX * 2
MESH = pl.DeviceIdType.MESH
F32, BF16 = jnp.float32, jnp.bfloat16

epsilon = 1e-05
rope_base = 500000.0
masked = -1e30


class Wires:
    def __init__(self, send, recv):
        self.send, self.recv, self.used, self.sent = send, recv, 0, []

    def copy(self, src, dst, device):
        i, slots = self.used, self.send.shape[0]
        self.used += 1
        assert i < self.recv.shape[0]
        if i >= slots:
            self.sent[i - slots].wait_send()
        c = pltpu.make_async_remote_copy(
            src_ref=src,
            dst_ref=dst,
            send_sem=self.send.at[i % slots],
            recv_sem=self.recv.at[i],
            device_id=device,
            device_id_type=MESH,
        )
        c.start()
        self.sent.append(c)
        return c

    def drain(self):
        for c in self.sent[-self.send.shape[0] :]:
            c.wait_send()
        self.sent, self.used = [], 0


class Now(list):
    pass


def advance(gen):
    needs = next(gen, None)
    while isinstance(needs, Now):
        for c in needs:
            c.wait_recv()
        needs = next(gen, None)
    return needs


class Steps:
    def __init__(self):
        self.queue, self.begun = collections.deque(), set()

    def add(self, gen, name="line", step=0):
        needs = advance(gen)
        if needs is not None:
            self.queue.append((needs, gen, name, step + 1))

    def go_on(self, entry):
        needs, gen, name, step = entry
        for c in needs:
            c.wait_recv()
        self.add(gen, name, step)

    def run(self, until=lambda: False):
        while self.queue and not until():
            self.go_on(self.queue.popleft())

    def play(self, order, begin):
        for word in (w for part in order for w in part.split()):
            if word.isupper():
                if word not in self.begun:
                    self.begun.add(word)
                    begin(word)
                continue
            name, step = word.split("/") if "/" in word else (word[0], word[1:])
            step = int(step)
            while True:
                found = [i for i, e in enumerate(self.queue) if e[2] == name]
                if not found or self.queue[found[0]][3] > step:
                    break
                entry = self.queue[found[0]]
                del self.queue[found[0]]
                self.go_on(entry)


class Place:
    def __init__(self):
        self.cp, self.tp = lax.axis_index("cp"), lax.axis_index("tp")
        self.z, self.y = self.cp // NY, self.cp % NY
        self.x, self.core = self.tp // 2, self.tp % 2

    def along_z(self, z):
        return {"cp": z * NY + self.y}

    def along_y(self, y):
        return {"cp": self.z * NY + y}

    def along_x(self, x):
        return {"tp": x * 2 + self.core}

    def partner(self):
        return {"tp": self.x * 2 + 1 - self.core}


def ring(n, me, device_of):
    return device_of((me + 1) % n), device_of((me + n - 1) % n)


def greet(devices):
    barrier = pltpu.get_barrier_semaphore()
    for device in devices:
        pl.semaphore_signal(barrier, inc=1, device_id=device, device_id_type=MESH)
    return len(devices)


def greet_group(axis, n, me):
    barrier = pltpu.get_barrier_semaphore()

    def signal(off, carry):
        pl.semaphore_signal(
            barrier, inc=1, device_id={axis: (me + off) % n}, device_id_type=MESH
        )
        return carry

    lax.fori_loop(1, n, signal, 0)
    return n - 1


def await_greetings(count):
    pl.semaphore_wait(pltpu.get_barrier_semaphore(), count)


def half_of(ref, h):
    d = ref.shape[0] // 2
    if d:
        return ref.at[pl.ds(h * d, d)]
    width = ref.shape[-1]
    d = -(-width // 256) * 128
    cols = pl.ds(0, d) if h == 0 else pl.ds(d, width - d)
    return ref.at[(slice(None),) * (len(ref.shape) - 1) + (cols,)]


def ring_gather(wires, block, n, me, device_of, arrived=None):
    right, left = ring(n, me, device_of)
    last = n // 2 - 1

    def send(k):
        r, l = block((me + n - k) % n), block((me + k) % n)
        if k == last:
            r, l = half_of(r, 0), half_of(l, 1)
        return wires.copy(r, r, right), wires.copy(l, l, left)

    flying = send(0)
    if arrived:
        arrived(me)
    for k in range(1, n // 2 + 1):
        yield flying
        if k <= last:
            flying = send(k)
            if arrived:
                arrived((me + n - k) % n)
                arrived((me + k) % n)
        elif arrived:
            arrived((me + n // 2) % n)


def add_rows(dst, terms, finish=None):
    if len(dst.shape) > 2:
        for i in range(dst.shape[0]):
            add_rows(dst.at[i], [t.at[i] for t in terms])
        return
    rows = dst.shape[0]
    step = min(rows, 16)

    def body(i, carry):
        at = pl.ds(pl.multiple_of(i * step, step), step)
        total = terms[0][at, :].astype(F32)
        for t in terms[1:]:
            total = total + t[at, :].astype(F32)
        dst[at, :] = total.astype(dst.dtype)
        return carry

    lax.fori_loop(0, rows // step, body, 0)


def ring_scatter(wires, own, out, from_left, from_right, n, me, device_of):
    right, left = ring(n, me, device_of)
    m = n // 2
    far = own((me + m) % n)
    r = wires.copy(half_of(far, 0), half_of(from_left.at[0], 0), right)
    l = wires.copy(half_of(far, 1), half_of(from_right.at[0], 1), left)
    for k in range(1, m):
        to_right, to_left = own((me + m - k) % n), own((me + n - m + k) % n)
        got_left, got_right = from_left.at[k - 1], from_right.at[k - 1]
        yield [r]
        if k == 1:
            add_rows(half_of(got_left, 0), [half_of(got_left, 0), half_of(to_right, 0)])
            add_rows(half_of(got_left, 1), [half_of(to_right, 1)])
        else:
            add_rows(got_left, [got_left, to_right])
        r = wires.copy(got_left, from_left.at[k], right)
        yield Now([l])
        if k == 1:
            add_rows(half_of(got_right, 1), [half_of(got_right, 1), half_of(to_left, 1)])
            add_rows(half_of(got_right, 0), [half_of(to_left, 0)])
        else:
            add_rows(got_right, [got_right, to_left])
        l = wires.copy(got_right, from_right.at[k], left)
    yield [r, l]
    add_rows(out, [own(me), from_left.at[m - 1], from_right.at[m - 1]])


def far_gather(wires, block, n, me, device_of, arrived):
    def send(ref, off):
        return wires.copy(ref, ref, device_of((me + n + off) % n))

    def whole(off):
        return block((me + n + off) % n)

    own = block(me)
    p2, m2, p1, m1 = send(own, 2), send(own, -2), send(own, 1), send(own, -1)
    arrived(0)
    yield [p2]
    p3, p4 = send(whole(-2), 1), send(half_of(whole(-2), 0), 2)
    yield Now([m2])
    m3, m4 = send(whole(2), -1), send(half_of(whole(2), 1), -2)
    yield Now([p1])
    arrived(7)
    yield Now([m1])
    for off in (1, 6, 2):
        arrived(off)
    yield [p3]
    arrived(5)
    yield Now([m3])
    arrived(3)
    yield Now([p4, m4])
    arrived(4)


def far_scatter(wires, own, out, bufs, n, me, device_of):
    lines = FarScatter(
        wires,
        lambda off: own((me + off) % n),
        out,
        bufs,
        lambda off: device_of((me + off) % n),
    )
    for off in (4, 3, 5, 1, 7):
        lines.send(off)
    yield from lines.turns("l")
    other = lines.turns("r")
    yield Now(next(other))
    next(other, None)
    yield from lines.last_round()


class FarScatter:
    def __init__(self, wires, own, out, bufs, device_of):
        self.wires, self.own, self.out, self.device_of = wires, own, out, device_of
        self.bufs, self.sent = bufs, {}

    def copy(self, name, src, dst, off):
        self.sent[name] = self.wires.copy(src, dst, self.device_of(off))

    def send(self, off):
        near_l, near_r, turn_l, turn_r, far_l, far_r = [self.bufs.at[i] for i in range(6)]
        term = self.own(off)
        if off == 1:
            self.copy("near_l", term, near_l, 1)
        elif off == 7:
            self.copy("near_r", term, near_r, 7)
        elif off == 3:
            self.copy("turn_l", term, turn_l, 1)
        elif off == 5:
            self.copy("turn_r", term, turn_r, 7)
        elif off == 4:
            self.copy("far_l", half_of(term, 0), half_of(far_l, 0), 2)
            self.copy("far_r", half_of(term, 1), half_of(far_r, 1), 6)

    def turn(self, side):
        n, off, full = (0, 2, 0) if side == "l" else (1, 6, 1)
        turn, far, into = self.bufs.at[2 + n], self.bufs.at[4 + n], self.bufs.at[6 + n]
        mine = self.own(off)
        add_rows(half_of(turn, full), [half_of(x, full) for x in (turn, far, mine)])
        add_rows(half_of(turn, 1 - full), [half_of(x, 1 - full) for x in (turn, mine)])
        self.copy("sum_" + side, turn, into, off)

    def turns(self, side):
        yield [self.sent["turn_" + side], self.sent["far_" + side]]
        self.turn(side)

    def last_round(self):
        yield [self.sent[n] for n in ("near_l", "near_r", "sum_l", "sum_r")]
        near_l, near_r, sum_l, sum_r = [self.bufs.at[i] for i in (0, 1, 6, 7)]
        add_rows(self.out, [self.own(0), near_l, near_r, sum_l, sum_r])


def exchange(send_sem, recv_sem, source, target, axis, n, me, meanwhile=None):
    def copy(off):
        peer = (me + off) % n
        return pltpu.make_async_remote_copy(
            src_ref=source(peer),
            dst_ref=target(me),
            send_sem=send_sem.at[off],
            recv_sem=recv_sem.at[off],
            device_id=axis(peer) if callable(axis) else {axis: peer},
            device_id_type=MESH,
        )

    def start(off, carry):
        copy(off).start()
        return carry

    def wait(off, carry):
        copy(off).wait()
        return carry

    lax.fori_loop(1, n, start, 0)
    if meanwhile:
        meanwhile()
    lax.fori_loop(1, n, wait, 0)


QKV_PARTS = ((0, 256), (256, 512), (768, 512))
QKV_ORDER = (
    "g2 K k1 q1",
    "O p2 A k2",
    "q2 B a1 k3",
    "b1 o1 H a2",
    "b2 k4",
)
GATHER_SPLIT = 768
DOWN_SPLIT = 640


CHUNKS = {"e": (0,), "b": (1, 7), "c": (3, 4), "d": (5,), "a": (2, 6)}
OUT_CHUNKS = {0: (0, 7, 1, 6, 2), 1: (5, 3, 4)}


def gather_rows(wires, steps, at, out_ref, split, chunks, ready):
    first, rest = pl.ds(0, split), pl.ds(split, out_ref.shape[-1] - split)
    seen = collections.Counter()

    def z_at(off):
        return (at.z + off) % NZ

    def mark(off):
        seen[off] += 1
        for c, chunk in chunks.items():
            if off in chunk and all(seen[o] == 2 for o in chunk):
                steps.add(ready(c), f"chunk{c}")

    def y_first():
        yield from ring_gather(
            wires, lambda j: out_ref.at[at.z, j, :, rest], NY, at.y, at.along_y
        )
        yield from far_gather(
            wires, lambda i: out_ref.at[i, :, :, rest], NZ, at.z, at.along_z, mark
        )

    def to_y(off):
        def line():
            yield from ring_gather(
                wires, lambda j: out_ref.at[z_at(off), j, :, first], NY, at.y, at.along_y
            )
            mark(off)

        steps.add(line(), f"y{off}")

    steps.add(y_first(), "yz")
    steps.add(
        far_gather(
            wires, lambda i: out_ref.at[i, at.y, :, first], NZ, at.z, at.along_z, to_y
        ),
        "z",
    )


def gather_small(wires, at, ref):
    handed = []

    def to_y(block):
        for off in (1, 3, 2):
            handed.append(wires.copy(block, block, at.along_y((at.y + off) % NY)))

    own = ref.at[at.z, at.y]
    order = (4, 3, 5, 2, 6, 1, 7)
    copies = {off: wires.copy(own, own, at.along_z((at.z + off) % NZ)) for off in order}
    to_y(own)
    yield []
    for off in (1, 7, 2, 6, 3, 5, 4):
        yield Now([copies[off]])
        to_y(ref.at[(at.z + NZ - off) % NZ, at.y])
    yield handed


def chunk_rows(ref, at, chunk):
    blocks = [ref[(at.z + off) % NZ] for off in chunk]
    return jnp.concatenate([b.reshape(-1, b.shape[-1]) for b in blocks], axis=0)


GATHER_ORDER = (
    "yz/1 y0/1 z/1 yz/2",
    "y0/2 E y7/1 y1/1",
    "e1 y6/1 y2/1 z/2",
    "yz/3 y7/2 y1/2 B",
    "e2 y6/2 y2/2 b1",
    "y5/1 y3/1 y4/1 yz/4",
    "e3 y5/2 y3/2 y4/2",
)
ORDER = (
    "b2 C D A",
    "e4 c1 d1 a1",
    "b3 c2 e5 d2",
    "a2 b4 c3 d3",
    "b5 e6 a3 b6",
    "c4 d4 e7 a4",
    "c5 c6 b7 d5",
    "d6 a5 a6 b8",
    "e8 c7 V v1",
    "W w1 d7 a7",
    "c8 d8 a8 T",
    "U N n1 t1",
    "u1 n2 L l1",
)


def feed_chunk(wires, at, r, c, produced, finished):
    partner = at.partner()
    units = r.gate.shape[1]
    part, held, total, hidden, down_part = (
        r[f"{name}_{c}"] for name in ("unit_part", "held", "unit_total", "hidden", "down_part")
    )

    def tile(w_ref, col, width, start):
        p = jnp.dot(
            chunk_rows(r.stream, at, CHUNKS[c]), w_ref[:, pl.ds(col, width)], preferred_element_type=F32
        )
        cols = pl.ds(start + col, width)
        part[:, :, :, :, cols] = p.astype(BF16).reshape(*part.shape[:4], width)

    for t in range(units // 256):
        tile(r.gate, t * 256, 256, 0)
        tile(r.up, t * 256, 256, units)
    if units % 256:
        tile(r.gate, units // 256 * 256, units % 256, 0)
        tile(r.up, units // 256 * 256, units % 256, units)
    yield [wires.copy(part.at[:, :, 1 - at.core], held, partner)]
    add_rows(held, [held, part.at[:, :, at.core]])
    yield from ring_scatter(
        wires,
        lambda i: held.at[:, i],
        total,
        r[f"from_left_{c}"],
        r[f"from_right_{c}"],
        NX,
        at.x,
        at.along_x,
    )
    for n in range(total.shape[0]):
        gate, up = total[n, :, pl.ds(0, units)], total[n, :, pl.ds(units, units)]
        hidden[n, at.x, at.core] = (jax.nn.silu(gate) * up).astype(BF16)
    handed = []

    def hand_over(i):
        ref = hidden.at[:, i, at.core]
        handed.append(wires.copy(ref, ref, partner))

    yield from ring_gather(
        wires, lambda i: hidden.at[:, i, at.core], NX, at.x, at.along_x, hand_over
    )
    yield handed

    def down(i, carry):
        cols = pl.ds(pl.multiple_of(i * 256, 256), 256)
        p = jnp.dot(
            hidden[...].reshape(-1, units), r.down[:, cols], preferred_element_type=F32
        )
        down_part[:, :, :, cols] = p.astype(BF16).reshape(*down_part.shape[:3], 256)
        return carry

    lax.fori_loop(0, down_part.shape[-1] // 256, down, 0)
    produced(c)
    yield from ring_scatter(
        wires,
        lambda j: down_part.at[:, j, :, pl.ds(0, DOWN_SPLIT)],
        r[f"down_sum_{c}"],
        r[f"down_left_{c}"],
        r[f"down_right_{c}"],
        NY,
        at.y,
        at.along_y,
    )
    finished(c)


def normalize(values, gain):
    mean_square = jnp.mean(values * values, axis=-1, keepdims=True)
    return (values * lax.rsqrt(mean_square + epsilon) * gain).astype(BF16)


WEIGHTS = ("key", "value", "query", "out", "gate", "up", "down")
SMALL = ("tokens", "attention_gain", "feed_gain")
ALONG_Y = ("key", "value", "query", "out")


class Refs(dict):
    __getattr__ = dict.__getitem__


def layer_kernel(names, *refs):
    r = Refs(zip(names, refs))
    at = Place()
    qkv_wires, wires = Wires(r.send, r.recv), Wires(r.send, r.recv_2)
    steps = Steps()
    tokens = r.tokens_held
    local_rows, model = tokens.shape
    attended, mixed = r.held_out.at[0], r.held_out.at[1]
    cos, sin = r.cos, r.sin

    greeted = greet_group("cp", CP, at.cp) + greet_group("tp", TP, at.tp)
    loads = {}
    for n, name in enumerate(SMALL):
        held = r[name + "_held"]
        loads[name] = pltpu.make_async_copy(r[name], held, r.load.at[len(WEIGHTS) + n])
        loads[name].start()
    for n, name in enumerate(WEIGHTS):
        held = r[name].at[at.y] if name in ALONG_Y else r[name]
        loads[name] = pltpu.make_async_copy(r[name + "_weight"], held, r.load.at[n])
        loads[name].start()

    block = cos.shape[0]
    positions = at.cp * block + lax.broadcasted_iota(jnp.int32, (block, HD), 0)
    angles = positions.astype(F32) * r.inverse[...]
    first_half = lax.broadcasted_iota(jnp.int32, (block, HD), 1) < HD // 2
    cos[...] = jnp.cos(angles)
    sin[...] = jnp.where(first_half, -jnp.sin(angles), jnp.sin(angles))

    for name in SMALL:
        loads[name].wait()
    normed = normalize(tokens[...].astype(F32), r.attention_gain_held[...])
    slices, got, columns = r.slices, r.got, r.columns
    wide = slices.shape[-1]
    for z in range(NZ):
        slices[z] = normed[:, z * wide : (z + 1) * wide]
    await_greetings(greeted)

    weight_wires = Wires(r.send_w, r.recv_w)
    query_cols, out_cols = r.query.shape[-1] // 2, r.out.shape[-1] // 2

    def gathered(*blocks):
        rings = [ring_gather(weight_wires, b, NY, at.y, at.along_y) for b in blocks]
        while True:
            flights = [advance(g) for g in rings]
            if flights[0] is None:
                return
            yield [c for some in flights for c in some]

    weight_parts = {
        "G": lambda: gathered(lambda j: r.key.at[j], lambda j: r.value.at[j]),
        "P": lambda: gathered(lambda j: r.query.at[j, :, pl.ds(0, query_cols)]),
        "Q": lambda: gathered(lambda j: r.query.at[j, :, pl.ds(query_cols, query_cols)]),
        "O": lambda: gathered(lambda j: r.out.at[j, :, pl.ds(0, out_cols)]),
        "H": lambda: gathered(lambda j: r.out.at[j, :, pl.ds(out_cols, out_cols)]),
    }

    def begin_weights(letter):
        steps.add(weight_parts[letter](), letter.lower())

    def keep_slice():
        for name in ALONG_Y:
            loads[name].wait()
        steps.play(("G P",), begin_weights)
        got[at.z] = slices[at.z]

    exchange(
        r.send, r.recv_2, lambda p: slices.at[p], lambda p: got.at[p], at.along_z, NZ, at.z, keep_slice
    )
    steps.play(("g1 Q",), begin_weights)

    def keep_columns():
        columns[at.tp] = got[...]

    exchange(
        r.send, r.r0, lambda p: got, lambda p: columns.at[p], "tp", TP, at.tp, keep_columns
    )
    rows_in = r.rows_in

    def in_order(b, carry):
        parts = [columns[t, b].astype(F32) for t in range(TP)]
        rows_in[b] = jnp.concatenate(parts, axis=0).astype(BF16)
        return carry

    steps.play(("p1",), begin_weights)
    lax.fori_loop(0, NZ, in_order, 0)

    part, summed, shared = r.qkv_part, r.summed, r.shared

    def product(name, cols, start):
        x = rows_in[...].reshape(-1, wide)
        w = r[name][:, :, cols].reshape(wide, -1)
        p = jnp.dot(x, w, preferred_element_type=F32)
        part[:, :, start : start + p.shape[1]] = p.astype(BF16).reshape(NZ, block, -1)

    def turned(v):
        return (v * cos[...] + pltpu.roll(v, HD // 2, 1) * sin[...]).astype(BF16)

    def unit(n):
        start, extent = QKV_PARTS[n]
        cols = pl.ds(start, extent)
        return far_scatter(
            qkv_wires,
            lambda i: part.at[i, :, cols],
            summed.at[:, cols],
            r[f"sum_{n}"],
            NZ,
            at.z,
            at.along_z,
        )

    def keys_and_values():
        yield from unit(0)
        shared[at.z, at.y, :, pl.ds(0, HD)] = turned(summed[:, pl.ds(0, HD)])
        shared[at.z, at.y, :, pl.ds(HD, HD)] = summed[:, pl.ds(HD, HD)].astype(BF16)
        yield from gather_small(qkv_wires, at, shared)

    def begin_part(letter):
        if letter == "K":
            product("key", slice(None), 0)
            product("value", slice(None), HD)
            steps.add(keys_and_values(), "k")
        elif letter in "AB":
            n = "KAB".index(letter)
            start, extent = QKV_PARTS[n]
            for col in range(0, extent, 256):
                at_col = start - 2 * HD + col
                product("query", slice(at_col, at_col + 256), start + col)
            steps.add(unit(n), letter.lower())
        else:
            begin_weights(letter)

    steps.play(QKV_ORDER, begin_part)
    steps.begun.clear()
    qkv_wires.drain()

    every = r.every
    heads = (summed.shape[1] - 2 * HD) // HD
    block = summed.shape[0]
    query = jnp.concatenate(
        [turned(summed[:, (2 + h) * HD : (3 + h) * HD]) for h in range(heads)], axis=0
    )
    keys = shared[:, :, :, 0:HD].reshape(-1, HD)
    values = shared[:, :, :, HD : 2 * HD].reshape(-1, HD)
    scores = lax.dot_general(
        query, keys, (((1,), (1,)), ((), ())), preferred_element_type=F32
    ) * HD ** (-0.5)
    key_at = lax.broadcasted_iota(jnp.int32, scores.shape, 1)
    query_at = lax.broadcasted_iota(jnp.int32, scores.shape, 0) % block + at.cp * block
    allowed = key_at <= query_at
    scores = jnp.where(allowed, scores, masked)
    top = jnp.max(scores, axis=-1, keepdims=True)
    weights = jnp.where(allowed, jnp.exp(scores - top), 0.0)
    total = jnp.sum(weights, axis=-1, keepdims=True)
    mean = jnp.dot(weights.astype(BF16), values, preferred_element_type=F32) / total
    mean = mean.astype(BF16)
    for h in range(heads):
        every[at.z, :, h * HD : (h + 1) * HD] = mean[h * block : (h + 1) * block]

    projected = r.projected
    owners, seen = [], set()

    def out_chunk(c):
        chunk = OUT_CHUNKS[c]
        part, arrived, total = r[f"out_part_{c}"], r[f"out_got_{c}"], r[f"out_total_{c}"]
        x = jnp.concatenate([every[(at.z + off) % NZ] for off in chunk], axis=0)
        cols = r.out.shape[-1]
        for y in range(NY):
            p = jnp.dot(x, r.out[y], preferred_element_type=F32)
            for n in range(len(chunk)):
                for t in range(TP):
                    first = n * block + t * local_rows
                    part[t, n, :, y * cols : (y + 1) * cols] = p[
                        first : first + local_rows
                    ].astype(BF16)
        copies = []
        for off in range(1, TP):
            to = (at.tp + off) % TP
            copies.append(wires.copy(part.at[to], arrived.at[at.tp], {"tp": to}))
        arrived[at.tp] = part[at.tp]
        yield copies
        for n, off in enumerate(chunk):
            sums = arrived[0, n].astype(F32)
            for t in range(1, TP):
                sums = sums + arrived[t, n].astype(F32)
            total[n] = sums.astype(BF16)
            if off == 0:
                projected[at.z] = total[n]
            else:
                to = at.along_z((at.z + off) % NZ)
                owners.append(wires.copy(total.at[n], projected.at[at.z], to))

    def att_there(off):
        seen.add(off)
        for c, chunk in OUT_CHUNKS.items():
            if off in chunk and seen >= set(chunk):
                steps.play(("o2 h1 h2",), None)
                steps.add(out_chunk(c), f"out{c}")

    steps.add(
        far_gather(wires, lambda i: every.at[i], NZ, at.z, at.along_z, att_there), "z"
    )
    steps.play(("h1 z/1 z/2",), None)
    steps.run()
    for c in owners:
        c.wait_recv()
    wires.drain()
    weight_wires.drain()
    wide = projected.shape[-1]
    for z in range(NZ):
        cols = slice(z * wide, (z + 1) * wide)
        attended[:, cols] = (tokens[:, cols].astype(F32) + projected[z].astype(F32)).astype(BF16)

    leaving = [
        pltpu.make_async_copy(r.held_out.at[n], r.streams.at[n], r.leave.at[n])
        for n in range(2)
    ]
    leaving[0].start()

    normed = normalize(attended[...].astype(F32), r.feed_gain_held[...])
    by_width, got_width, stream = r.by_width, r.got_width, r.stream
    wide = by_width.shape[-1]
    for t in range(TP):
        by_width[t] = normed[:, t * wide : (t + 1) * wide]

    def keep_width():
        got_width[at.tp] = by_width[at.tp]

    exchange(
        r.send,
        r.r1,
        lambda p: by_width.at[p],
        lambda p: got_width.at[p],
        "tp",
        TP,
        at.tp,
        keep_width,
    )
    stream[at.z, at.y] = jnp.concatenate(
        [got_width[t].astype(F32) for t in range(TP)], axis=0
    ).astype(BF16)
    for name in ("gate", "up", "down"):
        loads[name].wait()
    reduced = r.reduced
    places = {off: (c, n) for c, chunk in CHUNKS.items() for n, off in enumerate(chunk)}

    def piece(name, off):
        c, n = places[off]
        return r[f"{name}_{c}"].at[n]

    def to_z(off):
        return at.along_z((at.z + off) % NZ)

    lines = FarScatter(
        qkv_wires,
        lambda off: piece("down_sum", off),
        reduced.at[:, pl.ds(0, DOWN_SPLIT)],
        r.down_far,
        to_z,
    )
    rest = pl.ds(DOWN_SPLIT, reduced.shape[1] - DOWN_SPLIT)
    z_lines = FarScatter(
        qkv_wires,
        lambda off: piece("down_part", off).at[:, :, rest],
        r.z_sum,
        r.z_far,
        to_z,
    )
    there = {}

    def produced(c):
        for off in CHUNKS[c]:
            z_lines.send(off)

    def finished(c):
        for off in CHUNKS[c]:
            lines.send(off)

    def z_first_end():
        yield from z_lines.last_round()
        terms, beside = r.z_sum, []
        for off in (2, 1, 3):
            y = (at.y + off) % NY
            beside.append(qkv_wires.copy(terms.at[y], r.z_got.at[off], at.along_y(y)))
        yield beside
        arrived = [r.z_got.at[off] for off in range(1, NY)]
        add_rows(reduced.at[:, rest], [terms.at[at.y], *arrived])

    later = {
        "T": lambda: lines.turns("l"),
        "U": lambda: lines.turns("r"),
        "V": lambda: z_lines.turns("l"),
        "W": lambda: z_lines.turns("r"),
        "N": z_first_end,
        "L": lines.last_round,
    }

    def begin(letter):
        if letter in later:
            gen = later[letter]()
        else:
            assert letter.lower() in there
            gen = feed_chunk(qkv_wires, at, r, letter.lower(), produced, finished)
        steps.add(gen, letter.lower())

    def chunk_there(c):
        there[c] = True
        return iter(())

    gather_rows(qkv_wires, steps, at, stream, GATHER_SPLIT, CHUNKS, chunk_there)
    steps.play(GATHER_ORDER, begin)
    assert len(there) == len(CHUNKS)
    steps.play(ORDER, begin)
    assert not steps.queue
    qkv_wires.drain()
    by_token, lowered = r.by_token, r.lowered
    for t in range(TP):
        by_token[t] = reduced[pl.ds(t * local_rows, local_rows), :].astype(BF16)

    def keep_token():
        lowered[at.tp] = by_token[at.tp]

    exchange(
        r.send,
        r.r0,
        lambda p: by_token.at[p],
        lambda p: lowered.at[p],
        "tp",
        TP,
        at.tp,
        keep_token,
    )
    for t in range(TP):
        cols = slice(t * wide, (t + 1) * wide)
        mixed[:, cols] = (attended[:, cols].astype(F32) + lowered[t].astype(F32)).astype(BF16)
    leaving[1].start()
    for c in leaving:
        c.wait()


VMEM = pl.BlockSpec(memory_space=pltpu.VMEM)
ANY = pl.BlockSpec(memory_space=pl.ANY)
COPIES, COPIES_2, SLOTS = 157, NZ + 2 * (TP - 1) + NZ - 1, 36


def dma(count):
    return pltpu.SemaphoreType.DMA((count,))


def on_device(
    tokens,
    attention_gain,
    query_weight,
    key_weight,
    value_weight,
    out_weight,
    feed_gain,
    gate_weight,
    up_weight,
    down_weight,
):
    local_rows, model = tokens.shape
    block = local_rows * TP
    rows = block * CP
    qkv = query_weight.shape[1] + key_weight.shape[1] + value_weight.shape[1]
    units = gate_weight.shape[1]
    wide = model // TP

    pair = np.arange(HD, dtype=np.float32)[None] % (HD // 2)
    inverse = (np.float64(rope_base) ** (-(pair * 2.0 / HD))).astype(np.float32)

    inputs = dict(
        tokens=tokens,
        attention_gain=attention_gain[None],
        feed_gain=feed_gain[None],
        inverse=jnp.asarray(inverse),
        key_weight=key_weight,
        value_weight=value_weight,
        query_weight=query_weight,
        out_weight=out_weight,
        gate_weight=gate_weight,
        up_weight=up_weight,
        down_weight=down_weight,
    )

    def buf(*shape, kind=BF16):
        return pltpu.VMEM(shape, kind)

    scratch = {name: buf(*inputs[name + "_weight"].shape) for name in WEIGHTS}
    scratch |= dict(
        cos=buf(block, HD, kind=F32),
        sin=buf(block, HD, kind=F32),
        slices=buf(NZ, local_rows, wide),
        got=buf(NZ, local_rows, wide),
        columns=buf(TP, NZ, local_rows, wide),
        rows_in=buf(NZ, block, wide),
        qkv_part=buf(NZ, block, qkv),
        summed=buf(block, qkv, kind=F32),
        shared=buf(NZ, NY, block, 2 * HD),
        every=buf(NZ, block, wide),
        projected=buf(NZ, local_rows, wide),
        by_width=buf(TP, local_rows, wide),
        got_width=buf(TP, local_rows, wide),
        stream=buf(NZ, NY, block, wide),
        down_far=buf(8, block, DOWN_SPLIT),
        z_far=buf(8, NY, block, wide - DOWN_SPLIT),
        z_sum=buf(NY, block, wide - DOWN_SPLIT),
        z_got=buf(NY, block, wide - DOWN_SPLIT),
        reduced=buf(block, wide, kind=F32),
        by_token=buf(TP, local_rows, wide),
        lowered=buf(TP, local_rows, wide),
    )
    for name in SMALL:
        scratch[name + "_held"] = buf(*inputs[name].shape, kind=inputs[name].dtype)
    for name in ALONG_Y:
        scratch[name] = buf(NY, *inputs[name + "_weight"].shape)
    for c, chunk in OUT_CHUNKS.items():
        scratch |= {
            f"out_part_{c}": buf(TP, len(chunk), local_rows, wide),
            f"out_got_{c}": buf(TP, len(chunk), local_rows, wide),
            f"out_total_{c}": buf(len(chunk), local_rows, wide),
        }
    for c, chunk in CHUNKS.items():
        n, half = len(chunk), block // 2
        scratch |= {
            f"unit_part_{c}": buf(n, NX, 2, half, 2 * units),
            f"held_{c}": buf(n, NX, half, 2 * units),
            f"from_left_{c}": buf(NX // 2, n, half, 2 * units),
            f"from_right_{c}": buf(NX // 2, n, half, 2 * units),
            f"unit_total_{c}": buf(n, half, 2 * units, kind=F32),
            f"hidden_{c}": buf(n, NX, 2, half, units),
            f"down_part_{c}": buf(n, NY, block, wide),
            f"down_left_{c}": buf(NY // 2, n, block, DOWN_SPLIT),
            f"down_right_{c}": buf(NY // 2, n, block, DOWN_SPLIT),
            f"down_sum_{c}": buf(n, block, DOWN_SPLIT),
        }
    for n, (_, extent) in enumerate(QKV_PARTS):
        scratch[f"sum_{n}"] = buf(NZ, block, extent)
    scratch |= {f"r{n}": dma(TP) for n in range(2)}
    scratch |= {"load": dma(len(WEIGHTS) + len(SMALL)), "send": dma(SLOTS), "recv": dma(COPIES)}
    scratch |= {"held_out": buf(2, *tokens.shape), "leave": dma(2)}
    scratch |= {"recv_2": dma(COPIES_2), "send_w": dma(8), "recv_w": dma(24)}

    names = (*inputs, "streams", *scratch)
    streams = pl.pallas_call(
        functools.partial(layer_kernel, names),
        out_shape=jax.ShapeDtypeStruct((2, *tokens.shape), BF16),
        in_specs=[VMEM if name == "inverse" else ANY for name in inputs],
        out_specs=ANY,
        scratch_shapes=list(scratch.values()),
        compiler_params=pltpu.CompilerParams(
            collective_id=0,
            has_side_effects=True,
            vmem_limit_bytes=60 * 1024 * 1024,
        ),
        name="layer",
    )(*inputs.values())
    return streams[0], streams[1]


def solution(mesh):
    in_specs = (
        P(("cp", "tp"), None),
        P(),
        P("cp", "tp"),
        P("cp", "tp"),
        P("cp", "tp"),
        P("tp", "cp"),
        P(),
        P("tp", "cp"),
        P("tp", "cp"),
        P("cp", "tp"),
    )
    out_specs = (P(("cp", "tp"), None), P(("cp", "tp"), None))
    return jax.shard_map(
        on_device, mesh=mesh, in_specs=in_specs, out_specs=out_specs, check_vma=False
    )
```
